32 devices in a mesh: fsdp: 8 (over y, x, core), dp: 4 (over z).
Axes of the slice: x: 2, y: 2, z: 4, core: 2. Of those that a mesh axis runs over, the one named last changes fastest.
Arguments:
- tokens: bfloat16 [4096, 1536], P(('fsdp', 'dp')), may hold values from -6 to 6
- lengths: int32 [32, 4], P('fsdp'), may hold values from 1 to 64, 128 in all within a row
- cotangent: bfloat16 [4096, 1536], P(('fsdp', 'dp')), may hold values from -6 to 6
- attn_gain: bfloat16 [1, 1536], P(None, 'fsdp'), may hold values from 0.5 to 1.5
- w_query: bfloat16 [1, 1536, 1536], P(None, 'fsdp', 'dp'), may hold values from -0.15625 to 0.15625
- w_key: bfloat16 [1, 1536, 768], P(None, 'fsdp', 'dp'), may hold values from -0.15625 to 0.15625
- w_value: bfloat16 [1, 1536, 768], P(None, 'fsdp', 'dp'), may hold values from -0.15625 to 0.15625
- w_out: bfloat16 [1, 1536, 1536], P(None, 'dp', 'fsdp'), may hold values from -0.875 to 0.875
- mlp_gain: bfloat16 [1, 1536], P(None, 'fsdp'), may hold values from 0.5 to 1.5
- w_gate: bfloat16 [1, 1536, 4096], P(None, 'fsdp', 'dp'), may hold values from -0.15625 to 0.15625
- w_up: bfloat16 [1, 1536, 4096], P(None, 'fsdp', 'dp'), may hold values from -0.15625 to 0.15625
- w_down: bfloat16 [1, 4096, 1536], P(None, 'dp', 'fsdp'), may hold values from -0.09375 to 0.09375
Outputs:
- output: bfloat16 [4096, 1536], P(('fsdp', 'dp'))
- grad_tokens: float32 [4096, 1536], P(('fsdp', 'dp'))
- grad_attn_gain: float32 [1, 1536], P(None, 'fsdp')
- grad_w_query: float32 [1, 1536, 1536], P(None, 'fsdp', 'dp')
- grad_w_key: float32 [1, 1536, 768], P(None, 'fsdp', 'dp')
- grad_w_value: float32 [1, 1536, 768], P(None, 'fsdp', 'dp')
- grad_w_out: float32 [1, 1536, 1536], P(None, 'dp', 'fsdp')
- grad_mlp_gain: float32 [1, 1536], P(None, 'fsdp')
- grad_w_gate: float32 [1, 1536, 4096], P(None, 'fsdp', 'dp')
- grad_w_up: float32 [1, 1536, 4096], P(None, 'fsdp', 'dp')
- grad_w_down: float32 [1, 4096, 1536], P(None, 'dp', 'fsdp')
The draws below stay inside these ranges and needn't reach their ends.
Inputs may be any that keep to these rules, and one draw needn't show every extreme that they name: `lengths`: each row sums to 128 and its largest entry is 64.
All inputs are finite; a program needn't handle non-finite values.
Results may differ from the reference program's by a relative error of at most 0.019.
Values may be sent and summed in bfloat16 or wider, within the bound.
A program may use at most 320 MiB of HBM per device.

```python
import math
import jax
import jax.numpy as jnp
import numpy as np
from jax import lax

D = 1536
H = 16
KVH = 8
HD = 96
FF = 4096
LAYERS = 1
TOK_DEV = 128
SEQ_MAX = 64
NSEQ = 4
TOKENS = 4096
N_FSDP = 8
N_DP = 4


def level_of(rng, extent, shards, least, top_value):
    level = 1.0
    for position, parts in shards:
        heights = jax.random.uniform(jax.random.fold_in(jax.random.fold_in(rng, 6), position), (parts,), jnp.float32, least / len(shards), top_value / len(shards))
        level = level * jnp.repeat(jnp.exp(heights), extent[position] // parts).reshape((-1,) + (1,) * (len(extent) - 1 - position))
    return level


def split_up(number_of, total, reach, skew):
    portions = [(1 << 20) // math.isqrt(standing ** skew) + 1 for standing in range(2, number_of + 1)]
    rest, holding = total - reach - (number_of - 1), [1] * (number_of - 1)
    while rest > 0:
        candidates = [i for i in range(number_of - 1) if holding[i] < reach]
        whole, remaining = sum([portions[i] for i in candidates]), rest
        for i in candidates:
            more = min(reach - holding[i], max(1, remaining * portions[i] // whole), rest)
            holding[i] = holding[i] + more
            rest = rest - more
    return np.array([reach] + holding)


def uneven_parts(key, count, total, bound, lean):
    if count == 2:
        one = jax.random.randint(key, (), max(1, total - bound), min(bound, total - 1) + 1)
        return jnp.stack([one, total - one])
    tallies = jnp.asarray(split_up(count, total, bound, lean), jnp.int32)
    pairs = (count - 1) // 2
    giver, sink = tallies[1:1 + 2 * pairs:2], tallies[2:2 + 2 * pairs:2]
    slack = jnp.minimum(giver - 1, bound - sink)
    moved = jax.random.randint(jax.random.fold_in(key, 1), (pairs,), 0, 1 << 20) % (slack + 1)
    tallies = tallies.at[1:1 + 2 * pairs:2].set(giver - moved).at[2:2 + 2 * pairs:2].set(sink + moved)
    return tallies[jax.random.permutation(jax.random.fold_in(key, 2), count)]


def noise(stream_key, dims, width, reach, pieces=(), held_as=jnp.bfloat16):
    drawn = jax.random.normal(stream_key, dims, jnp.float32) * width
    if len(pieces) > 0:
        drawn = level_of(stream_key, dims, pieces, -0.22, 0.18) * drawn
    return jnp.clip(drawn, min=-reach, max=reach).astype(held_as)


def setup_inputs(seed: int = 0) -> dict:
    splits = jax.random.split(jax.random.key(seed), 13)
    return {
        "tokens": noise(splits[0], (TOKENS, D), 1.0, 6.0, ((0, 32),)),
        "lengths": jax.vmap(lambda own: uneven_parts(own, NSEQ, TOK_DEV, SEQ_MAX, 2))(jax.random.split(splits[1], (N_FSDP * N_DP))).reshape((N_FSDP * N_DP, NSEQ)).astype(jnp.int32),
        "cotangent": noise(splits[2], (TOKENS, D), 1.0, 6.0, ((0, 32),)),
        "attn_gain": jnp.clip(1.0 + 0.1 * jax.random.normal(splits[3], (LAYERS, D), jnp.float32), 0.5, 1.5).astype(jnp.bfloat16),
        "w_query": noise(splits[4], (LAYERS, D, D), D ** -0.5, 0.15625, ((1, 8), (2, 4))),
        "w_key": noise(splits[5], (LAYERS, D, KVH * HD), D ** -0.5, 0.15625, ((1, 8), (2, 4))),
        "w_value": noise(splits[6], (LAYERS, D, KVH * HD), D ** -0.5, 0.15625, ((1, 8), (2, 4))),
        "w_out": noise(splits[7], (LAYERS, D, D), (D // 32) ** -0.5, 0.875, ((1, 4), (2, 8))),
        "mlp_gain": jnp.clip(1.0 + 0.1 * jax.random.normal(splits[8], (LAYERS, D), jnp.float32), 0.5, 1.5).astype(jnp.bfloat16),
        "w_gate": noise(splits[9], (LAYERS, D, FF), D ** -0.5, 0.15625, ((1, 8), (2, 4))),
        "w_up": noise(splits[10], (LAYERS, D, FF), D ** -0.5, 0.15625, ((1, 8), (2, 4))),
        "w_down": noise(splits[11], (LAYERS, FF, D), FF ** -0.5, 0.09375, ((1, 4), (2, 8))),
    }


EPSILON = 1e-05
ROPE_BASE = 100000.0
NEG_FILL = -1e+30

def layout(seq_lengths, rows_here):
    seq_lengths = seq_lengths.astype(jnp.int32)
    seg_ends = jnp.cumsum(seq_lengths).astype(jnp.int32)
    seg_starts = (seg_ends - seq_lengths).astype(jnp.int32)
    positions = jnp.arange(rows_here, dtype=jnp.int32)
    segment = lax.optimization_barrier(jnp.sum((positions[:, None] >= seg_ends[None, :]).astype(jnp.int32), axis=1)).astype(jnp.int32)
    member = segment[:, None] == jnp.arange(seq_lengths.shape[0], dtype=jnp.int32)[None, :]
    offset = lax.optimization_barrier(jnp.sum(jnp.where(member, seg_starts[None, :], 0), axis=1)).astype(jnp.int32)
    where_in = (positions - offset).astype(jnp.int32)
    allowed = (segment[:, None] == segment[None, :]) & (positions[None, :] <= positions[:, None])
    half_dim = HD // 2
    frequency = ROPE_BASE ** (-jnp.arange(half_dim, dtype=jnp.float32) / half_dim)
    angles = where_in.astype(jnp.float32)[:, None] * frequency[None, :]
    return (allowed, jnp.cos(angles), jnp.sin(angles))

def rotate(values, cosine, sine_tab, sign_flip):
    half_dim = values.shape[-1] // 2
    front_half = values[..., :half_dim]
    back_half = values[..., half_dim:]
    cos_part = cosine[:, None, :]
    sin_part = sign_flip * sine_tab[:, None, :]
    return jnp.concatenate([front_half * cos_part - back_half * sin_part, back_half * cos_part + front_half * sin_part], axis=-1)

def rms_scale(stream):
    return lax.rsqrt(lax.optimization_barrier(jnp.mean(stream * stream, axis=-1, keepdims=True)) + EPSILON)

def matmul(left, right):
    return jnp.dot(left.astype(jnp.float32), right.astype(jnp.float32), preferred_element_type=jnp.float32)

def attend(queries, keys_rot, values_in, allowed):
    rows_here = queries.shape[0]
    grouped = queries.reshape(rows_here, KVH, H // KVH, HD).astype(jnp.float32)
    scores = jnp.einsum('qkgd,skd->kgqs', grouped, keys_rot.astype(jnp.float32)) * HD ** (-0.5)
    scores = jnp.where(allowed[None, None], scores, NEG_FILL)
    row_top = lax.optimization_barrier(jnp.max(scores, axis=-1, keepdims=True))
    log_total = row_top + jnp.log(lax.optimization_barrier(jnp.sum(jnp.exp(scores - row_top), axis=-1, keepdims=True)))
    attn_probs = jnp.where(allowed[None, None], jnp.exp(scores - log_total), 0.0)
    probs_low = attn_probs.astype(jnp.bfloat16)
    attn_mixed = jnp.einsum('kgqs,skd->qkgd', probs_low.astype(jnp.float32), values_in.astype(jnp.float32))
    return (attn_probs, attn_mixed.reshape(rows_here, H * HD).astype(jnp.bfloat16))

def attend_back(queries, keys_rot, values_in, attn_probs, attn_mixed, grad_mixed):
    rows_here = queries.shape[0]
    groups = H // KVH
    grouped = queries.reshape(rows_here, KVH, groups, HD).astype(jnp.float32)
    grad_grouped = grad_mixed.reshape(rows_here, KVH, groups, HD).astype(jnp.float32)
    mixed_grouped = attn_mixed.reshape(rows_here, KVH, groups, HD).astype(jnp.float32)
    delta = jnp.transpose(lax.optimization_barrier(jnp.sum(grad_grouped * mixed_grouped, axis=-1)), (1, 2, 0))[..., None]
    grad_probs = jnp.einsum('qkgd,skd->kgqs', grad_grouped, values_in.astype(jnp.float32))
    grad_score = (attn_probs * (grad_probs - delta) * HD ** (-0.5)).astype(jnp.bfloat16).astype(jnp.float32)
    probs_low = attn_probs.astype(jnp.bfloat16).astype(jnp.float32)
    grad_q = jnp.einsum('kgqs,skd->qkgd', grad_score, keys_rot.astype(jnp.float32)).reshape(rows_here, H, HD)
    grad_k = jnp.einsum('kgqs,qkgd->skd', grad_score, grouped)
    grad_v = jnp.einsum('kgqs,qkgd->skd', probs_low, grad_grouped)
    return (grad_q, grad_k, grad_v)

def layer_forward(stream, weights, allowed, cosine, sine_tab):
    attn_gain, w_query, w_key, w_value, w_out, mlp_gain, w_gate, w_up, w_down = weights
    rows_here = stream.shape[0]
    scale_one = rms_scale(stream)
    normed_one = stream * scale_one
    attn_in = (normed_one * attn_gain.astype(jnp.float32)).astype(jnp.bfloat16)
    queries = rotate(matmul(attn_in, w_query).reshape(rows_here, H, HD), cosine, sine_tab, 1.0).astype(jnp.bfloat16)
    keys_rot = rotate(matmul(attn_in, w_key).reshape(rows_here, KVH, HD), cosine, sine_tab, 1.0).astype(jnp.bfloat16)
    values_in = matmul(attn_in, w_value).reshape(rows_here, KVH, HD).astype(jnp.bfloat16)
    attn_probs, attn_mixed = attend(queries, keys_rot, values_in, allowed)
    middle = stream + matmul(attn_mixed, w_out)
    scale_two = rms_scale(middle)
    normed_two = middle * scale_two
    mlp_in = (normed_two * mlp_gain.astype(jnp.float32)).astype(jnp.bfloat16)
    gate_act = matmul(mlp_in, w_gate)
    up_act = matmul(mlp_in, w_up)
    hidden = (jax.nn.silu(gate_act) * up_act).astype(jnp.bfloat16)
    result = middle + matmul(hidden, w_down)
    kept_state = (scale_one, normed_one, attn_in, queries, keys_rot, values_in, attn_probs, attn_mixed, scale_two, normed_two, mlp_in, gate_act, up_act, hidden)
    return (result, kept_state)

def layer_backward(stream, weights, allowed, cosine, sine_tab, grad_stream):
    attn_gain, w_query, w_key, w_value, w_out, mlp_gain, w_gate, w_up, w_down = weights
    _, kept_state = layer_forward(stream, weights, allowed, cosine, sine_tab)
    scale_one, normed_one, attn_in, queries, keys_rot, values_in, attn_probs, attn_mixed, scale_two, normed_two, mlp_in, gate_act, up_act, hidden = kept_state
    rows_here = stream.shape[0]
    grad_low = grad_stream.astype(jnp.bfloat16)
    grad_down = matmul(hidden.T, grad_low)
    grad_hidden = matmul(grad_low, w_down.T)
    sigmoid_gate = jax.nn.sigmoid(gate_act)
    grad_up_act = (grad_hidden * gate_act * sigmoid_gate).astype(jnp.bfloat16)
    grad_gate_act = (grad_hidden * up_act * sigmoid_gate * (1.0 + gate_act * (1.0 - sigmoid_gate))).astype(jnp.bfloat16)
    grad_gate = matmul(mlp_in.T, grad_gate_act)
    grad_up = matmul(mlp_in.T, grad_up_act)
    grad_mlp_in = matmul(grad_gate_act, w_gate.T) + matmul(grad_up_act, w_up.T)
    grad_mlp_gain = lax.optimization_barrier(jnp.sum(grad_mlp_in * normed_two, axis=0))
    grad_normed = grad_mlp_in * mlp_gain.astype(jnp.float32)
    grad_middle = grad_stream + scale_two * (grad_normed - normed_two * lax.optimization_barrier(jnp.mean(grad_normed * normed_two, axis=-1, keepdims=True)))
    grad_middle_low = grad_middle.astype(jnp.bfloat16)
    grad_out = matmul(attn_mixed.T, grad_middle_low)
    grad_mixed = matmul(grad_middle_low, w_out.T).astype(jnp.bfloat16)
    grad_q, grad_k, grad_v = attend_back(queries, keys_rot, values_in, attn_probs, attn_mixed, grad_mixed)
    grad_q = rotate(grad_q, cosine, sine_tab, -1.0).reshape(rows_here, H * HD).astype(jnp.bfloat16)
    grad_k = rotate(grad_k, cosine, sine_tab, -1.0).reshape(rows_here, KVH * HD).astype(jnp.bfloat16)
    grad_v = grad_v.reshape(rows_here, KVH * HD).astype(jnp.bfloat16)
    grad_query = matmul(attn_in.T, grad_q)
    grad_key = matmul(attn_in.T, grad_k)
    grad_value = matmul(attn_in.T, grad_v)
    grad_attn_in = matmul(grad_q, w_query.T) + matmul(grad_k, w_key.T) + matmul(grad_v, w_value.T)
    grad_attn_gain = lax.optimization_barrier(jnp.sum(grad_attn_in * normed_one, axis=0))
    grad_normed_one = grad_attn_in * attn_gain.astype(jnp.float32)
    grad_input = grad_middle + scale_one * (grad_normed_one - normed_one * lax.optimization_barrier(jnp.mean(grad_normed_one * normed_one, axis=-1, keepdims=True)))
    return (grad_input, (grad_attn_gain, grad_query, grad_key, grad_value, grad_out, grad_mlp_gain, grad_gate, grad_up, grad_down))

def reference(tokens, lengths, cotangent, attn_gain, w_query, w_key, w_value, w_out, mlp_gain, w_gate, w_up, w_down):
    stacked = (attn_gain, w_query, w_key, w_value, w_out, mlp_gain, w_gate, w_up, w_down)
    wide_weights = tuple((member_w.astype(jnp.float32) for member_w in stacked))

    def one_block(running, block_in):
        block_tokens, block_lengths, block_cot = block_in
        allowed, cosine, sine_tab = layout(block_lengths, TOK_DEV)
        stream = block_tokens.astype(jnp.float32)
        inputs_kept = []
        for layer_idx in range(LAYERS):
            weights = tuple((member_w[layer_idx] for member_w in wide_weights))
            inputs_kept.append(stream)
            stream, _ = layer_forward(stream, weights, allowed, cosine, sine_tab)
        grad_stream = block_cot.astype(jnp.float32)
        grads_by_layer = [None] * LAYERS
        for layer_idx in reversed(range(LAYERS)):
            weights = tuple((member_w[layer_idx] for member_w in wide_weights))
            grad_stream, layer_terms = layer_backward(inputs_kept[layer_idx], weights, allowed, cosine, sine_tab, grad_stream)
            grads_by_layer[layer_idx] = layer_terms
        updated = tuple((running[slot_idx] + jnp.stack([grads_by_layer[layer_idx][slot_idx] for layer_idx in range(LAYERS)]) for slot_idx in range(9)))
        return (updated, (stream.astype(jnp.bfloat16), grad_stream))
    zero_grads = tuple((jnp.zeros(member_w.shape, jnp.float32) for member_w in stacked))
    blocks_in = (tokens.reshape(-1, TOK_DEV, D), lengths, cotangent.reshape(-1, TOK_DEV, D))
    running, (block_outs, block_grads) = lax.scan(one_block, zero_grads, blocks_in)
    return (block_outs.reshape(-1, D), block_grads.reshape(-1, D), running[0], running[1], running[2], running[3], running[4], running[5], running[6], running[7], running[8])
```

```python
from functools import partial

import jax
import jax.numpy as jnp
from jax import lax
from jax.sharding import PartitionSpec as P

HD = 96
LAYERS = 1


EPSILON = 1e-05
ROPE_BASE = 100000.0
NEG_FILL = -1e30


def layout(seq_lengths, rows_here):
    seg_ends = jnp.cumsum(seq_lengths)
    seg_starts = seg_ends - seq_lengths
    positions = jnp.arange(rows_here, dtype=jnp.int32)
    segment = jnp.sum((positions[:, None] >= seg_ends[None, :]).astype(jnp.int32), axis=1)
    member = segment[:, None] == jnp.arange(seq_lengths.shape[0], dtype=jnp.int32)[None, :]
    offset = jnp.sum(jnp.where(member, seg_starts[None, :], 0), axis=1)
    where_in = positions - offset
    allowed = (segment[:, None] == segment[None, :]) & (positions[None, :] <= positions[:, None])
    half_dim = HD // 2
    frequency = ROPE_BASE ** (-jnp.arange(half_dim, dtype=jnp.float32) / half_dim)
    angles = where_in.astype(jnp.float32)[:, None] * frequency[None, :]
    return (allowed, jnp.cos(angles), jnp.sin(angles))


def rotate(values, cosine, sine_tab, sign_flip):
    half_dim = values.shape[-1] // 2
    front_half = values[..., :half_dim]
    back_half = values[..., half_dim:]
    cos_part = cosine[:, None, :]
    sin_part = sign_flip * sine_tab[:, None, :]
    return jnp.concatenate(
        [
            front_half * cos_part - back_half * sin_part,
            back_half * cos_part + front_half * sin_part,
        ],
        axis=-1,
    )


def rms_scale(stream):
    return lax.rsqrt(jnp.mean(stream * stream, axis=-1, keepdims=True) + EPSILON)


def matmul(left, right):
    return jnp.dot(left, right, preferred_element_type=jnp.float32)


def inner_rows(left, right):
    return lax.dot_general(
        left, right, (((0,), (0,)), ((), ())), preferred_element_type=jnp.float32
    )


def times_transposed(left, right):
    return lax.dot_general(
        left, right, (((1,), (1,)), ((), ())), preferred_element_type=jnp.float32
    )


def attend(queries, keys_rot, values_in, allowed):
    rows_here = queries.shape[0]
    kv_heads = keys_rot.shape[1]
    grouped = queries.reshape(rows_here, kv_heads, queries.shape[1] // kv_heads, HD)
    scores = jnp.einsum(
        "qkgd,skd->kgqs", grouped, keys_rot, preferred_element_type=jnp.float32
    ) * HD ** (-0.5)
    scores = jnp.where(allowed[None, None], scores, NEG_FILL)
    row_top = jnp.max(scores, axis=-1, keepdims=True)
    log_total = row_top + jnp.log(jnp.sum(jnp.exp(scores - row_top), axis=-1, keepdims=True))
    attn_probs = jnp.where(allowed[None, None], jnp.exp(scores - log_total), 0.0)
    probs_low = attn_probs.astype(jnp.bfloat16)
    attn_mixed = jnp.einsum(
        "kgqs,skd->qkgd", probs_low, values_in, preferred_element_type=jnp.float32
    )
    return (attn_probs, attn_mixed.reshape(rows_here, queries.shape[1] * HD).astype(jnp.bfloat16))


def attend_back(queries, keys_rot, values_in, attn_probs, attn_mixed, grad_mixed):
    rows_here = queries.shape[0]
    kv_heads = keys_rot.shape[1]
    groups = queries.shape[1] // kv_heads
    grouped = queries.reshape(rows_here, kv_heads, groups, HD)
    grad_grouped = grad_mixed.reshape(rows_here, kv_heads, groups, HD)
    mixed_grouped = attn_mixed.reshape(rows_here, kv_heads, groups, HD)
    delta = jnp.sum(grad_grouped.astype(jnp.float32) * mixed_grouped.astype(jnp.float32), axis=-1)
    delta = jnp.transpose(delta, (1, 2, 0))[..., None]
    grad_probs = jnp.einsum(
        "qkgd,skd->kgqs", grad_grouped, values_in, preferred_element_type=jnp.float32
    )
    grad_score = (attn_probs * (grad_probs - delta) * HD ** (-0.5)).astype(jnp.bfloat16)
    probs_low = attn_probs.astype(jnp.bfloat16)
    grad_q = jnp.einsum(
        "kgqs,skd->qkgd", grad_score, keys_rot, preferred_element_type=jnp.float32
    ).reshape(rows_here, queries.shape[1], HD)
    grad_k = jnp.einsum("kgqs,qkgd->skd", grad_score, grouped, preferred_element_type=jnp.float32)
    grad_v = jnp.einsum(
        "kgqs,qkgd->skd", probs_low, grad_grouped, preferred_element_type=jnp.float32
    )
    return (grad_q, grad_k, grad_v)


def by_blocks(array_in, count):
    return array_in.reshape((count, array_in.shape[0] // count) + array_in.shape[1:])


def from_blocks(array_in):
    return array_in.reshape((array_in.shape[0] * array_in.shape[1],) + array_in.shape[2:])


def attend_blocks(queries, keys_rot, values_in, allowed):
    count = allowed.shape[0]
    attn_probs, attn_mixed = jax.vmap(attend)(
        by_blocks(queries, count), by_blocks(keys_rot, count), by_blocks(values_in, count), allowed
    )
    return (attn_probs, from_blocks(attn_mixed))


def attend_back_blocks(queries, keys_rot, values_in, attn_probs, attn_mixed, grad_mixed):
    count = attn_probs.shape[0]
    grad_q, grad_k, grad_v = jax.vmap(attend_back)(
        by_blocks(queries, count),
        by_blocks(keys_rot, count),
        by_blocks(values_in, count),
        attn_probs,
        by_blocks(attn_mixed, count),
        by_blocks(grad_mixed, count),
    )
    return (from_blocks(grad_q), from_blocks(grad_k), from_blocks(grad_v))


def layer_forward(stream, weights, allowed, cosine, sine_tab, spread, settle):
    attn_gain, w_query, w_key, w_value, w_out, mlp_gain, w_gate, w_up, w_down = weights
    scale_one = rms_scale(stream)
    normed_one = stream * scale_one
    attn_in = spread((normed_one * attn_gain.astype(jnp.float32)).astype(jnp.bfloat16))
    rows_here = attn_in.shape[0]
    queries = rotate(
        matmul(attn_in, w_query).reshape(rows_here, w_query.shape[1] // HD, HD),
        cosine,
        sine_tab,
        1.0,
    ).astype(jnp.bfloat16)
    keys_rot = rotate(
        matmul(attn_in, w_key).reshape(rows_here, w_key.shape[1] // HD, HD), cosine, sine_tab, 1.0
    ).astype(jnp.bfloat16)
    values_in = (
        matmul(attn_in, w_value).reshape(rows_here, w_value.shape[1] // HD, HD).astype(jnp.bfloat16)
    )
    attn_probs, attn_mixed = attend_blocks(queries, keys_rot, values_in, allowed)
    middle = stream + settle(matmul(attn_mixed, w_out))
    scale_two = rms_scale(middle)
    normed_two = middle * scale_two
    mlp_in = spread((normed_two * mlp_gain.astype(jnp.float32)).astype(jnp.bfloat16))
    gate_act = matmul(mlp_in, w_gate)
    up_act = matmul(mlp_in, w_up)
    hidden = (jax.nn.silu(gate_act) * up_act).astype(jnp.bfloat16)
    result = middle + settle(matmul(hidden, w_down))
    kept_state = (
        scale_one,
        normed_one,
        attn_in,
        queries,
        keys_rot,
        values_in,
        attn_probs,
        attn_mixed,
        scale_two,
        normed_two,
        mlp_in,
        gate_act,
        up_act,
        hidden,
    )
    return (result, kept_state)


def layer_backward(stream, weights, allowed, cosine, sine_tab, grad_stream, spread, settle):
    attn_gain, w_query, w_key, w_value, w_out, mlp_gain, w_gate, w_up, w_down = weights
    _, kept_state = layer_forward(stream, weights, allowed, cosine, sine_tab, spread, settle)
    (
        scale_one,
        normed_one,
        attn_in,
        queries,
        keys_rot,
        values_in,
        attn_probs,
        attn_mixed,
        scale_two,
        normed_two,
        mlp_in,
        gate_act,
        up_act,
        hidden,
    ) = kept_state
    rows_here = attn_in.shape[0]
    grad_low = spread(grad_stream.astype(jnp.bfloat16))
    grad_down = inner_rows(hidden, grad_low)
    grad_hidden = times_transposed(grad_low, w_down)
    sigmoid_gate = jax.nn.sigmoid(gate_act)
    grad_up_act = (grad_hidden * gate_act * sigmoid_gate).astype(jnp.bfloat16)
    grad_gate_act = (
        grad_hidden * up_act * sigmoid_gate * (1.0 + gate_act * (1.0 - sigmoid_gate))
    ).astype(jnp.bfloat16)
    grad_gate = inner_rows(mlp_in, grad_gate_act)
    grad_up = inner_rows(mlp_in, grad_up_act)
    grad_mlp_in = settle(
        times_transposed(grad_gate_act, w_gate) + times_transposed(grad_up_act, w_up)
    )
    grad_mlp_gain = jnp.sum(grad_mlp_in * normed_two, axis=0)
    grad_normed = grad_mlp_in * mlp_gain.astype(jnp.float32)
    grad_middle = grad_stream + scale_two * (
        grad_normed - normed_two * jnp.mean(grad_normed * normed_two, axis=-1, keepdims=True)
    )
    grad_middle_low = spread(grad_middle.astype(jnp.bfloat16))
    grad_out = inner_rows(attn_mixed, grad_middle_low)
    grad_mixed = times_transposed(grad_middle_low, w_out).astype(jnp.bfloat16)
    grad_q, grad_k, grad_v = attend_back_blocks(
        queries, keys_rot, values_in, attn_probs, attn_mixed, grad_mixed
    )
    grad_q = (
        rotate(grad_q, cosine, sine_tab, -1.0)
        .reshape(rows_here, w_query.shape[1])
        .astype(jnp.bfloat16)
    )
    grad_k = (
        rotate(grad_k, cosine, sine_tab, -1.0)
        .reshape(rows_here, w_key.shape[1])
        .astype(jnp.bfloat16)
    )
    grad_v = grad_v.reshape(rows_here, w_value.shape[1]).astype(jnp.bfloat16)
    grad_query = inner_rows(attn_in, grad_q)
    grad_key = inner_rows(attn_in, grad_k)
    grad_value = inner_rows(attn_in, grad_v)
    grad_attn_in = settle(
        times_transposed(grad_q, w_query)
        + times_transposed(grad_k, w_key)
        + times_transposed(grad_v, w_value)
    )
    grad_attn_gain = jnp.sum(grad_attn_in * normed_one, axis=0)
    grad_normed_one = grad_attn_in * attn_gain.astype(jnp.float32)
    grad_input = grad_middle + scale_one * (
        grad_normed_one
        - normed_one * jnp.mean(grad_normed_one * normed_one, axis=-1, keepdims=True)
    )
    return (
        grad_input,
        (
            grad_attn_gain,
            grad_query,
            grad_key,
            grad_value,
            grad_out,
            grad_mlp_gain,
            grad_gate,
            grad_up,
            grad_down,
        ),
    )


def fetch_fsdp(shards, layer_idx):
    return (
        lax.all_gather(shards[1][layer_idx], "fsdp", axis=0, tiled=True),
        lax.all_gather(shards[2][layer_idx], "fsdp", axis=0, tiled=True),
        lax.all_gather(shards[3][layer_idx], "fsdp", axis=0, tiled=True),
        lax.all_gather(shards[4][layer_idx], "fsdp", axis=1, tiled=True),
        lax.all_gather(shards[6][layer_idx], "fsdp", axis=0, tiled=True),
        lax.all_gather(shards[7][layer_idx], "fsdp", axis=0, tiled=True),
        lax.all_gather(shards[8][layer_idx], "fsdp", axis=1, tiled=True),
        lax.all_gather(shards[0][layer_idx], "fsdp", axis=0, tiled=True),
        lax.all_gather(shards[5][layer_idx], "fsdp", axis=0, tiled=True),
    )


def fetch_fsdp_back(shards, layer_idx):
    return (
        lax.all_gather(shards[1][layer_idx], "fsdp", axis=0, tiled=True),
        lax.all_gather(shards[2][layer_idx], "fsdp", axis=0, tiled=True),
        lax.all_gather(shards[3][layer_idx], "fsdp", axis=0, tiled=True),
        lax.all_gather(shards[4][layer_idx], "fsdp", axis=1, tiled=True),
        lax.all_gather(shards[6][layer_idx], "fsdp", axis=0, tiled=True),
        lax.all_gather(shards[7][layer_idx], "fsdp", axis=0, tiled=True),
        lax.all_gather(shards[8][layer_idx], "fsdp", axis=1, tiled=True),
        lax.all_gather(shards[0][layer_idx], "fsdp", axis=0, tiled=True),
        lax.all_gather(shards[5][layer_idx], "fsdp", axis=0, tiled=True),
    )


def arrange(matrices, pieces):
    return (
        pieces[7],
        matrices[0],
        matrices[1],
        matrices[2],
        matrices[3],
        pieces[8],
        matrices[4],
        matrices[5],
        matrices[6],
    )


def body(
    tokens,
    lengths,
    cotangent,
    attn_gain,
    w_query,
    w_key,
    w_value,
    w_out,
    mlp_gain,
    w_gate,
    w_up,
    w_down,
):
    shards = (attn_gain, w_query, w_key, w_value, w_out, mlp_gain, w_gate, w_up, w_down)

    def spread(rows_in):
        return lax.all_gather(rows_in, "dp", axis=0, tiled=True)

    def settle(terms_in):
        return lax.psum_scatter(
            terms_in.astype(jnp.bfloat16), "dp", scatter_dimension=0, tiled=True
        ).astype(jnp.float32)

    allowed, cosine, sine_tab = jax.vmap(partial(layout, rows_here=tokens.shape[0]))(lengths)
    cosine = from_blocks(cosine)
    sine_tab = from_blocks(sine_tab)
    stream = tokens.astype(jnp.float32)
    weights_kept = []
    layer_idx = 0
    pieces = fetch_fsdp(shards, layer_idx)
    weights = arrange(pieces[:7], pieces)
    weights_kept.append(weights)
    inputs_kept = [stream]
    stream, _ = layer_forward(stream, weights, allowed, cosine, sine_tab, spread, settle)
    output = stream.astype(jnp.bfloat16)
    grad_stream = cotangent.astype(jnp.float32)
    grads_by_layer = [None] * LAYERS
    for layer_idx in reversed(range(LAYERS)):
        weights = weights_kept[layer_idx]
        grad_stream, terms = layer_backward(
            inputs_kept[layer_idx], weights, allowed, cosine, sine_tab, grad_stream, spread, settle
        )
        gains = lax.psum((terms[0], terms[5]), "dp")
        owned = (
            lax.psum_scatter(
                terms[1].astype(jnp.bfloat16),
                "fsdp",
                scatter_dimension=0,
                tiled=True,
            ).astype(jnp.float32),
            lax.psum_scatter(
                terms[2].astype(jnp.bfloat16),
                "fsdp",
                scatter_dimension=0,
                tiled=True,
            ).astype(jnp.float32),
            lax.psum_scatter(
                terms[3].astype(jnp.bfloat16),
                "fsdp",
                scatter_dimension=0,
                tiled=True,
            ).astype(jnp.float32),
            lax.psum_scatter(
                terms[4].astype(jnp.bfloat16),
                "fsdp",
                scatter_dimension=1,
                tiled=True,
            ).astype(jnp.float32),
            lax.psum_scatter(
                terms[6].astype(jnp.bfloat16),
                "fsdp",
                scatter_dimension=0,
                tiled=True,
            ).astype(jnp.float32),
            lax.psum_scatter(
                terms[7].astype(jnp.bfloat16),
                "fsdp",
                scatter_dimension=0,
                tiled=True,
            ).astype(jnp.float32),
            lax.psum_scatter(
                terms[8].astype(jnp.bfloat16),
                "fsdp",
                scatter_dimension=1,
                tiled=True,
            ).astype(jnp.float32),
            lax.psum_scatter(
                gains[0].astype(jnp.bfloat16), "fsdp", scatter_dimension=0, tiled=True
            ).astype(jnp.float32),
            lax.psum_scatter(
                gains[1].astype(jnp.bfloat16), "fsdp", scatter_dimension=0, tiled=True
            ).astype(jnp.float32),
        )
        grads_by_layer[layer_idx] = arrange(owned, owned)
    stacked = tuple((jnp.stack([grads_by_layer[0][slot_idx]]) for slot_idx in range(9)))
    return (output, grad_stream) + stacked


def solution(mesh):
    placed = (
        P(("fsdp", "dp"), None),
        P("fsdp", None),
        P(("fsdp", "dp"), None),
        P(None, "fsdp"),
        P(None, "fsdp", "dp"),
        P(None, "fsdp", "dp"),
        P(None, "fsdp", "dp"),
        P(None, "dp", "fsdp"),
        P(None, "fsdp"),
        P(None, "fsdp", "dp"),
        P(None, "fsdp", "dp"),
        P(None, "dp", "fsdp"),
    )
    return jax.shard_map(
        body,
        mesh=mesh,
        in_specs=placed,
        out_specs=(
            P(("fsdp", "dp"), None),
            P(("fsdp", "dp"), None),
            P(None, "fsdp"),
            P(None, "fsdp", "dp"),
            P(None, "fsdp", "dp"),
            P(None, "fsdp", "dp"),
            P(None, "dp", "fsdp"),
            P(None, "fsdp"),
            P(None, "fsdp", "dp"),
            P(None, "fsdp", "dp"),
            P(None, "dp", "fsdp"),
        ),
        check_vma=False,
    )
```

```python
from functools import partial

import jax
import jax.numpy as jnp
from jax import lax
from jax.experimental import pallas as pl
from jax.experimental.pallas import tpu as pltpu
from jax.sharding import PartitionSpec as P

HD = 96
HALF = 48
LANES = 128
EPSILON = 1e-05
ROPE_BASE = 100000.0
NEG_FILL = -1e30
MESH = pl.DeviceIdType.MESH
BF = jnp.bfloat16
F32 = jnp.float32
TILE = 256
CHUNK = 32


def mm(left, right):
    return jnp.dot(left, right, preferred_element_type=F32)


def mm_nt(left, right):
    return lax.dot_general(left, right, (((1,), (1,)), ((), ())), preferred_element_type=F32)


def mm_tn(left, right):
    return lax.dot_general(left, right, (((0,), (0,)), ((), ())), preferred_element_type=F32)


def loop(count, body):
    def step(index, carry):
        body(index)
        return carry

    lax.fori_loop(0, count, step, 0)


def flip(chip, bits):
    other, bit = chip, 1
    while bit <= bits:
        if bits & bit:
            other = other + bit * (1 - 2 * ((chip // bit) % 2))
        bit *= 2
    return other


def layer_kernel(dims, *refs):
    n, chips, rows, width, nq, nkv, ff, nseq = dims
    nf = 2 * chips
    shard = width // nf
    total = n * rows
    widths = (nq * LANES + 2 * nkv * LANES, nq * LANES, ff, ff, ff)
    refs = list(refs)

    def take(count):
        taken = refs[:count]
        del refs[:count]
        return taken

    (lengths, freq, tokens, cot, gains_in) = take(5)
    srcs = take(5)
    (out_ref, gtok_ref, gains_out) = take(3)
    gouts = take(5)
    landing = take(5)
    weights = take(5)
    (x_buf, ct_buf, mi_buf, gm_buf) = take(4)
    (qkv, gqkv, probs, mixed, gmixed, hid, gg, gu) = take(8)
    (t_one, t_two) = take(2)
    (s_buf, r_buf, p_zero, p_one, middle, gmid) = take(6)
    (sc_one, sc_two, cos_t, sin_t) = take(4)
    (gain_in, gain_row, gain_z, gain_f, stage) = take(5)
    send_b = take(1)[0]
    sums = take(5)
    from_partner = take(5)
    (w_ss, w_fs, w_rs, w_ls) = take(4)
    (z_ss, z_rs) = take(2)
    (rs_ss, rs_rs) = take(2)
    (b_ss, b_rs, i_ss, i_rs, l_sem) = take(5)

    f = lax.axis_index("fsdp")
    d = lax.axis_index("dp")
    p = f // 2
    c = f % 2

    def at_f(index):
        return {"fsdp": index, "dp": d}

    def at_d(index):
        return {"fsdp": f, "dp": index}

    partner = p * 2 + 1 - c

    def remote(src, dst, ss, rs, where):
        return pltpu.make_async_remote_copy(
            src_ref=src, dst_ref=dst, send_sem=ss, recv_sem=rs, device_id=where, device_id_type=MESH
        )

    def block(ref, index, size=rows):
        return ref.at[pl.ds(pl.multiple_of(index * size, size), size)]

    def cols(index, size=TILE):
        return pl.ds(pl.multiple_of(index * size, size), size)

    barrier = pltpu.get_barrier_semaphore()
    for k in range(1, chips):
        pl.semaphore_signal(
            barrier, inc=1, device_id=at_f(flip(p, k) * 2 + c), device_id_type=MESH
        )
    pl.semaphore_signal(barrier, inc=1, device_id=at_f(partner), device_id_type=MESH)

    @pl.when(d > 0)
    def _():
        pl.semaphore_signal(barrier, inc=1, device_id=at_d(d - 1), device_id_type=MESH)

    @pl.when(d < n - 1)
    def _():
        pl.semaphore_signal(barrier, inc=1, device_id=at_d(d + 1), device_id_type=MESH)

    ends = (d == 0).astype(jnp.int32) + (d == n - 1).astype(jnp.int32)
    pl.semaphore_wait(barrier, chips + 2 - ends)

    class Gather:
        def __init__(self, slot, src, dst, size):
            self.slot, self.src, self.dst, self.size = slot, src, dst, size

        def part(self, index):
            return block(self.dst, index, self.size)

        def direct(self, k):
            where = partner if k == 0 else flip(p, k) * 2 + c
            return remote(
                self.src, self.part(f), w_ss.at[self.slot, k], w_rs.at[self.slot, f], at_f(where)
            )

        def onward(self, k):
            index = flip(p, k) * 2 + c
            return remote(
                self.part(index),
                self.part(index),
                w_fs.at[self.slot, k],
                w_rs.at[self.slot, index],
                at_f(partner),
            )

        def own(self):
            return pltpu.make_async_copy(self.src, self.part(f), w_ls.at[self.slot])

        def start(self):
            for k in list(range(1, chips)) + [0]:
                self.direct(k).start()
            self.own().start()

        def forward(self):
            for k in range(1, chips):
                copy = self.onward(k)
                copy.wait_recv()
                copy.start()

        def finish(self):
            for k in range(chips):
                index = flip(p, k) * 2 + 1 - c
                remote(
                    self.part(index),
                    self.part(index),
                    w_fs.at[self.slot, k],
                    w_rs.at[self.slot, index],
                    at_f(partner),
                ).wait_recv()
            self.own().wait()

        def drain(self):
            for k in range(chips):
                self.direct(k).wait_send()
            for k in range(1, chips):
                self.onward(k).wait_send()

    class Line:
        def __init__(self, slot, buf, size=rows, src=None):
            self.slot, self.buf, self.size, self.src = slot, buf, size, src

        def copy(self, index, side, own=False):
            part = block(self.buf, index, self.size)
            src = self.src if own and self.src is not None else part
            where = d + 1 if side == 0 else d - 1
            return remote(
                src, part, z_ss.at[self.slot, side, index], z_rs.at[self.slot, index], at_d(where)
            )

        def start(self):
            @pl.when(d < n - 1)
            def _():
                self.copy(d, 0, True).start()

            @pl.when(d > 0)
            def _():
                self.copy(d, 1, True).start()

        def step(self, s):
            @pl.when(d - s >= 0)
            def _():
                copy = self.copy(d - s, 0)
                copy.wait_recv()

                @pl.when(d < n - 1)
                def _():
                    copy.start()

            @pl.when(d + s < n)
            def _():
                copy = self.copy(d + s, 1)
                copy.wait_recv()

                @pl.when(d > 0)
                def _():
                    copy.start()

        def drain(self):
            for j in range(n):

                @pl.when((j <= d) & (d < n - 1))
                def _():
                    self.copy(j, 0).wait_send()

                @pl.when((j >= d) & (d > 0))
                def _():
                    self.copy(j, 1).wait_send()

    class Reduce:
        def __init__(self, slot, partial_of, sends, gets):
            self.slot, self.partial_of, self.sends, self.gets = slot, partial_of, sends, gets

        def copy(self, index, where, slot):
            return remote(
                block(self.sends, index),
                block(self.gets, slot),
                rs_ss.at[self.slot, index],
                rs_rs.at[self.slot, slot],
                at_d(where),
            )

        def got(self, slot):
            remote(
                block(self.gets, slot),
                block(self.gets, slot),
                rs_ss.at[self.slot, 0],
                rs_rs.at[self.slot, slot],
                at_d(d),
            ).wait_recv()

        def combine(self, acc, index, has_more):
            send, get = block(self.sends, index), block(self.gets, index)

            @pl.when(has_more)
            def _():
                self.got(index)

                def rows_of(i):
                    r = pl.ds(pl.multiple_of(i * CHUNK, CHUNK), CHUNK)
                    send[r, :] = (acc[r, :] + get[r, :].astype(F32)).astype(BF)

                loop(rows // CHUNK, rows_of)

            @pl.when(jnp.logical_not(has_more))
            def _():
                def rows_of(i):
                    r = pl.ds(pl.multiple_of(i * CHUNK, CHUNK), CHUNK)
                    send[r, :] = acc[r, :].astype(BF)

                loop(rows // CHUNK, rows_of)

        def step(self, s):
            right, left = d + s, d - s

            @pl.when(right < n)
            def _():
                self.partial_of(right, p_zero)

            @pl.when(left >= 0)
            def _():
                self.partial_of(left, p_one)

            @pl.when(right < n)
            def _():
                self.combine(p_zero, right, d > 0)
                self.copy(right, d + 1, right).start()

            @pl.when(left >= 0)
            def _():
                self.combine(p_one, left, d < n - 1)
                self.copy(left, d - 1, n if s == 1 else left).start()

        def final(self):
            self.partial_of(d, p_zero)

            def add(slot):
                self.got(slot)
                get = block(self.gets, slot)

                def rows_of(i):
                    r = pl.ds(pl.multiple_of(i * CHUNK, CHUNK), CHUNK)
                    p_zero[r, :] = p_zero[r, :] + get[r, :].astype(F32)

                loop(rows // CHUNK, rows_of)

            @pl.when(d > 0)
            def _():
                add(d)

            @pl.when(d < n - 1)
            def _():
                add(n)

        def drain(self):
            for j in range(n):

                @pl.when(d != j)
                def _():
                    self.copy(j, d, j).wait_send()

    class Grad:
        def __init__(self, group, turned, terms):
            self.group, self.turned, self.terms = group, turned, terms
            self.width = widths[group]

        def rows_for(self, index):
            return pl.ds(pl.multiple_of(index * shard, shard), shard)

        def hand_over(self, k):
            chip = flip(p, k)
            return remote(
                send_b.at[k, :, pl.ds(0, self.width)],
                from_partner[self.group].at[chip],
                b_ss.at[self.group, k],
                b_rs.at[self.group, chip],
                at_f(partner),
            )

        def ship(self, k):
            chip = flip(p, k)
            return remote(
                sums[self.group].at[chip],
                landing[self.group].at[k - 1],
                i_ss.at[self.group, k - 1],
                i_rs.at[self.group, k - 1],
                at_f(chip * 2 + c),
            )

        def send(self, k):
            left = self.turned.at[self.rows_for(flip(p, k) * 2 + 1 - c)]

            def tile(t):
                send_b[k, :, cols(t)] = mm(left[...], self.terms[:, cols(t)]).astype(BF)

            loop(self.width // TILE, tile)
            self.hand_over(k).start()

        def own(self, k):
            chip = flip(p, k)
            left = self.turned.at[self.rows_for(chip * 2 + c)]
            remote(
                from_partner[self.group].at[chip],
                from_partner[self.group].at[chip],
                b_ss.at[self.group, k],
                b_rs.at[self.group, chip],
                at_f(partner),
            ).wait_recv()

            def tile(t):
                term = mm(left[...], self.terms[:, cols(t)])
                other = from_partner[self.group][chip, :, cols(t)].astype(F32)
                sums[self.group][chip, :, cols(t)] = (term + other).astype(BF)

            loop(self.width // TILE, tile)
            if k > 0:
                self.ship(k).start()

        def send_all(self):
            for k in list(range(1, chips)) + [0]:
                self.send(k)

        def own_all(self):
            for k in list(range(1, chips)) + [0]:
                self.own(k)
            for k in range(chips):
                self.hand_over(k).wait_send()

        def fetch(self, k):
            return pltpu.make_async_copy(
                landing[self.group].at[k - 1],
                stage.at[k - 1, :, pl.ds(0, self.width)],
                l_sem.at[k - 1],
            )

        def finish(self):
            for k in range(1, chips):
                self.ship(k).wait()
                self.fetch(k).start()
            for k in range(1, chips):
                self.fetch(k).wait()
            out = gouts[self.group]

            def tile(t):
                acc = sums[self.group][p, :, cols(t)].astype(F32)
                for k in range(1, chips):
                    acc = acc + stage[k - 1, :, cols(t)].astype(F32)
                out[:, cols(t)] = acc

            loop(self.width // TILE, tile)

    def row_blocks(body):
        loop(rows // CHUNK, lambda i: body(pl.ds(pl.multiple_of(i * CHUNK, CHUNK), CHUNK)))

    def turn(src, dst):
        def lane_block(t):
            dst[cols(t, LANES), :] = src[pl.ds(0, total), cols(t, LANES)].T

        loop(width // LANES, lane_block)

    gathers = [Gather(g, srcs[g], weights[g], shard) for g in range(5)]
    gain_gather = Gather(5, gains_in, gain_in, 8)
    tok_line = Line(0, x_buf, src=tokens)
    cot_line = Line(1, ct_buf, src=cot)
    mi_line = Line(2, mi_buf)
    gm_line = Line(3, gm_buf)
    gain_line = Line(4, gain_z, 8)

    tok_line.start()
    gathers[0].start()
    gain_gather.start()
    for g in range(1, 5):
        gathers[g].start()
    block(x_buf, d)[...] = tokens[...]
    block(ct_buf, d)[...] = cot[...]

    def segments(b, shape, dim):
        index = lax.broadcasted_iota(jnp.int32, shape, dim)
        segment = jnp.zeros(shape, jnp.int32)
        offset = jnp.zeros(shape, jnp.int32)
        end = jnp.int32(0)
        for k in range(nseq):
            end = end + lengths[b, k]
            past = index >= end
            segment = segment + past.astype(jnp.int32)
            offset = jnp.where(past, end, offset)
        return index, segment, offset

    def tables(b):
        index, _, offset = segments(b, (rows, LANES), 0)
        angle = (index - offset).astype(F32) * freq[...]
        lane = lax.broadcasted_iota(jnp.int32, (rows, LANES), 1)
        sine = jnp.sin(angle)
        block(cos_t, b)[...] = jnp.cos(angle)
        block(sin_t, b)[...] = jnp.where(lane < LANES // 2, -sine, sine)

    loop(n, tables)
    tok_line.step(1)
    gathers[0].forward()
    gain_gather.forward()
    for s in range(2, n):
        tok_line.step(s)
    cot_line.start()
    gathers[0].finish()
    gain_gather.finish()

    gain_row[...] = gain_in[pl.ds(0, 8), :]
    for k in range(1, nf):
        gain_row[...] = gain_row[...] + gain_in[pl.ds(8 * k, 8), :]

    def rms(value):
        mean = jnp.sum(value * value, axis=-1, keepdims=True) / width
        return lax.rsqrt(mean + EPSILON)

    def norm_one(i):
        r = pl.ds(pl.multiple_of(i * CHUNK, CHUNK), CHUNK)
        value = x_buf[r, :].astype(F32)
        scale = rms(value)
        sc_one[r, :] = scale
        mi_buf[r, :] = (value * scale * gain_row[0:1, :]).astype(BF)

    loop(total // CHUNK, norm_one)

    def rope(value, sign, cos_v, sin_v):
        return value * cos_v + sign * (pltpu.roll(value, LANES // 2, 1) * sin_v)

    heads = nq + 2 * nkv
    half_rows = min(total, 2 * rows)

    def qkv_rows(m):
        r = pl.ds(pl.multiple_of(m * half_rows, half_rows), half_rows)
        cos_v, sin_v = cos_t[r, :], sin_t[r, :]
        for t in range(heads // 2):
            both = mm(mi_buf[r, :], weights[0][:, 2 * t * LANES : 2 * (t + 1) * LANES])
            for h in (2 * t, 2 * t + 1):
                value = both[:, (h - 2 * t) * LANES : (h - 2 * t + 1) * LANES]
                if h < nq + nkv:
                    value = rope(value, 1.0, cos_v, sin_v)
                qkv[r, h * LANES : (h + 1) * LANES] = value.astype(BF)

    loop(total // half_rows, qkv_rows)
    gathers[1].forward()

    def head(ref, r, h):
        return ref[r, h * LANES : (h + 1) * LANES]

    def attend(b):
        r = pl.ds(pl.multiple_of(b * rows, rows), rows)
        t_index, t_seg, _ = segments(b, (rows, rows), 0)
        s_index, s_seg, _ = segments(b, (rows, rows), 1)
        allowed = (t_seg == s_seg) & (s_index <= t_index)
        for h in range(nq):
            kv = h // (nq // nkv)
            score = mm_nt(head(qkv, r, h), head(qkv, r, nq + kv)) * HD ** (-0.5)
            score = jnp.where(allowed, score, NEG_FILL)
            top = jnp.max(score, axis=-1, keepdims=True)
            log_total = top + jnp.log(jnp.sum(jnp.exp(score - top), axis=-1, keepdims=True))
            prob = jnp.where(allowed, jnp.exp(score - log_total), 0.0)
            probs[b * nq + h] = prob
            mixed[r, h * LANES : (h + 1) * LANES] = mm(
                prob.astype(BF), head(qkv, r, nq + nkv + kv)
            ).astype(BF)

    loop(n, attend)
    cot_line.step(1)
    gathers[1].finish()

    def by_turned(pairs):
        def partial_of(j, acc):
            r = pl.ds(pl.multiple_of(j * rows, rows), rows)

            def tile(t):
                value = None
                for left, weight in pairs:
                    term = mm_nt(left[r, :], weight[cols(t), :])
                    value = term if value is None else value + term
                acc[:, cols(t)] = value

            loop(width // TILE, tile)

        return partial_of

    after_attn = Reduce(0, by_turned([(mixed, weights[1])]), s_buf, r_buf)
    extra = [
        lambda: gathers[2].forward(),
        lambda: gathers[3].forward(),
    ]
    for s in range(n - 1, 0, -1):
        after_attn.step(s)
        if 2 <= n - s + 1 < n:
            cot_line.step(n - s + 1)
        if extra:
            extra.pop(0)()
    for todo in extra:
        todo()
    after_attn.final()

    own_rows = d * rows

    def norm_two(i):
        r = pl.ds(pl.multiple_of(i * CHUNK, CHUNK), CHUNK)
        value = tokens[r, :].astype(F32) + p_zero[r, :]
        scale = rms(value)
        middle[r, :] = value
        sc_two[r, :] = scale
        here = pl.ds(pl.multiple_of(own_rows + i * CHUNK, CHUNK), CHUNK)
        mi_buf[here, :] = (value * scale * gain_row[1:2, :]).astype(BF)

    loop(rows // CHUNK, norm_two)
    mi_line.start()
    mi_line.step(1)
    gathers[4].forward()
    cot_line.drain()
    turn(ct_buf, t_one)
    for s in range(2, n):
        mi_line.step(s)
    for g in (2, 3, 4):
        gathers[g].finish()
    after_attn.drain()

    tiles_ff = ff // TILE

    def feed(index):
        m, t = index // tiles_ff, index % tiles_ff
        r = pl.ds(pl.multiple_of(m * half_rows, half_rows), half_rows)
        left = mi_buf[r, :]
        gate = mm(left, weights[2][:, cols(t)])
        up = mm(left, weights[3][:, cols(t)])
        grad_hidden = mm(ct_buf[r, :], weights[4][:, cols(t)])
        sig = 1.0 / (1.0 + jnp.exp(-gate))
        hid[r, cols(t)] = (gate * sig * up).astype(BF)
        gu[r, cols(t)] = (grad_hidden * gate * sig).astype(BF)
        gg[r, cols(t)] = (grad_hidden * up * sig * (1.0 + gate * (1.0 - sig))).astype(BF)

    loop((total // half_rows) * tiles_ff, feed)
    mi_line.drain()
    turn(mi_buf, t_two)

    after_mlp = Reduce(1, by_turned([(gg, weights[2]), (gu, weights[3])]), s_buf, r_buf)
    down = Grad(4, t_one, hid)
    gate_g = Grad(2, t_two, gg)
    up_g = Grad(3, t_two, gu)
    work = [down.send_all, down.own_all, gate_g.send_all]
    for s in range(n - 1, 0, -1):
        after_mlp.step(s)
        if work:
            work.pop(0)()
    for todo in work:
        todo()
    after_mlp.final()

    def back_two(i):
        r = pl.ds(pl.multiple_of(i * CHUNK, CHUNK), CHUNK)
        term = p_zero[r, :]
        scale = sc_two[r, :]
        normed = middle[r, :] * scale
        gain_sum = jnp.sum(term * normed, axis=0, keepdims=True)
        dn = term * gain_row[1:2, :]
        mean = jnp.sum(dn * normed, axis=-1, keepdims=True) / width
        value = cot[r, :].astype(F32) + scale * (dn - normed * mean)
        gmid[r, :] = value
        here = pl.ds(pl.multiple_of(own_rows + i * CHUNK, CHUNK), CHUNK)
        gm_buf[here, :] = value.astype(BF)
        gain_own[1:2, :] = gain_own[1:2, :] + gain_sum

    gain_own = block(gain_z, d, 8)
    gain_own[...] = jnp.zeros((8, width), F32)
    loop(rows // CHUNK, back_two)
    gm_line.start()
    after_mlp.drain()

    output = Reduce(2, by_turned([(hid, weights[4])]), ct_buf, mi_buf)
    work = [gate_g.own_all, up_g.send_all, up_g.own_all]
    for s in range(1, n):
        output.step(n - s)
        gm_line.step(s)
        if work:
            work.pop(0)()
    for todo in work:
        todo()
    turn(gm_buf, t_one)

    def grad_mixed(index):
        tiles = widths[1] // TILE
        m, t = index // tiles, index % tiles
        r = pl.ds(pl.multiple_of(m * half_rows, half_rows), half_rows)
        gmixed[r, cols(t)] = mm(gm_buf[r, :], weights[1][:, cols(t)]).astype(BF)

    loop((total // half_rows) * (widths[1] // TILE), grad_mixed)

    def attend_back(b):
        r = pl.ds(pl.multiple_of(b * rows, rows), rows)
        cos_v, sin_v = cos_t[r, :], sin_t[r, :]
        group = nq // nkv
        for kv in range(nkv):
            key, val = head(qkv, r, nq + kv), head(qkv, r, nq + nkv + kv)
            grad_k = grad_v = None
            for h in range(kv * group, (kv + 1) * group):
                query, gm_h = head(qkv, r, h), head(gmixed, r, h)
                prob = probs[b * nq + h]
                delta = jnp.sum(
                    gm_h.astype(F32) * head(mixed, r, h).astype(F32), axis=-1, keepdims=True
                )
                grad_p = mm_nt(gm_h, val)
                grad_s = (prob * (grad_p - delta) * HD ** (-0.5)).astype(BF)
                grad_q = mm(grad_s, key)
                gqkv[r, h * LANES : (h + 1) * LANES] = rope(grad_q, -1.0, cos_v, sin_v).astype(BF)
                k_term, v_term = mm_tn(grad_s, query), mm_tn(prob.astype(BF), gm_h)
                grad_k = k_term if grad_k is None else grad_k + k_term
                grad_v = v_term if grad_v is None else grad_v + v_term
            k_at, v_at = (nq + kv) * LANES, (nq + nkv + kv) * LANES
            gqkv[r, k_at : k_at + LANES] = rope(grad_k, -1.0, cos_v, sin_v).astype(BF)
            gqkv[r, v_at : v_at + LANES] = grad_v.astype(BF)

    loop(n, attend_back)

    base_in = by_turned([(gqkv, weights[0])])

    def grad_in(j, acc):
        base_in(j, acc)

        def add_gain(i):
            r = pl.ds(pl.multiple_of(i * CHUNK, CHUNK), CHUNK)
            there = pl.ds(pl.multiple_of(j * rows + i * CHUNK, CHUNK), CHUNK)
            normed = x_buf[there, :].astype(F32) * sc_one[there, :]
            gain_own[0:1, :] = gain_own[0:1, :] + jnp.sum(
                acc[r, :] * normed, axis=0, keepdims=True
            )

        loop(rows // CHUNK, add_gain)

    after_in = Reduce(3, grad_in, s_buf, r_buf)
    out_g = Grad(1, t_one, mixed)
    qkv_g = Grad(0, t_two, gqkv)

    def turn_attn_in():
        def one(b):
            there = pl.ds(pl.multiple_of(b * rows, rows), rows)

            def lane_block(t):
                value = x_buf[there, cols(t, LANES)].astype(F32) * sc_one[there, :]
                value = (value * gain_row[0:1, cols(t, LANES)]).astype(BF)
                t_two[cols(t, LANES), cols(b, rows)] = value.T

            loop(width // LANES, lane_block)

        loop(n, one)

    work = [turn_attn_in, qkv_g.send_all, qkv_g.own_all]
    for s in range(n - 1, 0, -1):
        after_in.step(s)
        if work:
            work.pop(0)()
    for todo in work:
        todo()
    out_g.send_all()
    out_g.own_all()
    after_in.final()

    def back_one(i):
        r = pl.ds(pl.multiple_of(i * CHUNK, CHUNK), CHUNK)
        there = pl.ds(pl.multiple_of(own_rows + i * CHUNK, CHUNK), CHUNK)
        scale = sc_one[there, :]
        normed = tokens[r, :].astype(F32) * scale
        dm = p_zero[r, :] * gain_row[0:1, :]
        mean = jnp.sum(dm * normed, axis=-1, keepdims=True) / width
        gtok_ref[r, :] = gmid[r, :] + scale * (dm - normed * mean)

    loop(rows // CHUNK, back_one)
    gain_line.start()
    output.final()

    def write_out(i):
        r = pl.ds(pl.multiple_of(i * CHUNK, CHUNK), CHUNK)
        out_ref[r, :] = (middle[r, :] + p_zero[r, :]).astype(BF)

    loop(rows // CHUNK, write_out)
    for s in range(1, n):
        gain_line.step(s)
    gain_sum = gain_z[pl.ds(0, 8), :]
    for k in range(1, n):
        gain_sum = gain_sum + gain_z[pl.ds(8 * k, 8), :]
    gain_row[...] = gain_sum
    gain_back = Gather(6, gain_row, gain_f, 8)
    gain_back.start()
    gain_back.forward()
    for grad in (down, gate_g, up_g, qkv_g, out_g):
        grad.finish()
    gain_back.finish()
    gain_sum = gain_f[pl.ds(0, 8), :]
    for k in range(1, nf):
        gain_sum = gain_sum + gain_f[pl.ds(8 * k, 8), :]
    gains_out[...] = gain_sum

    output.drain()
    after_in.drain()
    for line in (tok_line, gm_line, gain_line):
        line.drain()
    for gather in gathers + [gain_gather, gain_back]:
        gather.drain()


def run_layer(lengths, freq, tokens, cot, gains, shards, sizes):
    n, chips, nq, nkv = sizes
    rows, width = tokens.shape
    total = n * rows
    nf = 2 * chips
    shard = shards[0].shape[0]
    ff = shards[2].shape[1]
    widths = tuple(s.shape[1] for s in shards)
    dims = (n, chips, rows, width, nq, nkv, ff, lengths.shape[1])
    vmem = pl.BlockSpec(memory_space=pltpu.VMEM)
    anywhere = pl.BlockSpec(memory_space=pl.ANY)
    out_shape = (
        [
            jax.ShapeDtypeStruct((rows, width), BF),
            jax.ShapeDtypeStruct((rows, width), F32),
            jax.ShapeDtypeStruct((8, width), F32),
        ]
        + [jax.ShapeDtypeStruct((shard, w), F32) for w in widths]
        + [jax.ShapeDtypeStruct((chips - 1, shard, w), BF) for w in widths]
    )
    widest = max(widths)
    scratch = (
        [pltpu.VMEM((width, w), BF) for w in widths]
        + [
            pltpu.VMEM((total, width), BF),
            pltpu.VMEM((total, width), BF),
            pltpu.VMEM((total + rows, width), BF),
            pltpu.VMEM((total, width), BF),
            pltpu.VMEM((total, widths[0]), BF),
            pltpu.VMEM((total, widths[0]), BF),
            pltpu.VMEM((n * nq, rows, rows), F32),
            pltpu.VMEM((total, widths[1]), BF),
            pltpu.VMEM((total, widths[1]), BF),
            pltpu.VMEM((total, ff), BF),
            pltpu.VMEM((total, ff), BF),
            pltpu.VMEM((total, ff), BF),
            pltpu.VMEM((width, total), BF),
            pltpu.VMEM((width, total), BF),
            pltpu.VMEM((total, width), BF),
            pltpu.VMEM((total + rows, width), BF),
            pltpu.VMEM((rows, width), F32),
            pltpu.VMEM((rows, width), F32),
            pltpu.VMEM((rows, width), F32),
            pltpu.VMEM((rows, width), F32),
            pltpu.VMEM((total, 1), F32),
            pltpu.VMEM((rows, 1), F32),
            pltpu.VMEM((total, LANES), F32),
            pltpu.VMEM((total, LANES), F32),
            pltpu.VMEM((nf * 8, width), F32),
            pltpu.VMEM((8, width), F32),
            pltpu.VMEM((n * 8, width), F32),
            pltpu.VMEM((nf * 8, width), F32),
            pltpu.VMEM((chips - 1, shard, widest), BF),
            pltpu.VMEM((chips, shard, widest), BF),
        ]
        + [pltpu.VMEM((chips, shard, w), BF) for w in widths]
        + [pltpu.VMEM((chips, shard, w), BF) for w in widths]
        + [
            pltpu.SemaphoreType.DMA((7, chips)),
            pltpu.SemaphoreType.DMA((7, chips)),
            pltpu.SemaphoreType.DMA((7, nf)),
            pltpu.SemaphoreType.DMA((7,)),
            pltpu.SemaphoreType.DMA((5, 2, n)),
            pltpu.SemaphoreType.DMA((5, n)),
            pltpu.SemaphoreType.DMA((4, n)),
            pltpu.SemaphoreType.DMA((4, n + 1)),
            pltpu.SemaphoreType.DMA((5, chips)),
            pltpu.SemaphoreType.DMA((5, chips)),
            pltpu.SemaphoreType.DMA((5, chips)),
            pltpu.SemaphoreType.DMA((5, chips)),
            pltpu.SemaphoreType.DMA((chips,)),
        ]
    )
    return pl.pallas_call(
        partial(layer_kernel, dims),
        out_shape=out_shape,
        in_specs=[pl.BlockSpec(memory_space=pltpu.SMEM)] + [vmem] * 4 + [anywhere] * 5,
        out_specs=[vmem] * 8 + [anywhere] * 5,
        scratch_shapes=scratch,
        compiler_params=pltpu.CompilerParams(
            collective_id=0, has_side_effects=True, vmem_limit_bytes=67043328
        ),
        name="layer",
    )(lengths, freq, tokens, cot, gains, *shards)


def split_pad(weight, heads):
    lead = weight.shape[0]
    halves = weight.reshape(lead, heads, 2, HALF)
    return jnp.pad(halves, ((0, 0), (0, 0), (0, 0), (0, LANES // 2 - HALF))).reshape(lead, -1)


def end_pad(weight, heads):
    lead = weight.shape[0]
    return jnp.pad(
        weight.reshape(lead, heads, HD), ((0, 0), (0, 0), (0, LANES - HD))
    ).reshape(lead, -1)


def split_take(grad, heads):
    lead = grad.shape[0]
    return grad.reshape(lead, heads, 2, LANES // 2)[..., :HALF].reshape(lead, heads * HD)


def end_take(grad, heads):
    lead = grad.shape[0]
    return grad.reshape(lead, heads, LANES)[..., :HD].reshape(lead, heads * HD)


def body(
    n,
    chips,
    tokens,
    lengths,
    cotangent,
    attn_gain,
    w_query,
    w_key,
    w_value,
    w_out,
    mlp_gain,
    w_gate,
    w_up,
    w_down,
):
    shard = attn_gain.shape[1]
    width = tokens.shape[1]
    nq = w_query.shape[2] // HD
    nkv = w_key.shape[2] // HD
    start = lax.axis_index("fsdp") * shard
    both = jnp.concatenate([attn_gain, mlp_gain], axis=0).astype(F32)
    gains = lax.dynamic_update_slice(jnp.zeros((8, width), F32), both, (0, start))
    frequency = ROPE_BASE ** (-jnp.arange(HALF, dtype=F32) / HALF)
    frequency = jnp.pad(frequency, (0, LANES // 2 - HALF))
    freq = jnp.concatenate([frequency, frequency])[None, :]
    shards = (
        jnp.concatenate(
            [split_pad(w_query[0], nq), split_pad(w_key[0], nkv), end_pad(w_value[0], nkv)], axis=1
        ),
        end_pad(w_out[0].T, nq),
        w_gate[0],
        w_up[0],
        w_down[0].T,
    )
    results = run_layer(
        lengths, freq, tokens, cotangent, gains, shards, (n, chips, nq, nkv)
    )
    output, grad_tokens, gain_rows, g_qkv, g_out, g_gate, g_up, g_down = results[:8]
    gain_cut = lax.dynamic_slice(gain_rows, (0, start), (2, shard))
    q_end, k_end = nq * LANES, (nq + nkv) * LANES
    return (
        output,
        grad_tokens,
        gain_cut[0:1],
        split_take(g_qkv[:, :q_end], nq)[None],
        split_take(g_qkv[:, q_end:k_end], nkv)[None],
        end_take(g_qkv[:, k_end:], nkv)[None],
        end_take(g_out, nq).T[None],
        gain_cut[1:2],
        g_gate[None],
        g_up[None],
        g_down.T[None],
    )


def solution(mesh):
    placed = (
        P(("fsdp", "dp"), None),
        P("fsdp", None),
        P(("fsdp", "dp"), None),
        P(None, "fsdp"),
        P(None, "fsdp", "dp"),
        P(None, "fsdp", "dp"),
        P(None, "fsdp", "dp"),
        P(None, "dp", "fsdp"),
        P(None, "fsdp"),
        P(None, "fsdp", "dp"),
        P(None, "fsdp", "dp"),
        P(None, "dp", "fsdp"),
    )
    return jax.shard_map(
        partial(body, mesh.shape["dp"], mesh.shape["fsdp"] // 2),
        mesh=mesh,
        in_specs=placed,
        out_specs=(
            P(("fsdp", "dp"), None),
            P(("fsdp", "dp"), None),
            P(None, "fsdp"),
            P(None, "fsdp", "dp"),
            P(None, "fsdp", "dp"),
            P(None, "fsdp", "dp"),
            P(None, "dp", "fsdp"),
            P(None, "fsdp"),
            P(None, "fsdp", "dp"),
            P(None, "fsdp", "dp"),
            P(None, "dp", "fsdp"),
        ),
        check_vma=False,
    )
```

```python
from functools import partial

import jax
import jax.numpy as jnp
from jax import lax
from jax.experimental import pallas as pl
from jax.experimental.pallas import tpu as pltpu
from jax.sharding import PartitionSpec as P

HD = 96
HALF = 48
LANES = 128
EPSILON = 1e-05
ROPE_BASE = 100000.0
NEG_FILL = -1e30
MESH = pl.DeviceIdType.MESH
BF = jnp.bfloat16
F32 = jnp.float32
TILE = 256
CHUNK = 32


def mm(left, right):
    return jnp.dot(left, right, preferred_element_type=F32)


def mm_nt(left, right):
    return lax.dot_general(left, right, (((1,), (1,)), ((), ())), preferred_element_type=F32)


def mm_tn(left, right):
    return lax.dot_general(left, right, (((0,), (0,)), ((), ())), preferred_element_type=F32)


def loop(count, body):
    def step(index, carry):
        body(index)
        return carry

    lax.fori_loop(0, count, step, 0)


def flip(chip, bits):
    other, bit = chip, 1
    while bit <= bits:
        if bits & bit:
            other = other + bit * (1 - 2 * ((chip // bit) % 2))
        bit *= 2
    return other


def layer_kernel(dims, *refs):
    n, chips, rows, width, nq, nkv, ff, nseq = dims
    nf = 2 * chips
    shard = width // nf
    total = n * rows
    half = rows // 2
    q_wide, kv_wide = nq * LANES, nkv * LANES
    widths = (q_wide + 2 * kv_wide, q_wide, ff, ff, ff)
    near = [1] if chips > 1 else []
    far = [2 * k for k in range(1, chips // 2)]
    refs = list(refs)

    def take(count):
        taken = refs[:count]
        del refs[:count]
        return taken

    (lengths, freq, tokens, cot, gain_a, gain_m, w_q, w_k, w_v, w_o, w_d, w_g, w_u) = take(13)
    (out_ref, gtok_ref, out_ga, out_gm, out_q, out_k, out_v, out_o, out_g, out_u, out_d) = take(11)
    landing = take(5)
    weights = take(5)
    (x_buf, ct_buf, mi_buf, gm_buf) = take(4)
    (qkv, gqkv, probs, mixed, gmixed, hid, gg, gu) = take(8)
    (t_one, t_two) = take(2)
    (s_buf, r_buf, own_sum, middle, gmid) = take(5)
    (sc_one, sc_two, cos_t, sin_t) = take(4)
    (gains_in, gain_in, gain_row, gain_z, gain_f, stage) = take(6)
    (pick_rope, pick_end, same) = take(3)
    send_b = take(1)[0]
    sums = take(5)
    from_partner = take(5)
    (w_ss, w_fs, w_qs, w_rs, w_ls) = take(5)
    (z_ss, z_rs) = take(2)
    (rs_ss, rs_rs) = take(2)
    (b_ss, b_rs, i_ss, i_rs, l_sem) = take(5)

    f = lax.axis_index("fsdp")
    d = lax.axis_index("dp")
    p = f // 2
    c = f % 2

    def at_f(index):
        return {"fsdp": index, "dp": d}

    def at_d(index):
        return {"fsdp": f, "dp": index}

    partner = p * 2 + 1 - c

    def remote(src, dst, ss, rs, where):
        return pltpu.make_async_remote_copy(
            src_ref=src, dst_ref=dst, send_sem=ss, recv_sem=rs, device_id=where, device_id_type=MESH
        )

    def span(index, size):
        return pl.ds(pl.multiple_of(index * size, size), size)

    def block(ref, index, size=rows):
        return ref.at[span(index, size)]

    def cols(index, size=TILE):
        return span(index, size)

    barrier = pltpu.get_barrier_semaphore()
    for k in range(1, chips):
        pl.semaphore_signal(
            barrier, inc=1, device_id=at_f(flip(p, k) * 2 + c), device_id_type=MESH
        )
    pl.semaphore_signal(barrier, inc=1, device_id=at_f(partner), device_id_type=MESH)

    @pl.when(d > 0)
    def _():
        pl.semaphore_signal(barrier, inc=1, device_id=at_d(d - 1), device_id_type=MESH)

    @pl.when(d < n - 1)
    def _():
        pl.semaphore_signal(barrier, inc=1, device_id=at_d(d + 1), device_id_type=MESH)

    ends = (d == 0).astype(jnp.int32) + (d == n - 1).astype(jnp.int32)

    class Gather:
        def __init__(self, slot, dst, size, src=None):
            self.slot, self.dst, self.size = slot, dst, size
            self.src = self.part(f) if src is None else src
            self.local = src is not None

        def part(self, index):
            return block(self.dst, index, self.size)

        def direct(self, k):
            where = partner if k == 0 else flip(p, k) * 2 + c
            return remote(
                self.src, self.part(f), w_ss.at[self.slot, k], w_rs.at[self.slot, f], at_f(where)
            )

        def onward(self, k):
            index = flip(p, k) * 2 + c
            return remote(
                self.part(index),
                self.part(index),
                w_fs.at[self.slot, k],
                w_rs.at[self.slot, index],
                at_f(partner),
            )

        def across(self, first, second):
            index = flip(p, first) * 2 + c
            return remote(
                self.part(index),
                self.part(index),
                w_qs.at[self.slot, first + second],
                w_rs.at[self.slot, index],
                at_f(flip(p, second) * 2 + c),
            )

        def own(self):
            return pltpu.make_async_copy(self.src, self.part(f), w_ls.at[self.slot])

        def start(self):
            for k in near + far + [0]:
                self.direct(k).start()
            if self.local:
                self.own().start()

        def relay(self):
            for core, first, second in ((0, near, far), (1, far, near)):

                @pl.when(c == core)
                def _():
                    for k in first:
                        copy = self.onward(k)
                        copy.wait_recv()
                        for other in second:
                            self.across(k, other).start()
                        copy.start()

        def forward(self):
            for core, second in ((0, far), (1, near)):

                @pl.when(c == core)
                def _():
                    for k in second:
                        copy = self.onward(k)
                        copy.wait_recv()
                        copy.start()

            for k in near:
                for other in far:
                    copy = self.onward(k + other)
                    copy.wait_recv()
                    copy.start()

        def finish(self):
            for k in range(chips):
                index = flip(p, k) * 2 + 1 - c
                remote(
                    self.part(index),
                    self.part(index),
                    w_fs.at[self.slot, k],
                    w_rs.at[self.slot, index],
                    at_f(partner),
                ).wait_recv()
            if self.local:
                self.own().wait()

        def drain(self):
            for k in near + far + [0]:
                self.direct(k).wait_send()
            for k in range(1, chips):
                self.onward(k).wait_send()
            for k in near:
                for other in far:
                    remote(
                        self.part(f),
                        self.part(f),
                        w_qs.at[self.slot, k + other],
                        w_rs.at[self.slot, f],
                        at_f(partner),
                    ).wait_send()

    class Line:
        def __init__(self, slot, buf, size=rows, parts=1, src=None):
            self.slot, self.buf, self.size, self.parts, self.src = slot, buf, size, parts, src

        def copy(self, index, side, h, own=False):
            piece = self.size // self.parts
            part = block(self.buf, index * self.parts + h, piece)
            src = self.src if own and self.src is not None else part
            where = d + 1 if side == 0 else d - 1
            return remote(
                src,
                part,
                z_ss.at[self.slot, side, h, index],
                z_rs.at[self.slot, h, index],
                at_d(where),
            )

        def start(self, h=0):
            @pl.when(d < n - 1)
            def _():
                self.copy(d, 0, h, True).start()

            @pl.when(d > 0)
            def _():
                self.copy(d, 1, h, True).start()

        def step(self, s, h=0):
            @pl.when(d - s >= 0)
            def _():
                copy = self.copy(d - s, 0, h)
                copy.wait_recv()

                @pl.when(d < n - 1)
                def _():
                    copy.start()

            @pl.when(d + s < n)
            def _():
                copy = self.copy(d + s, 1, h)
                copy.wait_recv()

                @pl.when(d > 0)
                def _():
                    copy.start()

        def drain(self):
            for h in range(self.parts):
                for j in range(n):

                    @pl.when((j <= d) & (d < n - 1))
                    def _():
                        self.copy(j, 0, h).wait_send()

                    @pl.when((j >= d) & (d > 0))
                    def _():
                        self.copy(j, 1, h).wait_send()

    class Reduce:
        def __init__(self, slot, tiles_of, sends, gets):
            self.slot, self.tiles_of, self.sends, self.gets = slot, tiles_of, sends, gets

        def copy(self, index, where, slot, h):
            return remote(
                block(self.sends, 2 * index + h, half),
                block(self.gets, 2 * slot + h, half),
                rs_ss.at[self.slot, h, index],
                rs_rs.at[self.slot, h, slot],
                at_d(where),
            )

        def got(self, slot, h):
            part = block(self.gets, 2 * slot + h, half)
            remote(
                part, part, rs_ss.at[self.slot, h, 0], rs_rs.at[self.slot, h, slot], at_d(d)
            ).wait_recv()

        def right(self, index, h):
            return self.copy(index, d + 1, index, h)

        def left(self, index, h, last):
            return self.copy(index, d - 1, n if last else index, h)

        def compute(self):
            def store(j):
                def put(t, value):
                    self.sends[span(j, rows), cols(t)] = value.astype(BF)

                return put

            def keep(t, value):
                own_sum[:, cols(t)] = value

            def one(i):
                right, left = d + n - 1 - i, d - (n - 1 - i)

                @pl.when(right < n)
                def _():
                    self.tiles_of(right, store(right))

                @pl.when((right < n) & (i == 0))
                def _():
                    self.right(right, 0).start()

                @pl.when(left >= 0)
                def _():
                    self.tiles_of(left, store(left))

                @pl.when((left >= 0) & (i == 0))
                def _():
                    self.left(left, 0, n == 2).start()

            loop(n - 1, one)
            self.tiles_of(d, keep)

        def add_into(self, index, h):
            self.got(index, h)

            def some(i):
                r = pl.ds(pl.multiple_of(index * rows + h * half + i * CHUNK, CHUNK), CHUNK)
                self.sends[r, :] = (
                    self.sends[r, :].astype(F32) + self.gets[r, :].astype(F32)
                ).astype(BF)

            loop(half // CHUNK, some)

        def advance(self, s, h):
            right, left = d + s, d - s

            @pl.when(right < n)
            def _():
                @pl.when(d > 0)
                def _():
                    self.add_into(right, h)

                self.right(right, h).start()

            @pl.when(left >= 0)
            def _():
                @pl.when(d < n - 1)
                def _():
                    self.add_into(left, h)

                self.left(left, h, s == 1).start()

        def final(self, h):
            def add(slot):
                self.got(slot, h)

                def some(i):
                    r = pl.ds(pl.multiple_of(h * half + i * CHUNK, CHUNK), CHUNK)
                    there = pl.ds(
                        pl.multiple_of(slot * rows + h * half + i * CHUNK, CHUNK), CHUNK
                    )
                    own_sum[r, :] = own_sum[r, :] + self.gets[there, :].astype(F32)

                loop(half // CHUNK, some)

            @pl.when(d > 0)
            def _():
                add(d)

            @pl.when(d < n - 1)
            def _():
                add(n)

        def drain(self):
            for h in range(2):
                for j in range(n):

                    @pl.when(d != j)
                    def _():
                        self.copy(j, d, j, h).wait_send()

    class Grad:
        def __init__(self, group, turned, terms, emit):
            self.group, self.turned, self.terms, self.emit = group, turned, terms, emit
            self.width = widths[group]

        def hand_over(self, k):
            chip = flip(p, k)
            return remote(
                send_b.at[k, :, pl.ds(0, self.width)],
                from_partner[self.group].at[chip],
                b_ss.at[self.group, k],
                b_rs.at[self.group, chip],
                at_f(partner),
            )

        def ship(self, k):
            chip = flip(p, k)
            return remote(
                sums[self.group].at[chip],
                landing[self.group].at[k - 1],
                i_ss.at[self.group, k - 1],
                i_rs.at[self.group, k - 1],
                at_f(chip * 2 + c),
            )

        def send(self, k):
            left = self.turned.at[span(flip(p, k) * 2 + 1 - c, shard)]

            def tile(t):
                send_b[k, :, cols(t)] = mm(left[...], self.terms[:, cols(t)]).astype(BF)

            loop(self.width // TILE, tile)
            self.hand_over(k).start()

        def own(self, k):
            chip = flip(p, k)
            left = self.turned.at[span(chip * 2 + c, shard)]
            part = from_partner[self.group].at[chip]
            remote(
                part, part, b_ss.at[self.group, k], b_rs.at[self.group, chip], at_f(partner)
            ).wait_recv()

            def tile(t):
                term = mm(left[...], self.terms[:, cols(t)])
                other = from_partner[self.group][chip, :, cols(t)].astype(F32)
                sums[self.group][chip, :, cols(t)] = (term + other).astype(BF)

            loop(self.width // TILE, tile)
            if k > 0:
                self.ship(k).start()

        def send_all(self):
            for k in list(range(1, chips)) + [0]:
                self.send(k)

        def own_all(self):
            for k in list(range(1, chips)) + [0]:
                self.own(k)
            for k in range(chips):
                self.hand_over(k).wait_send()

        def fetch(self, k):
            return pltpu.make_async_copy(
                landing[self.group].at[k - 1],
                stage.at[k - 1, :, pl.ds(0, self.width)],
                l_sem.at[k - 1],
            )

        def finish(self):
            for k in range(1, chips):
                self.ship(k).wait()
                self.fetch(k).start()
            for k in range(1, chips):
                self.fetch(k).wait()

            def parts(lanes):
                yield sums[self.group][p, :, lanes]
                for k in range(1, chips):
                    yield stage[k - 1, :, lanes]

            self.emit(parts)

    def total_of(values):
        result = None
        for value in values:
            result = value if result is None else result + value
        return result

    def emit_plain(out):
        def emit(parts):
            def tile(t):
                out[:, cols(t)] = total_of(v.astype(F32) for v in parts(cols(t)))

            loop(ff // TILE, tile)

        return emit

    def emit_down(parts):
        def tile(t):
            out_d[cols(t), :] = total_of(mm_nt(same[...], v) for v in parts(cols(t)))

        loop(ff // TILE, tile)

    def emit_out(parts):
        lanes = pl.ds(0, q_wide)
        out_o[...] = total_of(mm_nt(pick_end[...], v) for v in parts(lanes))

    def emit_qkv(parts):
        kv_rows = nkv * HD
        lanes = pl.ds(0, q_wide)
        out_q[...] = total_of(mm_nt(v, pick_rope[...]) for v in parts(lanes))
        lanes = pl.ds(q_wide, kv_wide)
        pick = pick_rope[0:kv_rows, 0:kv_wide]
        out_k[...] = total_of(mm_nt(v, pick) for v in parts(lanes))
        lanes = pl.ds(q_wide + kv_wide, kv_wide)
        pick = pick_end[0:kv_rows, 0:kv_wide]
        out_v[...] = total_of(mm_nt(v, pick) for v in parts(lanes))

    def turn(src, dst):
        def lane_block(t):
            dst[cols(t, LANES), :] = src[pl.ds(0, total), cols(t, LANES)].T

        loop(width // LANES, lane_block)

    def at(s, work):
        if s == 0:
            work(d)
            return

        def side(i):
            j = d - s + 2 * s * i

            @pl.when((j >= 0) & (j < n))
            def _():
                work(j)

        loop(2, side)

    def one_hot(split):
        shape = (nq * HD, q_wide)
        row = lax.broadcasted_iota(jnp.int32, shape, 0)
        lane = lax.broadcasted_iota(jnp.int32, shape, 1)
        inside = lane % LANES
        start = (lane // LANES) * HD
        if split:
            gap = LANES // 2 - HALF
            upper = inside >= LANES // 2
            source = start + jnp.where(upper, inside - gap, inside)
            real = (inside % (LANES // 2)) < HALF
        else:
            source = start + inside
            real = inside < HD
        return jnp.where(real & (row == source), 1.0, 0.0).astype(BF)

    pick_rope[...] = one_hot(True)
    pick_end[...] = one_hot(False)
    square = (TILE, TILE)
    same[...] = jnp.where(
        lax.broadcasted_iota(jnp.int32, square, 0) == lax.broadcasted_iota(jnp.int32, square, 1),
        1.0,
        0.0,
    ).astype(BF)
    mine = span(f, shard)
    kv_rows = nkv * HD
    weights[0][mine, 0:q_wide] = mm(w_q[...], pick_rope[...]).astype(BF)
    weights[0][mine, q_wide : q_wide + kv_wide] = mm(
        w_k[...], pick_rope[0:kv_rows, 0:kv_wide]
    ).astype(BF)
    weights[0][mine, q_wide + kv_wide : q_wide + 2 * kv_wide] = mm(
        w_v[...], pick_end[0:kv_rows, 0:kv_wide]
    ).astype(BF)
    eye = same[0:shard, 0:shard]
    weights[1][mine, :] = mm(mm_nt(eye, w_o[...]).astype(BF), pick_end[...]).astype(BF)
    weights[4][mine, :] = mm_nt(eye, w_d[...]).astype(BF)
    gains_in[...] = jnp.zeros((8, width), F32)
    gains_in[0:1, 0:shard] = gain_a[...].astype(F32)
    gains_in[1:2, 0:shard] = gain_m[...].astype(F32)
    block(gain_in, f, 8)[...] = pltpu.roll(gains_in[...], f * shard, 1)

    gathers = [
        Gather(0, weights[0], shard),
        Gather(1, weights[1], shard),
        Gather(2, weights[2], shard, w_g),
        Gather(3, weights[3], shard, w_u),
        Gather(4, weights[4], shard),
    ]
    gain_gather = Gather(5, gain_in, 8)
    tok_line = Line(0, x_buf, src=tokens)
    cot_line = Line(1, ct_buf, src=cot)
    mi_line = Line(2, mi_buf, parts=2)
    gm_line = Line(3, gm_buf, parts=2)
    gain_line = Line(4, gain_z, 8)

    block(x_buf, d)[...] = tokens[...]
    block(ct_buf, d)[...] = cot[...]

    def segments(b, shape, dim):
        index = lax.broadcasted_iota(jnp.int32, shape, dim)
        segment = jnp.zeros(shape, jnp.int32)
        offset = jnp.zeros(shape, jnp.int32)
        end = jnp.int32(0)
        for k in range(nseq):
            end = end + lengths[b, k]
            past = index >= end
            segment = segment + past.astype(jnp.int32)
            offset = jnp.where(past, end, offset)
        return index, segment, offset

    def tables(b):
        index, _, offset = segments(b, (rows, LANES), 0)
        angle = (index - offset).astype(F32) * freq[...]
        lane = lax.broadcasted_iota(jnp.int32, (rows, LANES), 1)
        sine = jnp.sin(angle)
        block(cos_t, b)[...] = jnp.cos(angle)
        block(sin_t, b)[...] = jnp.where(lane < LANES // 2, -sine, sine)

    pl.semaphore_wait(barrier, chips + 2 - ends)
    tok_line.start()
    gain_gather.start()
    gathers[0].start()
    gathers[1].start()
    loop(n, tables)
    gain_gather.relay()
    gain_gather.forward()
    gain_gather.finish()
    gain_row[...] = total_of(gain_in[pl.ds(8 * k, 8), :] for k in range(nf))

    def rms(value):
        mean = jnp.sum(value * value, axis=-1, keepdims=True) / width
        return lax.rsqrt(mean + EPSILON)

    def norm_one(j):
        def some(i):
            r = pl.ds(pl.multiple_of(j * rows + i * CHUNK, CHUNK), CHUNK)
            value = x_buf[r, :].astype(F32)
            scale = rms(value)
            sc_one[r, :] = scale
            mi_buf[r, :] = (value * scale * gain_row[0:1, :]).astype(BF)

        loop(rows // CHUNK, some)

    def rope(value, sign, cos_v, sin_v):
        return value * cos_v + sign * (pltpu.roll(value, LANES // 2, 1) * sin_v)

    heads = nq + 2 * nkv

    def head(ref, r, h):
        return ref[r, h * LANES : (h + 1) * LANES]

    def attend(b):
        r = span(b, rows)
        cos_v, sin_v = cos_t[r, :], sin_t[r, :]
        for t in range(heads // 2):
            both = mm(mi_buf[r, :], weights[0][:, 2 * t * LANES : 2 * (t + 1) * LANES])
            for h in (2 * t, 2 * t + 1):
                value = both[:, (h - 2 * t) * LANES : (h - 2 * t + 1) * LANES]
                if h < nq + nkv:
                    value = rope(value, 1.0, cos_v, sin_v)
                qkv[r, h * LANES : (h + 1) * LANES] = value.astype(BF)
        t_index, t_seg, _ = segments(b, (rows, rows), 0)
        s_index, s_seg, _ = segments(b, (rows, rows), 1)
        allowed = (t_seg == s_seg) & (s_index <= t_index)
        for h in range(nq):
            kv = h // (nq // nkv)
            score = mm_nt(head(qkv, r, h), head(qkv, r, nq + kv)) * HD ** (-0.5)
            score = jnp.where(allowed, score, NEG_FILL)
            top = jnp.max(score, axis=-1, keepdims=True)
            log_total = top + jnp.log(jnp.sum(jnp.exp(score - top), axis=-1, keepdims=True))
            prob = jnp.where(allowed, jnp.exp(score - log_total), 0.0)
            probs[b * nq + h] = prob
            mixed[r, h * LANES : (h + 1) * LANES] = mm(
                prob.astype(BF), head(qkv, r, nq + nkv + kv)
            ).astype(BF)

    norm_one(d)
    tok_line.step(1)
    gathers[0].relay()
    gathers[2].start()
    at(1, norm_one)
    early = min(2, n - 1)
    if early == 2:
        tok_line.step(2)
        at(2, norm_one)
    gathers[1].relay()
    gathers[3].start()
    gathers[0].forward()
    gathers[0].finish()
    for s in range(early + 1):
        at(s, attend)
    gathers[2].relay()
    gathers[4].start()
    gathers[1].forward()
    for s in range(early + 1, n):
        tok_line.step(s)
        at(s, norm_one)
        at(s, attend)
    gathers[1].finish()

    def by_turned(pairs, also=None):
        def tiles_of(j, put):
            r = span(j, rows)

            def tile(t):
                value = total_of(mm_nt(left[r, :], weight[cols(t), :]) for left, weight in pairs)
                put(t, value)
                if also is not None:
                    also(j, t, value)

            loop(width // TILE, tile)

        return tiles_of

    def run(work):
        if work:
            todo = work.pop(0)
            if todo is not None:
                todo()

    def reduce_then_gather(red, finish_half, line, work):
        red.compute()
        run(work)
        for s in range(n - 2, 0, -1):
            red.advance(s, 0)
            run(work)
        red.advance(n - 1, 1)
        red.final(0)
        finish_half(0)
        line.start(0)
        for i in range(1, n - 1):
            red.advance(n - 1 - i, 1)
            run(work)
            line.step(i, 0)
        red.final(1)
        finish_half(1)
        line.start(1)
        line.step(n - 1, 0)

    def norm_two(h):
        def some(i):
            r = pl.ds(pl.multiple_of(h * half + i * CHUNK, CHUNK), CHUNK)
            value = tokens[r, :].astype(F32) + own_sum[r, :]
            scale = rms(value)
            middle[r, :] = value
            sc_two[r, :] = scale
            here = pl.ds(pl.multiple_of(d * rows + h * half + i * CHUNK, CHUNK), CHUNK)
            mi_buf[here, :] = (value * scale * gain_row[1:2, :]).astype(BF)

        loop(half // CHUNK, some)

    def up_stage():
        gathers[3].relay()
        gathers[2].forward()

    def down_stage():
        gathers[4].relay()
        gathers[3].forward()

    def cot_step(s):
        return lambda: cot_line.step(s)

    after_attn = Reduce(0, by_turned([(mixed, weights[1])]), s_buf, r_buf)
    work = [cot_line.start, up_stage, None, cot_step(1), down_stage]
    work += [cot_step(s) for s in range(2, n)]
    reduce_then_gather(after_attn, norm_two, mi_line, work)
    while work:
        run(work)
    gathers[4].forward()
    for g in (2, 3, 4):
        gathers[g].finish()

    def feed(j):
        r = span(j, rows)

        def tile(t):
            left = mi_buf[r, :]
            gate = mm(left, weights[2][:, cols(t)])
            up = mm(left, weights[3][:, cols(t)])
            grad_hidden = mm(ct_buf[r, :], weights[4][:, cols(t)])
            sig = 1.0 / (1.0 + jnp.exp(-gate))
            hid[r, cols(t)] = (gate * sig * up).astype(BF)
            gu[r, cols(t)] = (grad_hidden * gate * sig).astype(BF)
            gg[r, cols(t)] = (grad_hidden * up * sig * (1.0 + gate * (1.0 - sig))).astype(BF)

        loop(ff // TILE, tile)

    mi_line.step(1, 1)
    at(0, feed)
    at(1, feed)
    for s in range(2, n):
        mi_line.step(s, 1)
        if s == 2:
            turn(ct_buf, t_one)
        at(s, feed)
    if n == 2:
        turn(ct_buf, t_one)
    after_attn.drain()
    mi_line.drain()
    cot_line.drain()

    gain_own = block(gain_z, d, 8)
    gain_own[...] = jnp.zeros((8, width), F32)

    def back_two(h):
        def some(i):
            r = pl.ds(pl.multiple_of(h * half + i * CHUNK, CHUNK), CHUNK)
            term = own_sum[r, :]
            scale = sc_two[r, :]
            normed = middle[r, :] * scale
            gain_sum = jnp.sum(term * normed, axis=0, keepdims=True)
            dn = term * gain_row[1:2, :]
            mean = jnp.sum(dn * normed, axis=-1, keepdims=True) / width
            value = cot[r, :].astype(F32) + scale * (dn - normed * mean)
            gmid[r, :] = value
            here = pl.ds(pl.multiple_of(d * rows + h * half + i * CHUNK, CHUNK), CHUNK)
            gm_buf[here, :] = value.astype(BF)
            gain_own[1:2, :] = gain_own[1:2, :] + gain_sum

        loop(half // CHUNK, some)

    after_mlp = Reduce(1, by_turned([(gg, weights[2]), (gu, weights[3])]), s_buf, r_buf)
    down = Grad(4, t_one, hid, emit_down)
    gate_g = Grad(2, t_two, gg, emit_plain(out_g))
    up_g = Grad(3, t_two, gu, emit_plain(out_u))

    def turn_mi():
        turn(mi_buf, t_two)

    work = [turn_mi, down.send_all, down.own_all, gate_g.send_all, gate_g.own_all]
    reduce_then_gather(after_mlp, back_two, gm_line, work)
    while work:
        run(work)
    after_mlp.drain()

    def back(b):
        r = span(b, rows)

        def tile(t):
            gmixed[r, cols(t)] = mm(gm_buf[r, :], weights[1][:, cols(t)]).astype(BF)

        loop(q_wide // TILE, tile)
        cos_v, sin_v = cos_t[r, :], sin_t[r, :]
        group = nq // nkv
        for kv in range(nkv):
            key, val = head(qkv, r, nq + kv), head(qkv, r, nq + nkv + kv)
            grad_k = grad_v = None
            for h in range(kv * group, (kv + 1) * group):
                query, gm_h = head(qkv, r, h), head(gmixed, r, h)
                prob = probs[b * nq + h]
                delta = jnp.sum(
                    gm_h.astype(F32) * head(mixed, r, h).astype(F32), axis=-1, keepdims=True
                )
                grad_p = mm_nt(gm_h, val)
                grad_s = (prob * (grad_p - delta) * HD ** (-0.5)).astype(BF)
                grad_q = mm(grad_s, key)
                gqkv[r, h * LANES : (h + 1) * LANES] = rope(grad_q, -1.0, cos_v, sin_v).astype(BF)
                k_term, v_term = mm_tn(grad_s, query), mm_tn(prob.astype(BF), gm_h)
                grad_k = k_term if grad_k is None else grad_k + k_term
                grad_v = v_term if grad_v is None else grad_v + v_term
            k_at, v_at = (nq + kv) * LANES, (nq + nkv + kv) * LANES
            gqkv[r, k_at : k_at + LANES] = rope(grad_k, -1.0, cos_v, sin_v).astype(BF)
            gqkv[r, v_at : v_at + LANES] = grad_v.astype(BF)

    output = Reduce(2, by_turned([(hid, weights[4])]), ct_buf, mi_buf)

    gm_line.step(1, 1)
    at(0, back)
    at(1, back)
    for s in range(2, n):
        gm_line.step(s, 1)
        at(s, back)

    def add_gain(j, t, value):
        r = span(j, rows)
        normed = x_buf[r, cols(t)].astype(F32) * sc_one[r, :]
        gain_own[0:1, cols(t)] = gain_own[0:1, cols(t)] + jnp.sum(
            value * normed, axis=0, keepdims=True
        )

    def write_out(h):
        def some(i):
            r = pl.ds(pl.multiple_of(h * half + i * CHUNK, CHUNK), CHUNK)
            out_ref[r, :] = (middle[r, :] + own_sum[r, :]).astype(BF)

        loop(half // CHUNK, some)

    output.compute()
    work = [up_g.send_all, up_g.own_all]
    for s in range(n - 1, 0, -1):
        if s < n - 1:
            output.advance(s, 0)
        output.advance(s, 1)
        run(work)
    while work:
        run(work)
    for h in range(2):
        output.final(h)
        write_out(h)

    after_in = Reduce(3, by_turned([(gqkv, weights[0])], add_gain), s_buf, r_buf)
    out_g_grad = Grad(1, t_one, mixed, emit_out)
    qkv_g = Grad(0, t_two, gqkv, emit_qkv)

    def turn_attn_in():
        def one(b):
            there = span(b, rows)

            def lane_block(t):
                value = x_buf[there, cols(t, LANES)].astype(F32) * sc_one[there, :]
                value = (value * gain_row[0:1, cols(t, LANES)]).astype(BF)
                t_two[cols(t, LANES), cols(b, rows)] = value.T

            loop(width // LANES, lane_block)

        loop(n, one)

    def turn_gm():
        turn(gm_buf, t_one)

    after_in.compute()
    gain_line.start()
    turn_attn_in()
    qkv_g.send_all()
    work = [qkv_g.own_all, turn_gm, out_g_grad.send_all, out_g_grad.own_all]
    steps = list(range(1, n))
    for s in range(n - 1, 0, -1):
        if s < n - 1:
            after_in.advance(s, 0)
        after_in.advance(s, 1)
        run(work)
        if steps:
            gain_line.step(steps.pop(0))
    while work:
        run(work)
    block(gain_f, f, 8)[...] = total_of(gain_z[pl.ds(8 * k, 8), :] for k in range(n))
    gain_back = Gather(6, gain_f, 8)
    gain_back.start()
    down.finish()
    gate_g.finish()
    gain_back.relay()
    gain_back.forward()
    up_g.finish()

    def back_one(h):
        def some(i):
            r = pl.ds(pl.multiple_of(h * half + i * CHUNK, CHUNK), CHUNK)
            there = pl.ds(pl.multiple_of(d * rows + h * half + i * CHUNK, CHUNK), CHUNK)
            scale = sc_one[there, :]
            normed = tokens[r, :].astype(F32) * scale
            dm = own_sum[r, :] * gain_row[0:1, :]
            mean = jnp.sum(dm * normed, axis=-1, keepdims=True) / width
            gtok_ref[r, :] = gmid[r, :] + scale * (dm - normed * mean)

        loop(half // CHUNK, some)

    for h in range(2):
        after_in.final(h)
        back_one(h)
    qkv_g.finish()
    out_g_grad.finish()
    gain_back.finish()
    gain_sum = total_of(gain_f[pl.ds(8 * k, 8), :] for k in range(nf))
    gain_sum = pltpu.roll(gain_sum, (width - f * shard) % width, 1)
    out_ga[...] = gain_sum[0:1, 0:shard]
    out_gm[...] = gain_sum[1:2, 0:shard]

    output.drain()
    after_in.drain()
    for line in (tok_line, gm_line, gain_line):
        line.drain()
    for gather in gathers + [gain_gather, gain_back]:
        gather.drain()


def pass_on(*refs):
    count = (len(refs) - 2) // 3
    srcs, dsts, held = refs[:count], refs[count : 2 * count], refs[2 * count : 3 * count]
    in_sem, out_sem = refs[3 * count :]
    order = range(count)
    for i in order:
        pltpu.make_async_copy(srcs[i], held[i], in_sem.at[i]).start()
    for i in order:
        pltpu.make_async_copy(srcs[i], held[i], in_sem.at[i]).wait()
        pltpu.make_async_copy(held[i], dsts[i], out_sem.at[i]).start()
    for i in order:
        pltpu.make_async_copy(held[i], dsts[i], out_sem.at[i]).wait()


def run_layer(lengths, freq, tokens, cot, gain_a, gain_m, w_q, w_k, w_v, w_o, w_d, w_g, w_u, n, chips):
    rows, width = tokens.shape
    nq = w_q.shape[1] // HD
    nkv = w_k.shape[1] // HD
    total = n * rows
    nf = 2 * chips
    shard = w_q.shape[0]
    ff = w_g.shape[1]
    q_wide, kv_wide = nq * LANES, nkv * LANES
    widths = (q_wide + 2 * kv_wide, q_wide, ff, ff, ff)
    dims = (n, chips, rows, width, nq, nkv, ff, lengths.shape[1])
    vmem = pl.BlockSpec(memory_space=pltpu.VMEM)
    anywhere = pl.BlockSpec(memory_space=pl.ANY)
    results = [
        jax.ShapeDtypeStruct((rows, width), BF),
        jax.ShapeDtypeStruct((rows, width), F32),
        jax.ShapeDtypeStruct((1, shard), F32),
        jax.ShapeDtypeStruct((1, shard), F32),
    ] + [jax.ShapeDtypeStruct(w.shape, F32) for w in (w_q, w_k, w_v, w_o, w_g, w_u, w_d)]
    out_shape = results + [jax.ShapeDtypeStruct((chips - 1, shard, w), BF) for w in widths]
    widest = max(widths)
    scratch = (
        [pltpu.VMEM((width, w), BF) for w in widths]
        + [
            pltpu.VMEM((total, width), BF),
            pltpu.VMEM((total, width), BF),
            pltpu.VMEM((total + rows, width), BF),
            pltpu.VMEM((total, width), BF),
            pltpu.VMEM((total, widths[0]), BF),
            pltpu.VMEM((total, widths[0]), BF),
            pltpu.VMEM((n * nq, rows, rows), F32),
            pltpu.VMEM((total, q_wide), BF),
            pltpu.VMEM((total, q_wide), BF),
            pltpu.VMEM((total, ff), BF),
            pltpu.VMEM((total, ff), BF),
            pltpu.VMEM((total, ff), BF),
            pltpu.VMEM((width, total), BF),
            pltpu.VMEM((width, total), BF),
            pltpu.VMEM((total, width), BF),
            pltpu.VMEM((total + rows, width), BF),
            pltpu.VMEM((rows, width), F32),
            pltpu.VMEM((rows, width), F32),
            pltpu.VMEM((rows, width), F32),
            pltpu.VMEM((total, 1), F32),
            pltpu.VMEM((rows, 1), F32),
            pltpu.VMEM((total, LANES), F32),
            pltpu.VMEM((total, LANES), F32),
            pltpu.VMEM((8, width), F32),
            pltpu.VMEM((nf * 8, width), F32),
            pltpu.VMEM((8, width), F32),
            pltpu.VMEM((n * 8, width), F32),
            pltpu.VMEM((nf * 8, width), F32),
            pltpu.VMEM((chips - 1, shard, widest), BF),
            pltpu.VMEM((nq * HD, q_wide), BF),
            pltpu.VMEM((nq * HD, q_wide), BF),
            pltpu.VMEM((TILE, TILE), BF),
            pltpu.VMEM((chips, shard, widest), BF),
        ]
        + [pltpu.VMEM((chips, shard, w), BF) for w in widths]
        + [pltpu.VMEM((chips, shard, w), BF) for w in widths]
        + [
            pltpu.SemaphoreType.DMA((7, chips)),
            pltpu.SemaphoreType.DMA((7, chips)),
            pltpu.SemaphoreType.DMA((7, chips)),
            pltpu.SemaphoreType.DMA((7, nf)),
            pltpu.SemaphoreType.DMA((7,)),
            pltpu.SemaphoreType.DMA((5, 2, 2, n)),
            pltpu.SemaphoreType.DMA((5, 2, n)),
            pltpu.SemaphoreType.DMA((4, 2, n)),
            pltpu.SemaphoreType.DMA((4, 2, n + 1)),
            pltpu.SemaphoreType.DMA((5, chips)),
            pltpu.SemaphoreType.DMA((5, chips)),
            pltpu.SemaphoreType.DMA((5, chips)),
            pltpu.SemaphoreType.DMA((5, chips)),
            pltpu.SemaphoreType.DMA((chips,)),
        ]
    )
    made = pl.pallas_call(
        partial(layer_kernel, dims),
        out_shape=out_shape,
        in_specs=[pl.BlockSpec(memory_space=pltpu.SMEM)] + [vmem] * 10 + [anywhere] * 2,
        out_specs=[vmem] * 11 + [anywhere] * 5,
        scratch_shapes=scratch,
        compiler_params=pltpu.CompilerParams(
            collective_id=0, has_side_effects=True, vmem_limit_bytes=67043328
        ),
        name="layer",
    )(lengths, freq, tokens, cot, gain_a, gain_m, w_q, w_k, w_v, w_o, w_d, w_g, w_u)
    count = len(results)
    return pl.pallas_call(
        pass_on,
        out_shape=results,
        in_specs=[anywhere] * count,
        out_specs=[anywhere] * count,
        scratch_shapes=[pltpu.VMEM(r.shape, r.dtype) for r in results]
        + [pltpu.SemaphoreType.DMA((count,)), pltpu.SemaphoreType.DMA((count,))],
        compiler_params=pltpu.CompilerParams(vmem_limit_bytes=32 * 2**20),
        name="results",
    )(*made[:count])


def body(
    n,
    chips,
    tokens,
    lengths,
    cotangent,
    attn_gain,
    w_query,
    w_key,
    w_value,
    w_out,
    mlp_gain,
    w_gate,
    w_up,
    w_down,
):
    frequency = ROPE_BASE ** (-jnp.arange(HALF, dtype=F32) / HALF)
    frequency = jnp.pad(frequency, (0, LANES // 2 - HALF))
    freq = jnp.concatenate([frequency, frequency])[None, :]
    results = run_layer(
        lengths,
        freq,
        tokens,
        cotangent,
        attn_gain,
        mlp_gain,
        w_query[0],
        w_key[0],
        w_value[0],
        w_out[0],
        w_down[0],
        w_gate[0],
        w_up[0],
        n,
        chips,
    )
    output, grad_tokens, g_again, g_mgain, g_q, g_k, g_v, g_o, g_gate, g_up, g_down = results
    return (
        output,
        grad_tokens,
        g_again,
        g_q[None],
        g_k[None],
        g_v[None],
        g_o[None],
        g_mgain,
        g_gate[None],
        g_up[None],
        g_down[None],
    )


def solution(mesh):
    placed = (
        P(("fsdp", "dp"), None),
        P("fsdp", None),
        P(("fsdp", "dp"), None),
        P(None, "fsdp"),
        P(None, "fsdp", "dp"),
        P(None, "fsdp", "dp"),
        P(None, "fsdp", "dp"),
        P(None, "dp", "fsdp"),
        P(None, "fsdp"),
        P(None, "fsdp", "dp"),
        P(None, "fsdp", "dp"),
        P(None, "dp", "fsdp"),
    )
    return jax.shard_map(
        partial(body, mesh.shape["dp"], mesh.shape["fsdp"] // 2),
        mesh=mesh,
        in_specs=placed,
        out_specs=(
            P(("fsdp", "dp"), None),
            P(("fsdp", "dp"), None),
            P(None, "fsdp"),
            P(None, "fsdp", "dp"),
            P(None, "fsdp", "dp"),
            P(None, "fsdp", "dp"),
            P(None, "dp", "fsdp"),
            P(None, "fsdp"),
            P(None, "fsdp", "dp"),
            P(None, "fsdp", "dp"),
            P(None, "dp", "fsdp"),
        ),
        check_vma=False,
    )
```

```python
from functools import partial

import jax
import jax.numpy as jnp
from jax import lax
from jax.experimental import pallas as pl
from jax.experimental.pallas import tpu as pltpu
from jax.sharding import PartitionSpec as P

HD = 96
HALF = 48
LANES = 128
EPSILON = 1e-05
ROPE_BASE = 100000.0
NEG_FILL = -1e30
MESH = pl.DeviceIdType.MESH
BF = jnp.bfloat16
F32 = jnp.float32
TILE = 256
CHUNK = 32


def mm(left, right):
    return jnp.dot(left, right, preferred_element_type=F32)


def mm_nt(left, right):
    return lax.dot_general(left, right, (((1,), (1,)), ((), ())), preferred_element_type=F32)


def mm_tn(left, right):
    return lax.dot_general(left, right, (((0,), (0,)), ((), ())), preferred_element_type=F32)


def loop(count, body):
    def step(index, carry):
        body(index)
        return carry

    lax.fori_loop(0, count, step, 0)


def flip(chip, bits):
    other, bit = chip, 1
    while bit <= bits:
        if bits & bit:
            other = other + bit * (1 - 2 * ((chip // bit) % 2))
        bit *= 2
    return other


def layer_kernel(dims, *refs):
    n, chips, rows, width, nq, nkv, ff, nseq = dims
    nf = 2 * chips
    shard = width // nf
    total = n * rows
    half = rows // 2
    q_wide, kv_wide = nq * LANES, nkv * LANES
    widths = (q_wide + 2 * kv_wide, q_wide, ff, ff, ff)
    widest = max(widths)
    near = [1] if chips > 1 else []
    far = [2 * k for k in range(1, chips // 2)]
    refs = list(refs)

    def take(count):
        taken = refs[:count]
        del refs[:count]
        return taken

    (lengths, freq, gain_a, gain_m) = take(4)
    (tokens, cot, w_q, w_k, w_v, w_o, w_d, w_g, w_u) = take(9)
    (out_ref, gtok_ref, out_ga, out_gm, out_q, out_k, out_v, out_o, out_g, out_u, out_d) = take(11)
    far_landing = take(3)
    near_landing = take(2)
    landing = near_landing + far_landing
    weights = take(5)
    (x_buf, ct_buf, mi_buf, gm_buf) = take(4)
    (qkv, gqkv, probs, mixed, gmixed, hid, gg, gu) = take(8)
    (t_one, t_two) = take(2)
    (s_buf, r_buf, own_sum, middle, gmid, wide_tile) = take(6)
    (sc_one, sc_two, cos_t, sin_t) = take(4)
    (gain_in, gain_row, gain_own, gain_z, gain_f, stage) = take(6)
    (pick_rope, pick_end) = take(2)
    (q_in, k_in, v_in, o_in) = take(4)
    (out_own, q_own, k_own, v_own, o_own, big_own) = take(6)
    send_b = take(1)[0]
    sums = take(5)
    from_partner = take(5)
    (w_ss, w_fs, w_qs, w_rs, w_ls) = take(5)
    (z_ss, z_rs) = take(2)
    (rs_ss, rs_rs) = take(2)
    (b_ss, b_rs, i_ss, i_rs, l_sem, in_sem, out_sem) = take(7)

    f = lax.axis_index("fsdp")
    d = lax.axis_index("dp")
    p = f // 2
    c = f % 2

    def at_f(index):
        return {"fsdp": index, "dp": d}

    def at_d(index):
        return {"fsdp": f, "dp": index}

    partner = p * 2 + 1 - c

    def remote(src, dst, ss, rs, where):
        return pltpu.make_async_remote_copy(
            src_ref=src, dst_ref=dst, send_sem=ss, recv_sem=rs, device_id=where, device_id_type=MESH
        )

    def span(index, size):
        return pl.ds(pl.multiple_of(index * size, size), size)

    def block(ref, index, size=rows):
        return ref.at[span(index, size)]

    def cols(index, size=TILE):
        return span(index, size)

    loads = [
        pltpu.make_async_copy(src, dst, in_sem.at[i])
        for i, (src, dst) in enumerate(
            (
                (w_q, q_in),
                (w_k, k_in),
                (w_v, v_in),
                (w_o, o_in),
                (tokens, block(x_buf, d)),
                (cot, block(ct_buf, d)),
            )
        )
    ]
    for copy in loads:
        copy.start()

    barrier = pltpu.get_barrier_semaphore()
    for k in range(1, chips):
        pl.semaphore_signal(
            barrier, inc=1, device_id=at_f(flip(p, k) * 2 + c), device_id_type=MESH
        )
    pl.semaphore_signal(barrier, inc=1, device_id=at_f(partner), device_id_type=MESH)

    for k in range(1, n):
        pl.semaphore_signal(
            barrier, inc=1, device_id=at_d((d + k) % n), device_id_type=MESH
        )

    class Gather:
        def __init__(self, slot, dst, size, src=None, plain=False):
            self.slot, self.dst, self.size = slot, dst, size
            self.src = self.part(f) if src is None else src
            self.local = src is not None
            self.aimed = list(range(1, chips)) if plain else near + far
            self.plain = plain

        def part(self, index):
            return block(self.dst, index, self.size)

        def direct(self, k):
            where = partner if k == 0 else flip(p, k) * 2 + c
            return remote(
                self.src, self.part(f), w_ss.at[self.slot, k], w_rs.at[self.slot, f], at_f(where)
            )

        def onward(self, k):
            index = flip(p, k) * 2 + c
            return remote(
                self.part(index),
                self.part(index),
                w_fs.at[self.slot, k],
                w_rs.at[self.slot, index],
                at_f(partner),
            )

        def across(self, first, second):
            index = flip(p, first) * 2 + c
            return remote(
                self.part(index),
                self.part(index),
                w_qs.at[self.slot, first + second],
                w_rs.at[self.slot, index],
                at_f(flip(p, second) * 2 + c),
            )

        def own(self):
            return pltpu.make_async_copy(self.src, self.part(f), w_ls.at[self.slot])

        def start(self):
            for k in self.aimed + [0]:
                self.direct(k).start()
            if self.local:
                self.own().start()

        def relay(self):
            for core, first, second in ((0, near, far), (1, far, near)):

                @pl.when(c == core)
                def _():
                    for k in first:
                        copy = self.onward(k)
                        copy.wait_recv()
                        for other in second:
                            self.across(k, other).start()
                        copy.start()

        def forward(self):
            if self.plain:
                for k in range(1, chips):
                    copy = self.onward(k)
                    copy.wait_recv()
                    copy.start()
                return

            for core, second in ((0, far), (1, near)):

                @pl.when(c == core)
                def _():
                    for k in second:
                        copy = self.onward(k)
                        copy.wait_recv()
                        copy.start()

            for k in near:
                for other in far:
                    copy = self.onward(k + other)
                    copy.wait_recv()
                    copy.start()

        def finish(self):
            for k in range(chips):
                index = flip(p, k) * 2 + 1 - c
                remote(
                    self.part(index),
                    self.part(index),
                    w_fs.at[self.slot, k],
                    w_rs.at[self.slot, index],
                    at_f(partner),
                ).wait_recv()
            if self.local:
                self.own().wait()

        def drain(self):
            for k in self.aimed + [0]:
                self.direct(k).wait_send()
            for k in range(1, chips):
                self.onward(k).wait_send()
            if self.plain:
                return
            for k in near:
                for other in far:
                    remote(
                        self.part(f),
                        self.part(f),
                        w_qs.at[self.slot, k + other],
                        w_rs.at[self.slot, f],
                        at_f(partner),
                    ).wait_send()

    class Line:
        def __init__(self, slot, buf, size=rows, parts=1, src=None):
            self.slot, self.buf, self.size, self.parts, self.src = slot, buf, size, parts, src

        def copy(self, index, side, h, own=False):
            piece = self.size // self.parts
            part = block(self.buf, index * self.parts + h, piece)
            src = part
            if own and self.src is not None:
                src = self.src.at[pl.ds(h * piece, piece)]
            where = d + 1 if side == 0 else d - 1
            return remote(
                src,
                part,
                z_ss.at[self.slot, side, h, index],
                z_rs.at[self.slot, h, index],
                at_d(where),
            )

        def start(self, h=0):
            @pl.when(d < n - 1)
            def _():
                self.copy(d, 0, h, True).start()

            @pl.when(d > 0)
            def _():
                self.copy(d, 1, h, True).start()

        def pass_on(self, index, side, h):
            copy = self.copy(index, side, h)
            copy.wait_recv()
            copy.start()

        def inward(self, s, h=0):
            @pl.when((d > 0) & (d < n // 2) & (d + s < n))
            def _():
                self.pass_on(d + s, 1, h)

            @pl.when((d < n - 1) & (d >= n // 2) & (d - s >= 0))
            def _():
                self.pass_on(d - s, 0, h)

        def outward(self, s, h=0):
            @pl.when((d < n // 2) & (d - s >= 0))
            def _():
                self.pass_on(d - s, 0, h)

            @pl.when((d >= n // 2) & (d + s < n))
            def _():
                self.pass_on(d + s, 1, h)

        def step(self, s, h=0):
            self.inward(s, h)
            self.outward(s, h)

        def arrive(self, s, h=0):
            @pl.when((d - s >= 0) & (d == n - 1))
            def _():
                self.copy(d - s, 0, h).wait_recv()

            @pl.when((d + s < n) & (d == 0))
            def _():
                self.copy(d + s, 1, h).wait_recv()

        def drain(self):
            for h in range(self.parts):
                for j in range(n):

                    @pl.when((j <= d) & (d < n - 1))
                    def _():
                        self.copy(j, 0, h).wait_send()

                    @pl.when((j >= d) & (d > 0))
                    def _():
                        self.copy(j, 1, h).wait_send()

    class Reduce:
        def __init__(self, slot, tile_of, sends, gets, also=None):
            self.slot, self.tile_of, self.sends, self.gets = slot, tile_of, sends, gets
            self.also = also

        def copy(self, index, where, slot, h):
            return remote(
                block(self.sends, 2 * index + h, half),
                block(self.gets, 2 * slot + h, half),
                rs_ss.at[self.slot, h, index],
                rs_rs.at[self.slot, h, slot],
                at_d(where),
            )

        def got(self, slot, h):
            part = block(self.gets, 2 * slot + h, half)
            remote(
                part, part, rs_ss.at[self.slot, h, 0], rs_rs.at[self.slot, h, slot], at_d(d)
            ).wait_recv()

        def right(self, index, h):
            return self.copy(index, d + 1, index, h)

        def left(self, index, h, last):
            return self.copy(index, d - 1, n if last else index, h)

        def compute(self):
            def tile(t):
                value = self.tile_of(t)
                wide_tile[...] = value
                own_sum[:, cols(t)] = wide_tile[span(d, rows), :]
                self.sends[pl.ds(0, total), cols(t)] = value.astype(BF)
                if self.also is not None:
                    self.also(t, value)

            loop(width // TILE, tile)

        def launch(self, halves_first):
            order = [(s, h) for h in range(2) for s in range(n - 1, 0, -1)]
            if not halves_first:
                order = [(s, h) for s in range(n - 1, 0, -1) for h in range(2)]

            @pl.when(d == 0)
            def _():
                for s, h in order:
                    self.right(d + s, h).start()

            @pl.when(d == n - 1)
            def _():
                for s, h in order:
                    self.left(d - s, h, s == 1).start()

        def add_into(self, index, h):
            self.got(index, h)

            def some(i):
                r = pl.ds(pl.multiple_of(index * rows + h * half + i * CHUNK, CHUNK), CHUNK)
                self.sends[r, :] = (
                    self.sends[r, :].astype(F32) + self.gets[r, :].astype(F32)
                ).astype(BF)

            loop(half // CHUNK, some)

        def advance(self, s, h):
            right, left = d + s, d - s

            @pl.when((right < n) & (d > 0))
            def _():
                self.add_into(right, h)
                self.right(right, h).start()

            @pl.when((left >= 0) & (d < n - 1))
            def _():
                self.add_into(left, h)
                self.left(left, h, s == 1).start()

        def final(self, h):
            self.final_into(own_sum, h)

        def final_into(self, acc, h):
            def add(slot):
                self.got(slot, h)

                def some(i):
                    r = pl.ds(pl.multiple_of(h * half + i * CHUNK, CHUNK), CHUNK)
                    there = pl.ds(
                        pl.multiple_of(slot * rows + h * half + i * CHUNK, CHUNK), CHUNK
                    )
                    acc[r, :] = acc[r, :] + self.gets[there, :].astype(F32)

                loop(half // CHUNK, some)

            @pl.when(d > 0)
            def _():
                add(d)

            @pl.when(d < n - 1)
            def _():
                add(n)

        def drain(self):
            for h in range(2):
                for j in range(n):

                    @pl.when(d != j)
                    def _():
                        self.copy(j, d, j, h).wait_send()

    handing = []

    class Grad:
        def __init__(self, group, turned, terms, emit):
            self.group, self.turned, self.terms, self.emit = group, turned, terms, emit
            self.width = widths[group]

        def hand_over(self):
            src = send_b if self.width == widest else send_b.at[:, :, pl.ds(0, self.width)]
            return remote(
                src,
                from_partner[self.group],
                b_ss.at[self.group],
                b_rs.at[self.group],
                at_f(partner),
            )

        def ship(self, k):
            chip = flip(p, k)
            return remote(
                sums[self.group].at[chip],
                landing[self.group].at[k - 1],
                i_ss.at[self.group, k - 1],
                i_rs.at[self.group, k - 1],
                at_f(chip * 2 + c),
            )

        def blocks_of(self, core, t):
            left = jnp.concatenate(
                [self.turned[span(q * 2 + core, shard), :] for q in range(chips)], axis=0
            )
            value = mm(left, self.terms[:, cols(t)])
            return [value[q * shard : (q + 1) * shard] for q in range(chips)]

        def release(self):
            self.hand_over().wait_send()

        def send_all(self):
            if handing:
                handing.pop().release()

            def tile(t):
                for q, value in enumerate(self.blocks_of(1 - c, t)):
                    send_b[q, :, cols(t)] = value.astype(BF)

            loop(self.width // TILE, tile)
            self.hand_over().start()
            handing.append(self)

        def own_all(self):
            self.hand_over().wait_recv()

            def tile(t):
                for q, value in enumerate(self.blocks_of(c, t)):
                    other = from_partner[self.group][q, :, cols(t)].astype(F32)
                    sums[self.group][q, :, cols(t)] = (value + other).astype(BF)

            loop(self.width // TILE, tile)
            for k in range(1, chips):
                self.ship(k).start()

        def fetch(self, k):
            return pltpu.make_async_copy(
                landing[self.group].at[k - 1],
                stage.at[k - 1, :, pl.ds(0, self.width)],
                l_sem.at[k - 1],
            )

        def collect(self):
            for k in range(1, chips):
                self.ship(k).wait()
                if self.group >= 2:
                    self.fetch(k).start()

        def finish(self):
            if self.group >= 2:
                for k in range(1, chips):
                    self.fetch(k).wait()

            def parts(lanes):
                yield sums[self.group][p, :, lanes]
                for k in range(1, chips):
                    if self.group >= 2:
                        yield stage[k - 1, :, lanes]
                    else:
                        yield landing[self.group][k - 1, :, lanes]

            self.emit(parts)

    def total_of(values):
        result = None
        for value in values:
            result = value if result is None else result + value
        return result

    stores = []

    def store(src, dst):
        copy = pltpu.make_async_copy(src, dst, out_sem.at[len(stores)])
        copy.start()
        stores.append(copy)

    def emit_plain(out):
        def emit(parts):
            def tile(t):
                big_own[:, cols(t)] = total_of(v.astype(F32) for v in parts(cols(t)))

            if big_stores:
                big_stores.pop().wait()
            loop(ff // TILE, tile)
            copy = pltpu.make_async_copy(big_own, out, l_sem.at[chips - 1])
            copy.start()
            big_stores.append(copy)

        return emit

    big_stores = []

    def emit_out(parts):
        lanes = pl.ds(0, q_wide)
        o_own[...] = total_of(mm_nt(v, pick_end[...]) for v in parts(lanes))
        store(o_own, out_o)

    def emit_qkv(parts):
        kv_rows = nkv * HD
        lanes = pl.ds(0, q_wide)
        q_own[...] = total_of(mm_nt(v, pick_rope[...]) for v in parts(lanes))
        store(q_own, out_q)
        lanes = pl.ds(q_wide, kv_wide)
        pick = pick_rope[0:kv_rows, 0:kv_wide]
        k_own[...] = total_of(mm_nt(v, pick) for v in parts(lanes))
        store(k_own, out_k)
        lanes = pl.ds(q_wide + kv_wide, kv_wide)
        pick = pick_end[0:kv_rows, 0:kv_wide]
        v_own[...] = total_of(mm_nt(v, pick) for v in parts(lanes))
        store(v_own, out_v)

    def turn(src, dst):
        def lane_block(t):
            dst[cols(t, LANES), :] = src[pl.ds(0, total), cols(t, LANES)].T

        loop(width // LANES, lane_block)

    def at(s, work):
        if s == 0:
            work(d)
            return

        def side(i):
            j = d - s + 2 * s * i

            @pl.when((j >= 0) & (j < n))
            def _():
                work(j)

        loop(2, side)

    def one_hot(split):
        shape = (nq * HD, q_wide)
        row = lax.broadcasted_iota(jnp.int32, shape, 0)
        lane = lax.broadcasted_iota(jnp.int32, shape, 1)
        inside = lane % LANES
        start = (lane // LANES) * HD
        if split:
            gap = LANES // 2 - HALF
            upper = inside >= LANES // 2
            source = start + jnp.where(upper, inside - gap, inside)
            real = (inside % (LANES // 2)) < HALF
        else:
            source = start + inside
            real = inside < HD
        return jnp.where(real & (row == source), 1.0, 0.0).astype(BF)

    pick_rope[...] = one_hot(True)
    pick_end[...] = one_hot(False)
    mine = span(f, shard)
    kv_rows = nkv * HD
    for copy in loads[:4]:
        copy.wait()
    weights[0][mine, 0:q_wide] = mm(q_in[...], pick_rope[...]).astype(BF)
    weights[0][mine, q_wide : q_wide + kv_wide] = mm(
        k_in[...], pick_rope[0:kv_rows, 0:kv_wide]
    ).astype(BF)
    weights[0][mine, q_wide + kv_wide : q_wide + 2 * kv_wide] = mm(
        v_in[...], pick_end[0:kv_rows, 0:kv_wide]
    ).astype(BF)
    weights[1][mine, :] = mm(o_in[...], pick_end[...]).astype(BF)
    gain_mine = block(gain_in, f, 8)
    gain_mine[...] = jnp.zeros(gain_mine.shape, F32)
    gain_mine[0:1, 0:shard] = gain_a[...].astype(F32)
    gain_mine[1:2, 0:shard] = gain_m[...].astype(F32)

    gathers = [
        Gather(0, weights[0], shard, plain=True),
        Gather(1, weights[1], shard, plain=True),
        Gather(2, weights[2], shard, w_g),
        Gather(3, weights[3], shard, w_u),
        Gather(4, weights[4], shard, w_d),
    ]
    gain_gather = Gather(5, gain_in, 8, plain=True)
    tok_line = Line(0, x_buf, parts=2, src=tokens)
    cot_line = Line(1, ct_buf, src=cot)
    mi_line = Line(2, mi_buf, parts=2)
    gm_line = Line(3, gm_buf, parts=2)

    def gain_swap(k):
        mine = block(gain_z, d, 8)
        return remote(
            mine, mine, z_ss.at[4, 0, 0, k], z_rs.at[4, 0, d], at_d((d + k) % n)
        )

    def gain_got(k):
        other = (d + k) % n
        part = block(gain_z, other, 8)
        remote(part, part, z_ss.at[4, 0, 0, k], z_rs.at[4, 0, other], at_d(d)).wait_recv()

    def segments(b, shape, dim):
        index = lax.broadcasted_iota(jnp.int32, shape, dim)
        segment = jnp.zeros(shape, jnp.int32)
        offset = jnp.zeros(shape, jnp.int32)
        end = jnp.int32(0)
        for k in range(nseq):
            end = end + lengths[b, k]
            past = index >= end
            segment = segment + past.astype(jnp.int32)
            offset = jnp.where(past, end, offset)
        return index, segment, offset

    def tables(b):
        index, _, offset = segments(b, (rows, LANES), 0)
        angle = (index - offset).astype(F32) * freq[...]
        lane = lax.broadcasted_iota(jnp.int32, (rows, LANES), 1)
        sine = jnp.sin(angle)
        block(cos_t, b)[...] = jnp.cos(angle)
        block(sin_t, b)[...] = jnp.where(lane < LANES // 2, -sine, sine)

    loop(n, tables)
    pl.semaphore_wait(barrier, chips + n - 1)
    for h in range(2):
        tok_line.start(h)
    gain_gather.start()
    gathers[0].start()
    gathers[1].start()

    @pl.when((d == 0) | (d == n - 1))
    def _():
        cot_line.start()

    for g in range(2, 5):
        gathers[g].start()
    loads[4].wait()
    gain_gather.forward()
    gain_gather.finish()
    for k in range(nf):
        gain_row[:, k * shard : (k + 1) * shard] = gain_in[8 * k : 8 * k + 8, 0:shard]

    def rms(value):
        mean = jnp.sum(value * value, axis=-1, keepdims=True) / width
        return lax.rsqrt(mean + EPSILON)

    def norm_one(j):
        def some(i):
            r = pl.ds(pl.multiple_of(j * rows + i * CHUNK, CHUNK), CHUNK)
            value = x_buf[r, :].astype(F32)
            scale = rms(value)
            sc_one[r, :] = scale
            mi_buf[r, :] = (value * scale * gain_row[0:1, :]).astype(BF)

        loop(rows // CHUNK, some)

    def rope(value, sign, cos_v, sin_v):
        return value * cos_v + sign * (pltpu.roll(value, LANES // 2, 1) * sin_v)

    heads = nq + 2 * nkv

    def head(ref, r, h):
        return ref[r, h * LANES : (h + 1) * LANES]

    def attend(b):
        r = span(b, rows)
        cos_v, sin_v = cos_t[r, :], sin_t[r, :]
        for t in range(heads // 2):
            both = mm(mi_buf[r, :], weights[0][:, 2 * t * LANES : 2 * (t + 1) * LANES])
            for h in (2 * t, 2 * t + 1):
                value = both[:, (h - 2 * t) * LANES : (h - 2 * t + 1) * LANES]
                if h < nq + nkv:
                    value = rope(value, 1.0, cos_v, sin_v)
                qkv[r, h * LANES : (h + 1) * LANES] = value.astype(BF)
        t_index, t_seg, _ = segments(b, (rows, rows), 0)
        s_index, s_seg, _ = segments(b, (rows, rows), 1)
        allowed = (t_seg == s_seg) & (s_index <= t_index)
        for h in range(nq):
            kv = h // (nq // nkv)
            score = mm_nt(head(qkv, r, h), head(qkv, r, nq + kv)) * HD ** (-0.5)
            score = jnp.where(allowed, score, NEG_FILL)
            top = jnp.max(score, axis=-1, keepdims=True)
            log_total = top + jnp.log(jnp.sum(jnp.exp(score - top), axis=-1, keepdims=True))
            prob = jnp.where(allowed, jnp.exp(score - log_total), 0.0)
            probs[b * nq + h] = prob
            mixed[r, h * LANES : (h + 1) * LANES] = mm(
                prob.astype(BF), head(qkv, r, nq + nkv + kv)
            ).astype(BF)

    def tokens_at(s):
        for h in range(2):
            tok_line.step(s, h)
            tok_line.arrive(s, h)

    norm_one(d)
    tokens_at(1)
    at(1, norm_one)
    early = min(2, n - 1)
    if early == 2:
        for h in range(2):
            tok_line.step(2, h)

    @pl.when((d > 0) & (d < n - 1))
    def _():
        cot_line.start()

    gathers[0].forward()
    if early == 2:
        for h in range(2):
            tok_line.arrive(2, h)
        at(2, norm_one)
    gathers[0].finish()
    for s in range(early + 1):
        at(s, attend)
    gathers[1].forward()
    cot_line.outward(1)
    for s in range(early + 1, n):
        tokens_at(s)
        at(s, norm_one)
        at(s, attend)
    gathers[1].finish()

    def by_turned(pairs):
        def tile_of(t):
            return total_of(mm_nt(left[...], weight[cols(t), :]) for left, weight in pairs)

        return tile_of

    def run(work):
        if work:
            todo = work.pop(0)
            if todo is not None:
                todo()

    def reduce_then_gather(red, finish_half, line, work):
        red.compute()
        red.launch(True)
        run(work)
        for s in range(n - 2, 0, -1):
            red.advance(s, 0)
            run(work)
        red.final(0)
        finish_half(0)
        line.start(0)
        run(work)
        for i in range(1, n - 1):
            red.advance(n - 1 - i, 1)
            if i == 1:
                line.inward(i, 0)
            run(work)
        red.final(1)
        finish_half(1)
        line.start(1)
        for i in range(1, n - 1):
            if i > 1:
                line.inward(i, 0)
            line.outward(i, 0)

    def arrived(line, s):
        line.step(s, 1)
        line.arrive(s, 0)
        line.arrive(s, 1)

    def norm_two(h):
        def some(i):
            r = pl.ds(pl.multiple_of(h * half + i * CHUNK, CHUNK), CHUNK)
            here = pl.ds(pl.multiple_of(d * rows + h * half + i * CHUNK, CHUNK), CHUNK)
            value = x_buf[here, :].astype(F32) + own_sum[r, :]
            scale = rms(value)
            middle[r, :] = value
            sc_two[r, :] = scale
            mi_buf[here, :] = (value * scale * gain_row[1:2, :]).astype(BF)

        loop(half // CHUNK, some)

    def both(*todo):
        def do():
            for one in todo:
                one()

        return do

    def cot_on(s):
        def do():
            cot_line.inward(s)
            if s > 1:
                cot_line.outward(s)

        return do

    after_attn = Reduce(0, by_turned([(mixed, weights[1])]), s_buf, r_buf)
    work = [cot_on(1)]
    work += [both(cot_on(2), gathers[2].relay)] if n > 2 else [gathers[2].relay]
    work += [gathers[3].relay, None, gathers[4].relay, gathers[2].forward]
    work += [cot_on(s) for s in range(3, n - 1)]
    reduce_then_gather(after_attn, norm_two, mi_line, work)
    while work:
        run(work)
    gathers[3].forward()
    gathers[4].forward()
    for g in (2, 3, 4):
        gathers[g].finish()
    loads[5].wait()

    def feed(j):
        r = span(j, rows)

        def tile(t):
            left = mi_buf[r, :]
            gate = mm(left, weights[2][:, cols(t)])
            up = mm(left, weights[3][:, cols(t)])
            grad_hidden = mm(ct_buf[r, :], weights[4][:, cols(t)])
            sig = 1.0 / (1.0 + jnp.exp(-gate))
            hid[r, cols(t)] = (gate * sig * up).astype(BF)
            gu[r, cols(t)] = (grad_hidden * gate * sig).astype(BF)
            gg[r, cols(t)] = (grad_hidden * up * sig * (1.0 + gate * (1.0 - sig))).astype(BF)

        loop(ff // TILE, tile)

    at(0, feed)
    for s in range(1, n):
        arrived(mi_line, s)
        cot_line.arrive(s)
        if s == n - 1:
            at(s, feed)
            turn(ct_buf, t_one)
        else:
            at(s, feed)
    after_attn.drain()
    mi_line.drain()
    cot_line.drain()

    gain_own[...] = jnp.zeros((8, width), F32)

    def back_two(h):
        def some(i):
            r = pl.ds(pl.multiple_of(h * half + i * CHUNK, CHUNK), CHUNK)
            term = own_sum[r, :]
            scale = sc_two[r, :]
            normed = middle[r, :] * scale
            gain_sum = jnp.sum(term * normed, axis=0, keepdims=True)
            dn = term * gain_row[1:2, :]
            mean = jnp.sum(dn * normed, axis=-1, keepdims=True) / width
            here = pl.ds(pl.multiple_of(d * rows + h * half + i * CHUNK, CHUNK), CHUNK)
            value = ct_buf[here, :].astype(F32) + scale * (dn - normed * mean)
            gmid[r, :] = value
            gm_buf[here, :] = value.astype(BF)
            gain_own[1:2, :] = gain_own[1:2, :] + gain_sum

        loop(half // CHUNK, some)

    after_mlp = Reduce(1, by_turned([(gg, weights[2]), (gu, weights[3])]), s_buf, r_buf)
    down = Grad(4, t_one, hid, emit_plain(out_d))
    gate_g = Grad(2, t_two, gg, emit_plain(out_g))
    up_g = Grad(3, t_two, gu, emit_plain(out_u))

    def turn_mi():
        turn(mi_buf, t_two)

    def attn_in_again(j):
        def some(i):
            r = pl.ds(pl.multiple_of(j * rows + i * CHUNK, CHUNK), CHUNK)
            value = x_buf[r, :].astype(F32) * sc_one[r, :]
            s_buf[r, :] = (value * gain_row[0:1, :]).astype(BF)

        loop(rows // CHUNK, some)

    work = [
        both(turn_mi, down.send_all),
        down.own_all,
        gate_g.send_all,
        both(gate_g.own_all, up_g.send_all),
        up_g.own_all,
    ]
    reduce_then_gather(after_mlp, back_two, gm_line, work)
    while work:
        run(work)
    after_mlp.drain()

    def back(b):
        r = span(b, rows)

        def tile(t):
            gmixed[r, cols(t)] = mm(gm_buf[r, :], weights[1][:, cols(t)]).astype(BF)

        loop(q_wide // TILE, tile)
        cos_v, sin_v = cos_t[r, :], sin_t[r, :]
        group = nq // nkv
        for kv in range(nkv):
            key, val = head(qkv, r, nq + kv), head(qkv, r, nq + nkv + kv)
            grad_k = grad_v = None
            for h in range(kv * group, (kv + 1) * group):
                query, gm_h = head(qkv, r, h), head(gmixed, r, h)
                prob = probs[b * nq + h]
                delta = jnp.sum(
                    gm_h.astype(F32) * head(mixed, r, h).astype(F32), axis=-1, keepdims=True
                )
                grad_p = mm_nt(gm_h, val)
                grad_s = (prob * (grad_p - delta) * HD ** (-0.5)).astype(BF)
                grad_q = mm(grad_s, key)
                gqkv[r, h * LANES : (h + 1) * LANES] = rope(grad_q, -1.0, cos_v, sin_v).astype(BF)
                k_term, v_term = mm_tn(grad_s, query), mm_tn(prob.astype(BF), gm_h)
                grad_k = k_term if grad_k is None else grad_k + k_term
                grad_v = v_term if grad_v is None else grad_v + v_term
            k_at, v_at = (nq + kv) * LANES, (nq + nkv + kv) * LANES
            gqkv[r, k_at : k_at + LANES] = rope(grad_k, -1.0, cos_v, sin_v).astype(BF)
            gqkv[r, v_at : v_at + LANES] = grad_v.astype(BF)

    output = Reduce(2, by_turned([(hid, weights[4])]), ct_buf, mi_buf)

    output.compute()
    output.launch(False)
    middle[...] = middle[...] + own_sum[...]
    at(0, back)
    loop(n, attn_in_again)
    turn(s_buf, t_two)
    later = [(s, h) for s in range(n - 2, 0, -1) for h in range(2)]
    for s in range(1, n):
        arrived(gm_line, s)
        at(s, back)
        if s < n - 1 and later:
            output.advance(*later.pop(0))

    def add_gain(t, value):
        normed = x_buf[:, cols(t)].astype(F32) * sc_one[...]
        gain_own[0:1, cols(t)] = jnp.sum(value * normed, axis=0, keepdims=True)

    after_in = Reduce(3, by_turned([(gqkv, weights[0])]), s_buf, r_buf, add_gain)
    out_g_grad = Grad(1, t_one, mixed, emit_out)
    qkv_g = Grad(0, t_two, gqkv, emit_qkv)

    after_in.compute()
    quarter = width // 4
    gain_mine = block(gain_z, d, 8)
    for i in range(8):
        gain_mine[i : i + 1, :] = gain_own[i // 4 : i // 4 + 1, pl.ds(i % 4 * quarter, quarter)]
    for k in range(1, n):
        gain_swap(k).start()
    after_in.launch(False)
    qkv_g.send_all()
    for k in range(1, n):
        gain_got(k)
    block(gain_f, f, 8)[...] = total_of(gain_z[8 * k : 8 * k + 8, :] for k in range(n))
    gain_back = Gather(6, gain_f, 8, plain=True)
    gain_back.start()
    qkv_g.own_all()

    def output_end():
        for h in range(2):
            output.final_into(middle, h)
        out_own[...] = middle[...].astype(BF)
        store(out_own, out_ref)

    def gain_end():
        gain_back.forward()
        gain_back.finish()
        gain_all = total_of(gain_f[8 * k : 8 * k + 8, :] for k in range(nf))
        for i in range(8):
            gain_own[i // 4 : i // 4 + 1, pl.ds(i % 4 * quarter, quarter)] = gain_all[i : i + 1, :]
        gain_all = pltpu.roll(gain_own[...], (width - f * shard) % width, 1)
        out_ga[...] = gain_all[0:1, 0:shard]
        out_gm[...] = gain_all[1:2, 0:shard]

    def turn_gm():
        turn(gm_buf, t_one)

    def output_later():
        while later:
            output.advance(*later.pop(0))

    work = [
        both(turn_gm, out_g_grad.send_all),
        both(output_later, out_g_grad.own_all),
        gain_end,
    ]
    for s in range(n - 2, 0, -1):
        for h in range(2):
            after_in.advance(s, h)
            run(work)
    while work:
        run(work)
    output_end()
    for grad in (down, gate_g, up_g):
        grad.collect()
        grad.finish()

    def back_one(h):
        def some(i):
            r = pl.ds(pl.multiple_of(h * half + i * CHUNK, CHUNK), CHUNK)
            there = pl.ds(pl.multiple_of(d * rows + h * half + i * CHUNK, CHUNK), CHUNK)
            scale = sc_one[there, :]
            normed = x_buf[there, :].astype(F32) * scale
            dm = own_sum[r, :] * gain_row[0:1, :]
            mean = jnp.sum(dm * normed, axis=-1, keepdims=True) / width
            gmid[r, :] = gmid[r, :] + scale * (dm - normed * mean)

        loop(half // CHUNK, some)

    for h in range(2):
        after_in.final(h)
        back_one(h)
        part = pl.ds(h * half, half)
        store(gmid.at[part], gtok_ref.at[part])
    for grad in (qkv_g, out_g_grad):
        grad.collect()
        grad.finish()

    handing.pop().release()
    output.drain()
    after_in.drain()
    tok_line.drain()
    gm_line.drain()
    for k in range(1, n):
        gain_swap(k).wait_send()
    for gather in gathers + [gain_gather, gain_back]:
        gather.drain()
    big_stores.pop().wait()
    for copy in stores:
        copy.wait()


def pass_on(*refs):
    count = (len(refs) - 2) // 3
    srcs, dsts, held = refs[:count], refs[count : 2 * count], refs[2 * count : 3 * count]
    in_sem, out_sem = refs[3 * count :]
    order = range(count)
    for i in order:
        pltpu.make_async_copy(srcs[i], held[i], in_sem.at[i]).start()
    for i in order:
        pltpu.make_async_copy(srcs[i], held[i], in_sem.at[i]).wait()
        pltpu.make_async_copy(held[i], dsts[i], out_sem.at[i]).start()
    for i in order:
        pltpu.make_async_copy(held[i], dsts[i], out_sem.at[i]).wait()


def run_layer(lengths, freq, tokens, cot, gain_a, gain_m, w_q, w_k, w_v, w_o, w_d, w_g, w_u, n, chips):
    rows, width = tokens.shape
    nq = w_q.shape[1] // HD
    nkv = w_k.shape[1] // HD
    total = n * rows
    nf = 2 * chips
    shard = w_q.shape[0]
    ff = w_g.shape[1]
    q_wide, kv_wide = nq * LANES, nkv * LANES
    widths = (q_wide + 2 * kv_wide, q_wide, ff, ff, ff)
    dims = (n, chips, rows, width, nq, nkv, ff, lengths.shape[1])
    vmem = pl.BlockSpec(memory_space=pltpu.VMEM)
    hbm = pl.BlockSpec(memory_space=pltpu.HBM)
    results = [
        jax.ShapeDtypeStruct((rows, width), BF),
        jax.ShapeDtypeStruct((rows, width), F32),
        jax.ShapeDtypeStruct((1, shard), F32),
        jax.ShapeDtypeStruct((1, shard), F32),
    ] + [jax.ShapeDtypeStruct(w.shape, F32) for w in (w_q, w_k, w_v, w_o, w_g, w_u, w_d)]
    out_shape = results + [jax.ShapeDtypeStruct((chips - 1, shard, w), BF) for w in widths[2:]]
    widest = max(widths)
    scratch = (
        [pltpu.VMEM((chips - 1, shard, w), BF) for w in widths[:2]]
        + [pltpu.VMEM((width, w), BF) for w in widths]
        + [
            pltpu.VMEM((total, width), BF),
            pltpu.VMEM((total, width), BF),
            pltpu.VMEM((total + rows, width), BF),
            pltpu.VMEM((total, width), BF),
            pltpu.VMEM((total, widths[0]), BF),
            pltpu.VMEM((total, widths[0]), BF),
            pltpu.VMEM((n * nq, rows, rows), F32),
            pltpu.VMEM((total, q_wide), BF),
            pltpu.VMEM((total, q_wide), BF),
            pltpu.VMEM((total, ff), BF),
            pltpu.VMEM((total, ff), BF),
            pltpu.VMEM((total, ff), BF),
            pltpu.VMEM((width, total), BF),
            pltpu.VMEM((width, total), BF),
            pltpu.VMEM((total, width), BF),
            pltpu.VMEM((total + rows, width), BF),
            pltpu.VMEM((rows, width), F32),
            pltpu.VMEM((rows, width), F32),
            pltpu.VMEM((rows, width), F32),
            pltpu.VMEM((total, TILE), F32),
            pltpu.VMEM((total, 1), F32),
            pltpu.VMEM((rows, 1), F32),
            pltpu.VMEM((total, LANES), F32),
            pltpu.VMEM((total, LANES), F32),
            pltpu.VMEM((nf * 8, -(-shard // LANES) * LANES), F32),
            pltpu.VMEM((8, width), F32),
            pltpu.VMEM((8, width), F32),
            pltpu.VMEM((n * 8, width // 4), F32),
            pltpu.VMEM((nf * 8, width // 4), F32),
            pltpu.VMEM((chips - 1, shard, widest), BF),
            pltpu.VMEM((nq * HD, q_wide), BF),
            pltpu.VMEM((nq * HD, q_wide), BF),
        ]
        + [pltpu.VMEM(w.shape, BF) for w in (w_q, w_k, w_v, w_o)]
        + [pltpu.VMEM((rows, width), BF)]
        + [pltpu.VMEM(w.shape, F32) for w in (w_q, w_k, w_v, w_o, w_g)]
        + [
            pltpu.VMEM((chips, shard, widest), BF),
        ]
        + [pltpu.VMEM((chips, shard, w), BF) for w in widths]
        + [pltpu.VMEM((chips, shard, w), BF) for w in widths]
        + [
            pltpu.SemaphoreType.DMA((7, chips)),
            pltpu.SemaphoreType.DMA((7, chips)),
            pltpu.SemaphoreType.DMA((7, chips)),
            pltpu.SemaphoreType.DMA((7, nf)),
            pltpu.SemaphoreType.DMA((7,)),
            pltpu.SemaphoreType.DMA((5, 2, 2, n)),
            pltpu.SemaphoreType.DMA((5, 2, n)),
            pltpu.SemaphoreType.DMA((4, 2, n)),
            pltpu.SemaphoreType.DMA((4, 2, n + 1)),
            pltpu.SemaphoreType.DMA((5,)),
            pltpu.SemaphoreType.DMA((5,)),
            pltpu.SemaphoreType.DMA((5, chips)),
            pltpu.SemaphoreType.DMA((5, chips)),
            pltpu.SemaphoreType.DMA((chips,)),
            pltpu.SemaphoreType.DMA((6,)),
            pltpu.SemaphoreType.DMA((7,)),
        ]
    )
    made = pl.pallas_call(
        partial(layer_kernel, dims),
        out_shape=out_shape,
        in_specs=[pl.BlockSpec(memory_space=pltpu.SMEM)] + [vmem] * 3 + [hbm] * 9,
        out_specs=[hbm] * 2 + [vmem] * 2 + [hbm] * 10,
        scratch_shapes=scratch,
        compiler_params=pltpu.CompilerParams(
            collective_id=0, has_side_effects=True, vmem_limit_bytes=67043328
        ),
        name="layer",
    )(lengths, freq, gain_a, gain_m, tokens, cot, w_q, w_k, w_v, w_o, w_d, w_g, w_u)
    count = len(results)
    return pl.pallas_call(
        pass_on,
        out_shape=results,
        in_specs=[hbm] * count,
        out_specs=[hbm] * count,
        scratch_shapes=[pltpu.VMEM(r.shape, r.dtype) for r in results]
        + [pltpu.SemaphoreType.DMA((count,)), pltpu.SemaphoreType.DMA((count,))],
        compiler_params=pltpu.CompilerParams(vmem_limit_bytes=67043328),
        name="results",
    )(*made[:count])


def body(
    n,
    chips,
    tokens,
    lengths,
    cotangent,
    attn_gain,
    w_query,
    w_key,
    w_value,
    w_out,
    mlp_gain,
    w_gate,
    w_up,
    w_down,
):
    frequency = ROPE_BASE ** (-jnp.arange(HALF, dtype=F32) / HALF)
    frequency = jnp.pad(frequency, (0, LANES // 2 - HALF))
    freq = jnp.concatenate([frequency, frequency])[None, :]
    results = run_layer(
        lengths,
        freq,
        tokens,
        cotangent,
        attn_gain,
        mlp_gain,
        w_query[0],
        w_key[0],
        w_value[0],
        w_out[0].T,
        w_down[0].T,
        w_gate[0],
        w_up[0],
        n,
        chips,
    )
    output, grad_tokens, g_again, g_mgain, g_q, g_k, g_v, g_o, g_gate, g_up, g_down = results
    return (
        output,
        grad_tokens,
        g_again,
        g_q[None],
        g_k[None],
        g_v[None],
        g_o.T[None],
        g_mgain,
        g_gate[None],
        g_up[None],
        g_down.T[None],
    )


def solution(mesh):
    placed = (
        P(("fsdp", "dp"), None),
        P("fsdp", None),
        P(("fsdp", "dp"), None),
        P(None, "fsdp"),
        P(None, "fsdp", "dp"),
        P(None, "fsdp", "dp"),
        P(None, "fsdp", "dp"),
        P(None, "dp", "fsdp"),
        P(None, "fsdp"),
        P(None, "fsdp", "dp"),
        P(None, "fsdp", "dp"),
        P(None, "dp", "fsdp"),
    )
    return jax.shard_map(
        partial(body, mesh.shape["dp"], mesh.shape["fsdp"] // 2),
        mesh=mesh,
        in_specs=placed,
        out_specs=(
            P(("fsdp", "dp"), None),
            P(("fsdp", "dp"), None),
            P(None, "fsdp"),
            P(None, "fsdp", "dp"),
            P(None, "fsdp", "dp"),
            P(None, "fsdp", "dp"),
            P(None, "dp", "fsdp"),
            P(None, "fsdp"),
            P(None, "fsdp", "dp"),
            P(None, "fsdp", "dp"),
            P(None, "dp", "fsdp"),
        ),
        check_vma=False,
    )
```

```python
from functools import partial

import jax
import jax.numpy as jnp
from jax import lax
from jax.experimental import pallas as pl
from jax.experimental.pallas import tpu as pltpu
from jax.sharding import PartitionSpec as P

HD = 96
HALF = 48
LANES = 128
EPSILON = 1e-05
ROPE_BASE = 100000.0
NEG_FILL = -1e30
MESH = pl.DeviceIdType.MESH
BF = jnp.bfloat16
F32 = jnp.float32
TILE = 256
CHUNK = 32


def mm(left, right):
    return jnp.dot(left, right, preferred_element_type=F32)


def mm_nt(left, right):
    return lax.dot_general(left, right, (((1,), (1,)), ((), ())), preferred_element_type=F32)


def mm_tn(left, right):
    return lax.dot_general(left, right, (((0,), (0,)), ((), ())), preferred_element_type=F32)


def loop(count, body):
    def step(index, carry):
        body(index)
        return carry

    lax.fori_loop(0, count, step, 0)


def whole_lanes(count):
    return -(-count // LANES) * LANES


def packed_widths(nq, nkv, ff):
    return (whole_lanes((nq + 2 * nkv) * HD), whole_lanes(nq * HD), ff, ff, ff)


def flip(chip, bits):
    other, bit = chip, 1
    while bit <= bits:
        if bits & bit:
            other = other + bit * (1 - 2 * ((chip // bit) % 2))
        bit *= 2
    return other


def layer_kernel(dims, *refs):
    n, chips, rows, width, nq, nkv, ff, nseq = dims
    nf = 2 * chips
    shard = width // nf
    total = n * rows
    half = rows // 2
    q_wide, kv_wide = nq * LANES, nkv * LANES
    widths = (q_wide + 2 * kv_wide, q_wide, ff, ff, ff)
    gwidths = packed_widths(nq, nkv, ff)
    widest = max(gwidths)
    near = [1] if chips > 1 else []
    far = [2 * k for k in range(1, chips // 2)]
    refs = list(refs)

    def take(count):
        taken = refs[:count]
        del refs[:count]
        return taken

    (lengths, freq, gain_a, gain_m) = take(4)
    (tokens, cot, w_q, w_k, w_v, w_o, w_d, w_g, w_u) = take(9)
    (out_ref, gtok_ref, out_ga, out_gm, out_q, out_k, out_v, out_o, out_g, out_u, out_d) = take(11)
    far_landing = take(3)
    near_landing = take(2)
    landing = near_landing + far_landing
    weights = take(5)
    (x_buf, ct_buf, mi_buf, gm_buf, r_two, cot_own) = take(6)
    (qkv, gqkv, probs, mixed, gmixed, hid, gg, gu, gqkv_pack, mixed_pack) = take(10)
    (t_one, t_two) = take(2)
    (s_buf, r_buf, own_sum, middle, gmid, wide_tile) = take(6)
    (sc_one, sc_two, cos_t, sin_t) = take(4)
    (gain_in, gain_row, gain_own, gain_z, gain_f, stage) = take(6)
    (pick_rope, pick_end) = take(2)
    (q_in, k_in, v_in, o_in) = take(4)
    (out_own, q_own, k_own, v_own, o_own, big_own) = take(6)
    send_b = take(1)[0]
    sums = take(5)
    from_partner = take(5)
    (w_ss, w_fs, w_qs, w_rs, w_ls) = take(5)
    (z_ss, z_rs) = take(2)
    (rs_ss, rs_rs) = take(2)
    (b_ss, b_rs, i_ss, i_rs, l_sem, in_sem, out_sem) = take(7)

    f = lax.axis_index("fsdp")
    d = lax.axis_index("dp")
    p = f // 2
    c = f % 2

    def at_f(index):
        return {"fsdp": index, "dp": d}

    def at_d(index):
        return {"fsdp": f, "dp": index}

    partner = p * 2 + 1 - c
    low = 1 - d // (n // 2)
    inner, outer = d - 1 + 2 * low, d + 1 - 2 * low
    end = (d == 0) | (d == n - 1)

    def remote(src, dst, ss, rs, where):
        return pltpu.make_async_remote_copy(
            src_ref=src, dst_ref=dst, send_sem=ss, recv_sem=rs, device_id=where, device_id_type=MESH
        )

    def span(index, size):
        return pl.ds(pl.multiple_of(index * size, size), size)

    def block(ref, index, size=rows):
        return ref.at[span(index, size)]

    def cols(index, size=TILE):
        return span(index, size)

    loads = [
        pltpu.make_async_copy(src, dst, in_sem.at[i])
        for i, (src, dst) in enumerate(
            (
                (w_q, q_in),
                (w_k, k_in),
                (w_v, v_in),
                (w_o, o_in),
                (tokens, block(x_buf, d)),
                (cot, block(ct_buf, d)),
                (cot, cot_own),
            )
        )
    ]
    for copy in loads:
        copy.start()

    barrier = pltpu.get_barrier_semaphore()
    for k in range(1, chips):
        pl.semaphore_signal(
            barrier, inc=1, device_id=at_f(flip(p, k) * 2 + c), device_id_type=MESH
        )
    pl.semaphore_signal(barrier, inc=1, device_id=at_f(partner), device_id_type=MESH)

    for k in range(1, n):
        pl.semaphore_signal(
            barrier, inc=1, device_id=at_d((d + k) % n), device_id_type=MESH
        )

    class Gather:
        def __init__(self, slot, dst, size, src=None, plain=False):
            self.slot, self.dst, self.size = slot, dst, size
            self.src = self.part(f) if src is None else src
            self.local = src is not None
            self.aimed = list(range(1, chips)) if plain else near + far
            self.plain = plain

        def part(self, index):
            return block(self.dst, index, self.size)

        def direct(self, k):
            where = partner if k == 0 else flip(p, k) * 2 + c
            return remote(
                self.src, self.part(f), w_ss.at[self.slot, k], w_rs.at[self.slot, f], at_f(where)
            )

        def onward(self, k):
            index = flip(p, k) * 2 + c
            return remote(
                self.part(index),
                self.part(index),
                w_fs.at[self.slot, k],
                w_rs.at[self.slot, index],
                at_f(partner),
            )

        def across(self, first, second):
            index = flip(p, first) * 2 + c
            return remote(
                self.part(index),
                self.part(index),
                w_qs.at[self.slot, first + second],
                w_rs.at[self.slot, index],
                at_f(flip(p, second) * 2 + c),
            )

        def own(self):
            return pltpu.make_async_copy(self.src, self.part(f), w_ls.at[self.slot])

        def start(self):
            for k in self.aimed + [0]:
                self.direct(k).start()
            if self.local:
                self.own().start()

        def relay(self):
            for core, first, second in ((0, near, far), (1, far, near)):

                @pl.when(c == core)
                def _():
                    for k in first:
                        copy = self.onward(k)
                        copy.wait_recv()
                        for other in second:
                            self.across(k, other).start()
                        copy.start()

        def forward(self):
            if self.plain:
                for k in range(1, chips):
                    copy = self.onward(k)
                    copy.wait_recv()
                    copy.start()
                return

            for core, second in ((0, far), (1, near)):

                @pl.when(c == core)
                def _():
                    for k in second:
                        copy = self.onward(k)
                        copy.wait_recv()
                        copy.start()

            for k in near:
                for other in far:
                    copy = self.onward(k + other)
                    copy.wait_recv()
                    copy.start()

        def finish(self):
            for k in range(chips):
                index = flip(p, k) * 2 + 1 - c
                remote(
                    self.part(index),
                    self.part(index),
                    w_fs.at[self.slot, k],
                    w_rs.at[self.slot, index],
                    at_f(partner),
                ).wait_recv()
            if self.local:
                self.own().wait()

        def drain(self):
            for k in self.aimed + [0]:
                self.direct(k).wait_send()
            for k in range(1, chips):
                self.onward(k).wait_send()
            if self.plain:
                return
            for k in near:
                for other in far:
                    remote(
                        self.part(f),
                        self.part(f),
                        w_qs.at[self.slot, k + other],
                        w_rs.at[self.slot, f],
                        at_f(partner),
                    ).wait_send()

    class Line:
        def __init__(self, slot, buf, size=rows, parts=1, src=None):
            self.slot, self.buf, self.size, self.parts, self.src = slot, buf, size, parts, src

        def copy(self, index, side, h, own=False):
            piece = self.size // self.parts
            part = block(self.buf, index * self.parts + h, piece)
            src = part
            if own and self.src is not None:
                src = self.src.at[pl.ds(h * piece, piece)]
            where = d + 1 if side == 0 else d - 1
            return remote(
                src,
                part,
                z_ss.at[self.slot, side, h, index],
                z_rs.at[self.slot, h, index],
                at_d(where),
            )

        def start(self, h=0):
            @pl.when(d < n - 1)
            def _():
                self.copy(d, 0, h, True).start()

            @pl.when(d > 0)
            def _():
                self.copy(d, 1, h, True).start()

        def pass_on(self, index, side, h):
            copy = self.copy(index, side, h)
            copy.wait_recv()
            copy.start()

        def inward(self, s, h=0):
            @pl.when((d > 0) & (d < n // 2) & (d + s < n))
            def _():
                self.pass_on(d + s, 1, h)

            @pl.when((d < n - 1) & (d >= n // 2) & (d - s >= 0))
            def _():
                self.pass_on(d - s, 0, h)

        def outward(self, s, h=0):
            @pl.when((d < n // 2) & (d - s >= 0))
            def _():
                self.pass_on(d - s, 0, h)

            @pl.when((d >= n // 2) & (d + s < n))
            def _():
                self.pass_on(d + s, 1, h)

        def step(self, s, h=0):
            self.inward(s, h)
            self.outward(s, h)

        def arrive(self, s, h=0):
            @pl.when((d - s >= 0) & (d == n - 1))
            def _():
                self.copy(d - s, 0, h).wait_recv()

            @pl.when((d + s < n) & (d == 0))
            def _():
                self.copy(d + s, 1, h).wait_recv()

        def drain(self):
            for h in range(self.parts):
                for j in range(n):

                    @pl.when((j <= d) & (d < n - 1))
                    def _():
                        self.copy(j, 0, h).wait_send()

                    @pl.when((j >= d) & (d > 0))
                    def _():
                        self.copy(j, 1, h).wait_send()

    class Reduce:
        def __init__(self, slot, tile_of, sends, gets, also=None):
            self.slot, self.tile_of, self.sends, self.gets = slot, tile_of, sends, gets
            self.also = also

        def copy(self, index, where, slot, h):
            return remote(
                block(self.sends, 2 * index + h, half),
                block(self.gets, 2 * slot + h, half),
                rs_ss.at[self.slot, h, index],
                rs_rs.at[self.slot, h, slot],
                at_d(where),
            )

        def got(self, slot, h):
            part = block(self.gets, 2 * slot + h, half)
            remote(
                part, part, rs_ss.at[self.slot, h, 0], rs_rs.at[self.slot, h, slot], at_d(d)
            ).wait_recv()

        def right(self, index, h):
            return self.copy(index, d + 1, index, h)

        def left(self, index, h, last):
            return self.copy(index, d - 1, n if last else index, h)

        def compute(self, keep=True):
            def tile(t):
                value = self.tile_of(t, pl.ds(0, total))
                if keep:
                    wide_tile[...] = value
                    own_sum[:, cols(t)] = wide_tile[span(d, rows), :]
                self.sends[pl.ds(0, total), cols(t)] = value.astype(BF)

            loop(width // TILE, tile)

        def pair(self):
            first = d - 1 + low

            def tile(t):
                value = self.tile_of(t, pl.ds(pl.multiple_of(first * rows, rows), 2 * rows))
                wide_tile[0 : 2 * rows, :] = value
                own_sum[:, cols(t)] = wide_tile[span(1 - low, rows), :]
                self.sends[span(inner, rows), cols(t)] = wide_tile[span(low, rows), :].astype(BF)
                if self.also is not None:
                    self.also(t, value, pl.ds(pl.multiple_of(first * rows, rows), 2 * rows))

            loop(width // TILE, tile)

        def single(self, j):
            def tile(t):
                value = self.tile_of(t, span(j, rows))
                self.sends[span(j, rows), cols(t)] = value.astype(BF)
                if self.also is not None:
                    self.also(t, value, span(j, rows))

            loop(width // TILE, tile)

        def send_at(self, s):
            @pl.when(d == 0)
            def _():
                for h in range(2):
                    self.right(d + s, h).start()

            @pl.when(d == n - 1)
            def _():
                for h in range(2):
                    self.left(d - s, h, s == 1).start()

        def add_right(self, index, h):
            self.add_into(index, h)
            self.right(index, h).start()

        def add_left(self, index, h, last):
            self.add_into(index, h)
            self.left(index, h, last).start()

        def out_adv(self, s, h):
            @pl.when((d > 0) & (d < n // 2) & (d + s < n))
            def _():
                self.add_right(d + s, h)

            @pl.when((d < n - 1) & (d >= n // 2) & (d - s >= 0))
            def _():
                self.add_left(d - s, h, s == 1)

        def in_adv(self, s, h):
            @pl.when((d < n // 2) & (d - s >= 0))
            def _():
                self.add_left(d - s, h, s == 1)

            @pl.when((d >= n // 2) & (d + s < n))
            def _():
                self.add_right(d + s, h)

        def launch(self, halves_first):
            order = [(s, h) for h in range(2) for s in range(n - 1, 0, -1)]
            if not halves_first:
                order = [(s, h) for s in range(n - 1, 0, -1) for h in range(2)]

            @pl.when(d == 0)
            def _():
                for s, h in order:
                    self.right(d + s, h).start()

            @pl.when(d == n - 1)
            def _():
                for s, h in order:
                    self.left(d - s, h, s == 1).start()

        def add_into(self, index, h):
            self.got(index, h)

            def some(i):
                r = pl.ds(pl.multiple_of(index * rows + h * half + i * CHUNK, CHUNK), CHUNK)
                self.sends[r, :] = (
                    self.sends[r, :].astype(F32) + self.gets[r, :].astype(F32)
                ).astype(BF)

            loop(half // CHUNK, some)

        def advance(self, s, h):
            right, left = d + s, d - s

            @pl.when((right < n) & (d > 0))
            def _():
                self.add_into(right, h)
                self.right(right, h).start()

            @pl.when((left >= 0) & (d < n - 1))
            def _():
                self.add_into(left, h)
                self.left(left, h, s == 1).start()

        def final(self, h):
            self.final_into(own_sum, h)

        def final_into(self, acc, h):
            def add(slot):
                self.got(slot, h)

                def some(i):
                    r = pl.ds(pl.multiple_of(h * half + i * CHUNK, CHUNK), CHUNK)
                    there = pl.ds(
                        pl.multiple_of(slot * rows + h * half + i * CHUNK, CHUNK), CHUNK
                    )
                    acc[r, :] = acc[r, :] + self.gets[there, :].astype(F32)

                loop(half // CHUNK, some)

            @pl.when(d > 0)
            def _():
                add(d)

            @pl.when(d < n - 1)
            def _():
                add(n)

        def drain(self):
            for h in range(2):
                for j in range(n):

                    @pl.when(d != j)
                    def _():
                        self.copy(j, d, j, h).wait_send()

    def tiles(wide, body):
        if wide % TILE == 0:
            loop(wide // TILE, lambda t: body(cols(t)))
        else:
            for start in range(0, wide, TILE):
                body(pl.ds(start, min(TILE, wide - start)))

    handing = []

    class Grad:
        def __init__(self, group, turned, terms, emit):
            self.group, self.turned, self.terms, self.emit = group, turned, terms, emit
            self.width = gwidths[group]

        def hand_over(self):
            src = send_b if self.width == widest else send_b.at[:, :, pl.ds(0, self.width)]
            return remote(
                src,
                from_partner[self.group],
                b_ss.at[self.group],
                b_rs.at[self.group],
                at_f(partner),
            )

        def ship(self, k):
            chip = flip(p, k)
            return remote(
                sums[self.group].at[chip],
                landing[self.group].at[k - 1],
                i_ss.at[self.group, k - 1],
                i_rs.at[self.group, k - 1],
                at_f(chip * 2 + c),
            )

        def blocks_of(self, core, lanes):
            left = jnp.concatenate(
                [self.turned[span(q * 2 + core, shard), :] for q in range(chips)], axis=0
            )
            value = mm(left, self.terms[:, lanes])
            return [value[q * shard : (q + 1) * shard] for q in range(chips)]

        def release(self):
            self.hand_over().wait_send()

        def send_all(self):
            if handing:
                handing.pop().release()

            def tile(lanes):
                for q, value in enumerate(self.blocks_of(1 - c, lanes)):
                    send_b[q, :, lanes] = value.astype(BF)

            tiles(self.width, tile)
            self.hand_over().start()
            handing.append(self)

        def own_sums(self):
            self.hand_over().wait_recv()

            def tile(lanes):
                for q, value in enumerate(self.blocks_of(c, lanes)):
                    other = from_partner[self.group][q, :, lanes].astype(F32)
                    sums[self.group][q, :, lanes] = (value + other).astype(BF)

            tiles(self.width, tile)

        def ship_all(self):
            for k in range(1, chips):
                self.ship(k).start()

        def own_all(self):
            self.own_sums()
            self.ship_all()

        def fetch(self, k):
            return pltpu.make_async_copy(
                landing[self.group].at[k - 1],
                stage.at[k - 1, :, pl.ds(0, self.width)],
                l_sem.at[k - 1],
            )

        def collect(self):
            for k in range(1, chips):
                self.ship(k).wait()
                if self.group >= 2:
                    self.fetch(k).start()

        def finish(self):
            if self.group >= 2:
                for k in range(1, chips):
                    self.fetch(k).wait()

            def parts(lanes):
                yield sums[self.group][p, :, lanes]
                for k in range(1, chips):
                    if self.group >= 2:
                        yield stage[k - 1, :, lanes]
                    else:
                        yield landing[self.group][k - 1, :, lanes]

            self.emit(parts)

    def total_of(values):
        result = None
        for value in values:
            result = value if result is None else result + value
        return result

    stores = []

    def store(src, dst):
        copy = pltpu.make_async_copy(src, dst, out_sem.at[len(stores)])
        copy.start()
        stores.append(copy)

    def emit_plain(out):
        def emit(parts):
            def tile(t):
                big_own[:, cols(t)] = total_of(v.astype(F32) for v in parts(cols(t)))

            if big_stores:
                big_stores.pop().wait()
            loop(ff // TILE, tile)
            copy = pltpu.make_async_copy(big_own, out, l_sem.at[chips - 1])
            copy.start()
            big_stores.append(copy)

        return emit

    big_stores = []

    def summed(parts, start, size):
        return total_of(v.astype(F32) for v in parts(pl.ds(start, size)))

    q_real, kv_real = nq * HD, nkv * HD

    def emit_out(parts):
        o_own[...] = summed(parts, 0, q_real)
        store(o_own, out_o)

    def emit_qkv(parts):
        q_own[...] = summed(parts, 0, q_real)
        store(q_own, out_q)
        k_own[...] = summed(parts, q_real, kv_real)
        store(k_own, out_k)
        v_own[...] = summed(parts, q_real + kv_real, kv_real)
        store(v_own, out_v)

    def fill(dst, r, value):
        spare = dst.shape[1] - value.shape[1]
        if spare:
            value = jnp.concatenate([value, jnp.zeros((value.shape[0], spare), F32)], axis=1)
        dst[r, :] = value.astype(BF)

    def pack_mixed():
        def one(b):
            r = span(b, rows)
            fill(mixed_pack, r, mm_nt(mixed[r, :], pick_end[...]))

        loop(n, one)

    def pack_gqkv():
        def one(b):
            r = span(b, rows)
            keys = slice(q_wide, q_wide + kv_wide)
            vals = slice(q_wide + kv_wide, q_wide + 2 * kv_wide)
            value = jnp.concatenate(
                [
                    mm_nt(gqkv[r, 0:q_wide], pick_rope[...]),
                    mm_nt(gqkv[r, keys], pick_rope[0:kv_real, 0:kv_wide]),
                    mm_nt(gqkv[r, vals], pick_end[0:kv_real, 0:kv_wide]),
                ],
                axis=1,
            )
            fill(gqkv_pack, r, value)

        loop(n, one)

    def turn(src, dst):
        def lane_block(t):
            dst[cols(t, LANES), :] = src[pl.ds(0, total), cols(t, LANES)].T

        loop(width // LANES, lane_block)

    def at(s, work):
        if s == 0:
            work(d)
            return

        def side(i):
            j = d - s + 2 * s * i

            @pl.when((j >= 0) & (j < n))
            def _():
                work(j)

        loop(2, side)

    def one_hot(split):
        shape = (nq * HD, q_wide)
        row = lax.broadcasted_iota(jnp.int32, shape, 0)
        lane = lax.broadcasted_iota(jnp.int32, shape, 1)
        inside = lane % LANES
        start = (lane // LANES) * HD
        if split:
            gap = LANES // 2 - HALF
            upper = inside >= LANES // 2
            source = start + jnp.where(upper, inside - gap, inside)
            real = (inside % (LANES // 2)) < HALF
        else:
            source = start + inside
            real = inside < HD
        return jnp.where(real & (row == source), 1.0, 0.0).astype(BF)

    pick_rope[...] = one_hot(True)
    pick_end[...] = one_hot(False)
    gain_mine = block(gain_in, f, 8)
    gain_mine[...] = jnp.zeros(gain_mine.shape, F32)
    gain_mine[0:1, 0:shard] = gain_a[...].astype(F32)
    gain_mine[1:2, 0:shard] = gain_m[...].astype(F32)

    gathers = [
        Gather(0, weights[0], shard, plain=True),
        Gather(1, weights[1], shard, plain=True),
        Gather(2, weights[2], shard, w_g),
        Gather(3, weights[3], shard, w_u),
        Gather(4, weights[4], shard, w_d),
    ]
    gain_gather = Gather(5, gain_in, 8, plain=True)
    tok_line = Line(0, x_buf, parts=2, src=tokens)
    cot_line = Line(1, ct_buf, src=cot)
    mi_line = Line(2, mi_buf, parts=2)
    gm_line = Line(3, gm_buf, parts=2)

    def gain_swap(k):
        mine = block(gain_z, d, 8)
        return remote(
            mine, mine, z_ss.at[4, 0, 0, k], z_rs.at[4, 0, d], at_d((d + k) % n)
        )

    def gain_got(k):
        other = (d + k) % n
        part = block(gain_z, other, 8)
        remote(part, part, z_ss.at[4, 0, 0, k], z_rs.at[4, 0, other], at_d(d)).wait_recv()

    def segments(b, shape, dim):
        index = lax.broadcasted_iota(jnp.int32, shape, dim)
        segment = jnp.zeros(shape, jnp.int32)
        offset = jnp.zeros(shape, jnp.int32)
        end = jnp.int32(0)
        for k in range(nseq):
            end = end + lengths[b, k]
            past = index >= end
            segment = segment + past.astype(jnp.int32)
            offset = jnp.where(past, end, offset)
        return index, segment, offset

    def tables(b):
        index, _, offset = segments(b, (rows, LANES), 0)
        angle = (index - offset).astype(F32) * freq[...]
        lane = lax.broadcasted_iota(jnp.int32, (rows, LANES), 1)
        sine = jnp.sin(angle)
        block(cos_t, b)[...] = jnp.cos(angle)
        block(sin_t, b)[...] = jnp.where(lane < LANES // 2, -sine, sine)

    pl.semaphore_wait(barrier, chips + n - 1)
    for h in range(2):
        tok_line.start(h)

    @pl.when(end)
    def _():
        cot_line.start()

    gain_gather.start()
    mine = span(f, shard)
    kv_rows = nkv * HD
    for copy in loads[:4]:
        copy.wait()
    weights[0][mine, 0:q_wide] = mm(q_in[...], pick_rope[...]).astype(BF)
    weights[0][mine, q_wide : q_wide + kv_wide] = mm(
        k_in[...], pick_rope[0:kv_rows, 0:kv_wide]
    ).astype(BF)
    weights[0][mine, q_wide + kv_wide : q_wide + 2 * kv_wide] = mm(
        v_in[...], pick_end[0:kv_rows, 0:kv_wide]
    ).astype(BF)
    gathers[0].start()
    weights[1][mine, :] = mm(o_in[...], pick_end[...]).astype(BF)
    for g in range(1, 5):
        gathers[g].start()
    loop(n, tables)
    loads[4].wait()
    gain_gather.forward()
    gain_gather.finish()
    for k in range(nf):
        gain_row[:, k * shard : (k + 1) * shard] = gain_in[8 * k : 8 * k + 8, 0:shard]

    def rms(value):
        mean = jnp.sum(value * value, axis=-1, keepdims=True) / width
        return lax.rsqrt(mean + EPSILON)

    def norm_one(j):
        def some(i):
            r = pl.ds(pl.multiple_of(j * rows + i * CHUNK, CHUNK), CHUNK)
            value = x_buf[r, :].astype(F32)
            scale = rms(value)
            sc_one[r, :] = scale
            mi_buf[r, :] = (value * scale * gain_row[0:1, :]).astype(BF)

        loop(rows // CHUNK, some)

    def rope(value, sign, cos_v, sin_v):
        return value * cos_v + sign * (pltpu.roll(value, LANES // 2, 1) * sin_v)

    heads = nq + 2 * nkv

    def head(ref, r, h):
        return ref[r, h * LANES : (h + 1) * LANES]

    def attend(b):
        r = span(b, rows)
        cos_v, sin_v = cos_t[r, :], sin_t[r, :]
        for t in range(heads // 2):
            both = mm(mi_buf[r, :], weights[0][:, 2 * t * LANES : 2 * (t + 1) * LANES])
            for h in (2 * t, 2 * t + 1):
                value = both[:, (h - 2 * t) * LANES : (h - 2 * t + 1) * LANES]
                if h < nq + nkv:
                    value = rope(value, 1.0, cos_v, sin_v)
                qkv[r, h * LANES : (h + 1) * LANES] = value.astype(BF)
        t_index, t_seg, _ = segments(b, (rows, rows), 0)
        s_index, s_seg, _ = segments(b, (rows, rows), 1)
        allowed = (t_seg == s_seg) & (s_index <= t_index)
        for h in range(nq):
            kv = h // (nq // nkv)
            score = mm_nt(head(qkv, r, h), head(qkv, r, nq + kv)) * HD ** (-0.5)
            score = jnp.where(allowed, score, NEG_FILL)
            top = jnp.max(score, axis=-1, keepdims=True)
            log_total = top + jnp.log(jnp.sum(jnp.exp(score - top), axis=-1, keepdims=True))
            prob = jnp.where(allowed, jnp.exp(score - log_total), 0.0)
            probs[b * nq + h] = prob
            mixed[r, h * LANES : (h + 1) * LANES] = mm(
                prob.astype(BF), head(qkv, r, nq + nkv + kv)
            ).astype(BF)

    def tokens_at(s):
        for h in range(2):
            tok_line.step(s, h)
            tok_line.arrive(s, h)

    norm_one(d)
    tokens_at(1)
    at(1, norm_one)
    early = min(2, n - 1)
    if early == 2:
        for h in range(2):
            tok_line.step(2, h)

    @pl.when((d > 0) & (d < n - 1))
    def _():
        cot_line.start()

    gathers[0].forward()
    if early == 2:
        for h in range(2):
            tok_line.arrive(2, h)
        at(2, norm_one)
    gathers[0].finish()
    for s in range(early + 1):
        at(s, attend)
    gathers[1].forward()
    cot_line.outward(1)
    for s in range(early + 1, n):
        tokens_at(s)
        at(s, norm_one)
        at(s, attend)
    gathers[1].finish()

    def by_turned(pairs):
        def tile_of(t, r):
            return total_of(mm_nt(left[r, :], weight[cols(t), :]) for left, weight in pairs)

        return tile_of

    def run(work):
        if work:
            todo = work.pop(0)
            if todo is not None:
                todo()

    def reduce_then_gather(red, finish_half, line, work):
        red.compute()
        red.launch(True)
        run(work)
        for s in range(n - 2, 0, -1):
            red.advance(s, 0)
            run(work)
        red.final(0)
        finish_half(0)
        line.start(0)
        run(work)
        for i in range(1, n - 1):
            red.advance(n - 1 - i, 1)
            if i == 1:
                line.inward(i, 0)
            run(work)
        red.final(1)
        finish_half(1)
        line.start(1)
        for i in range(1, n - 1):
            if i > 1:
                line.inward(i, 0)
            line.outward(i, 0)

    def arrived(line, s):
        line.step(s, 1)
        line.arrive(s, 0)
        line.arrive(s, 1)

    def norm_two(h):
        def some(i):
            r = pl.ds(pl.multiple_of(h * half + i * CHUNK, CHUNK), CHUNK)
            here = pl.ds(pl.multiple_of(d * rows + h * half + i * CHUNK, CHUNK), CHUNK)
            value = x_buf[here, :].astype(F32) + own_sum[r, :]
            scale = rms(value)
            middle[r, :] = value
            sc_two[r, :] = scale
            mi_buf[here, :] = (value * scale * gain_row[1:2, :]).astype(BF)

        loop(half // CHUNK, some)

    def both(*todo):
        def do():
            for one in todo:
                one()

        return do

    def cot_on(s):
        def do():
            cot_line.inward(s)
            if s > 1:
                cot_line.outward(s)

        return do

    after_attn = Reduce(0, by_turned([(mixed, weights[1])]), s_buf, r_buf)
    work = [cot_on(1)]
    work += [both(cot_on(2), gathers[2].relay)] if n > 2 else [gathers[2].relay]
    work += [gathers[3].relay, None, gathers[4].relay, gathers[2].forward]
    work += [cot_on(s) for s in range(3, n - 1)]
    reduce_then_gather(after_attn, norm_two, mi_line, work)
    while work:
        run(work)
    pack_mixed()
    gathers[3].forward()
    gathers[4].forward()
    for g in (2, 3, 4):
        gathers[g].finish()
    loads[5].wait()
    loads[6].wait()

    def feed(j):
        r = span(j, rows)

        def tile(t):
            left = mi_buf[r, :]
            gate = mm(left, weights[2][:, cols(t)])
            up = mm(left, weights[3][:, cols(t)])
            grad_hidden = mm(ct_buf[r, :], weights[4][:, cols(t)])
            sig = 1.0 / (1.0 + jnp.exp(-gate))
            hid[r, cols(t)] = (gate * sig * up).astype(BF)
            gu[r, cols(t)] = (grad_hidden * gate * sig).astype(BF)
            gg[r, cols(t)] = (grad_hidden * up * sig * (1.0 + gate * (1.0 - sig))).astype(BF)

        loop(ff // TILE, tile)

    def at_outer(work):
        @pl.when((outer >= 0) & (outer < n))
        def _():
            work(outer)

    after_mlp = Reduce(1, by_turned([(gg, weights[2]), (gu, weights[3])]), s_buf, r_buf)
    after_attn.drain()
    at(0, feed)
    mi_line.step(1, 1)
    for s in range(1, n):
        for h in range(2):
            mi_line.arrive(s, h)
        cot_line.arrive(s)
        at(s, feed)
        if s + 1 < n:
            mi_line.step(s + 1, 1)
        if s == 1:
            after_mlp.pair()
            after_mlp.send_at(1)
            at_outer(after_mlp.single)
        else:
            at(s, after_mlp.single)
            after_mlp.send_at(s)

    gain_own[...] = jnp.zeros((8, width), F32)

    def back_two(h):
        def some(i):
            r = pl.ds(pl.multiple_of(h * half + i * CHUNK, CHUNK), CHUNK)
            term = own_sum[r, :]
            scale = sc_two[r, :]
            normed = middle[r, :] * scale
            gain_sum = jnp.sum(term * normed, axis=0, keepdims=True)
            dn = term * gain_row[1:2, :]
            mean = jnp.sum(dn * normed, axis=-1, keepdims=True) / width
            here = pl.ds(pl.multiple_of(d * rows + h * half + i * CHUNK, CHUNK), CHUNK)
            value = cot_own[r, :].astype(F32) + scale * (dn - normed * mean)
            gmid[r, :] = value
            gm_buf[here, :] = value.astype(BF)
            gain_own[1:2, :] = gain_own[1:2, :] + gain_sum

        loop(half // CHUNK, some)

    down = Grad(4, t_one, hid, emit_plain(out_d))
    gate_g = Grad(2, t_two, gg, emit_plain(out_g))
    up_g = Grad(3, t_two, gu, emit_plain(out_u))

    def turn_mi():
        turn(mi_buf, t_two)

    def attn_in_again(j):
        def some(i):
            r = pl.ds(pl.multiple_of(j * rows + i * CHUNK, CHUNK), CHUNK)
            value = x_buf[r, :].astype(F32) * sc_one[r, :]
            s_buf[r, :] = (value * gain_row[0:1, :]).astype(BF)

        loop(rows // CHUNK, some)

    output = Reduce(2, by_turned([(hid, weights[4])]), ct_buf, r_two)

    def finish_mlp():
        for h in range(2):
            after_mlp.final(h)
            back_two(h)
            if h == 0:
                gm_line.start(h)

    turn(ct_buf, t_one)
    cot_line.drain()
    turn_mi()
    down.send_all()
    for h in range(2):
        after_mlp.out_adv(1, h)
    output.compute(keep=False)
    for s in range(n - 1, 1, -1):
        output.send_at(s)
    if n == 2:
        output.send_at(1)
    down.own_all()
    for s in range(2, n - 1):
        for h in range(2):
            after_mlp.out_adv(s, h)

    @pl.when(jnp.logical_not(end))
    def _():
        finish_mlp()

    gate_g.send_all()
    for s in range(1, n - 1):
        for h in range(2):
            after_mlp.in_adv(s, h)

    @pl.when(jnp.logical_not(end))
    def _():
        gm_line.start(1)

    for h in range(2):
        gm_line.inward(1, h)
    gate_g.own_all()
    up_g.send_all()
    gm_line.outward(1, 0)
    up_g.own_all()
    gm_line.outward(1, 1)

    @pl.when(end)
    def _():
        finish_mlp()
        gm_line.start(1)

    after_mlp.drain()
    mi_line.drain()

    def back(b):
        r = span(b, rows)

        def tile(t):
            gmixed[r, cols(t)] = mm(gm_buf[r, :], weights[1][:, cols(t)]).astype(BF)

        loop(q_wide // TILE, tile)
        cos_v, sin_v = cos_t[r, :], sin_t[r, :]
        group = nq // nkv
        for kv in range(nkv):
            key, val = head(qkv, r, nq + kv), head(qkv, r, nq + nkv + kv)
            grad_k = grad_v = None
            for h in range(kv * group, (kv + 1) * group):
                query, gm_h = head(qkv, r, h), head(gmixed, r, h)
                prob = probs[b * nq + h]
                delta = jnp.sum(
                    gm_h.astype(F32) * head(mixed, r, h).astype(F32), axis=-1, keepdims=True
                )
                grad_p = mm_nt(gm_h, val)
                grad_s = (prob * (grad_p - delta) * HD ** (-0.5)).astype(BF)
                grad_q = mm(grad_s, key)
                gqkv[r, h * LANES : (h + 1) * LANES] = rope(grad_q, -1.0, cos_v, sin_v).astype(BF)
                k_term, v_term = mm_tn(grad_s, query), mm_tn(prob.astype(BF), gm_h)
                grad_k = k_term if grad_k is None else grad_k + k_term
                grad_v = v_term if grad_v is None else grad_v + v_term
            k_at, v_at = (nq + kv) * LANES, (nq + nkv + kv) * LANES
            gqkv[r, k_at : k_at + LANES] = rope(grad_k, -1.0, cos_v, sin_v).astype(BF)
            gqkv[r, v_at : v_at + LANES] = grad_v.astype(BF)

    def add_gain(t, value, r):
        normed = x_buf[r, cols(t)].astype(F32) * sc_one[r, :]
        gain_own[0:1, cols(t)] = gain_own[0:1, cols(t)] + jnp.sum(
            value * normed, axis=0, keepdims=True
        )

    after_in = Reduce(3, by_turned([(gqkv, weights[0])]), s_buf, r_buf, add_gain)
    out_g_grad = Grad(1, t_one, mixed_pack, emit_out)
    qkv_g = Grad(0, t_two, gqkv_pack, emit_qkv)

    def pass_gm(h):
        for s in range(2, n - 1):
            gm_line.inward(s, h)
            gm_line.outward(s, h)

    at(0, back)
    pass_gm(0)
    for h in range(2):
        gm_line.arrive(1, h)
    back(inner)
    pass_gm(1)
    for s in range(n - 2, 1, -1):
        for h in range(2):
            output.out_adv(s, h)
    loop(n, attn_in_again)
    turn(s_buf, t_two)
    after_in.pair()
    after_in.send_at(1)
    if n > 2:
        for h in range(2):
            output.out_adv(1, h)

    def outer_back(j):
        back(j)
        after_in.single(j)

    at_outer(outer_back)
    for s in range(2, n):
        for h in range(2):
            gm_line.arrive(s, h)
        at(s, outer_back)
        if s < n - 1:
            after_in.send_at(s)
    quarter = width // 4
    gain_mine = block(gain_z, d, 8)
    for i in range(8):
        gain_mine[i : i + 1, :] = gain_own[i // 4 : i // 4 + 1, pl.ds(i % 4 * quarter, quarter)]
    for k in range(1, n):
        gain_swap(k).start()
    if n > 2:
        after_in.send_at(n - 1)
        output.send_at(1)
    for s in range(1, n - 1):
        for h in range(2):
            output.in_adv(s, h)
    turn(gm_buf, t_one)
    out_g_grad.send_all()
    pack_gqkv()
    out_g_grad.own_all()
    qkv_g.send_all()
    for h in range(2):
        after_in.out_adv(n - 2, h)
    qkv_g.own_sums()
    for k in range(1, n):
        gain_got(k)
    block(gain_f, f, 8)[...] = total_of(gain_z[8 * k : 8 * k + 8, :] for k in range(n))
    gain_back = Gather(6, gain_f, 8, plain=True)
    gain_back.start()
    qkv_g.ship_all()
    for s in range(n - 3, 0, -1):
        for h in range(2):
            after_in.out_adv(s, h)

    def output_end():
        middle[...] = middle[...] + block(ct_buf, d)[...].astype(F32)
        for h in range(2):
            output.final_into(middle, h)
        out_own[...] = middle[...].astype(BF)
        store(out_own, out_ref)

    def gain_end():
        gain_back.forward()
        gain_back.finish()
        gain_all = total_of(gain_f[8 * k : 8 * k + 8, :] for k in range(nf))
        for i in range(8):
            gain_own[i // 4 : i // 4 + 1, pl.ds(i % 4 * quarter, quarter)] = gain_all[i : i + 1, :]
        gain_all = pltpu.roll(gain_own[...], (width - f * shard) % width, 1)
        out_ga[...] = gain_all[0:1, 0:shard]
        out_gm[...] = gain_all[1:2, 0:shard]

    work = [gain_end]
    for grad in (down, gate_g, up_g):
        work.append(both(grad.collect, grad.finish))
    for s in range(1, n - 1):
        for h in range(2):
            after_in.in_adv(s, h)
    while work:
        run(work)

    def back_one(h):
        def some(i):
            r = pl.ds(pl.multiple_of(h * half + i * CHUNK, CHUNK), CHUNK)
            there = pl.ds(pl.multiple_of(d * rows + h * half + i * CHUNK, CHUNK), CHUNK)
            scale = sc_one[there, :]
            normed = x_buf[there, :].astype(F32) * scale
            dm = own_sum[r, :] * gain_row[0:1, :]
            mean = jnp.sum(dm * normed, axis=-1, keepdims=True) / width
            gmid[r, :] = gmid[r, :] + scale * (dm - normed * mean)

        loop(half // CHUNK, some)

    for h in range(2):
        after_in.final(h)
        back_one(h)
        part = pl.ds(h * half, half)
        store(gmid.at[part], gtok_ref.at[part])
    output_end()
    for grad in (qkv_g, out_g_grad):
        grad.collect()
        grad.finish()

    handing.pop().release()
    output.drain()
    after_in.drain()
    tok_line.drain()
    gm_line.drain()
    for k in range(1, n):
        gain_swap(k).wait_send()
    for gather in gathers + [gain_gather, gain_back]:
        gather.drain()
    big_stores.pop().wait()
    for copy in stores:
        copy.wait()


def pass_on(*refs):
    count = (len(refs) - 2) // 3
    srcs, dsts, held = refs[:count], refs[count : 2 * count], refs[2 * count : 3 * count]
    in_sem, out_sem = refs[3 * count :]
    order = range(count)
    for i in order:
        pltpu.make_async_copy(srcs[i], held[i], in_sem.at[i]).start()
    for i in order:
        pltpu.make_async_copy(srcs[i], held[i], in_sem.at[i]).wait()
        pltpu.make_async_copy(held[i], dsts[i], out_sem.at[i]).start()
    for i in order:
        pltpu.make_async_copy(held[i], dsts[i], out_sem.at[i]).wait()


def run_layer(lengths, freq, tokens, cot, gain_a, gain_m, w_q, w_k, w_v, w_o, w_d, w_g, w_u, n, chips):
    rows, width = tokens.shape
    nq = w_q.shape[1] // HD
    nkv = w_k.shape[1] // HD
    total = n * rows
    nf = 2 * chips
    shard = w_q.shape[0]
    ff = w_g.shape[1]
    q_wide, kv_wide = nq * LANES, nkv * LANES
    widths = (q_wide + 2 * kv_wide, q_wide, ff, ff, ff)
    dims = (n, chips, rows, width, nq, nkv, ff, lengths.shape[1])
    vmem = pl.BlockSpec(memory_space=pltpu.VMEM)
    hbm = pl.BlockSpec(memory_space=pltpu.HBM)
    results = [
        jax.ShapeDtypeStruct((rows, width), BF),
        jax.ShapeDtypeStruct((rows, width), F32),
        jax.ShapeDtypeStruct((1, shard), F32),
        jax.ShapeDtypeStruct((1, shard), F32),
    ] + [jax.ShapeDtypeStruct(w.shape, F32) for w in (w_q, w_k, w_v, w_o, w_g, w_u, w_d)]
    out_shape = results + [jax.ShapeDtypeStruct((chips - 1, shard, w), BF) for w in widths[2:]]
    gwidths = packed_widths(nq, nkv, ff)
    widest = max(gwidths)
    scratch = (
        [pltpu.VMEM((chips - 1, shard, w), BF) for w in gwidths[:2]]
        + [pltpu.VMEM((width, w), BF) for w in widths]
        + [
            pltpu.VMEM((total, width), BF),
            pltpu.VMEM((total, width), BF),
            pltpu.VMEM((total, width), BF),
            pltpu.VMEM((total, width), BF),
            pltpu.VMEM((total + rows, width), BF),
            pltpu.VMEM((rows, width), BF),
            pltpu.VMEM((total, widths[0]), BF),
            pltpu.VMEM((total, widths[0]), BF),
            pltpu.VMEM((n * nq, rows, rows), F32),
            pltpu.VMEM((total, q_wide), BF),
            pltpu.VMEM((total, q_wide), BF),
            pltpu.VMEM((total, ff), BF),
            pltpu.VMEM((total, ff), BF),
            pltpu.VMEM((total, ff), BF),
            pltpu.VMEM((total, gwidths[0]), BF),
            pltpu.VMEM((total, gwidths[1]), BF),
            pltpu.VMEM((width, total), BF),
            pltpu.VMEM((width, total), BF),
            pltpu.VMEM((total, width), BF),
            pltpu.VMEM((total + rows, width), BF),
            pltpu.VMEM((rows, width), F32),
            pltpu.VMEM((rows, width), F32),
            pltpu.VMEM((rows, width), F32),
            pltpu.VMEM((total, TILE), F32),
            pltpu.VMEM((total, 1), F32),
            pltpu.VMEM((rows, 1), F32),
            pltpu.VMEM((total, LANES), F32),
            pltpu.VMEM((total, LANES), F32),
            pltpu.VMEM((nf * 8, -(-shard // LANES) * LANES), F32),
            pltpu.VMEM((8, width), F32),
            pltpu.VMEM((8, width), F32),
            pltpu.VMEM((n * 8, width // 4), F32),
            pltpu.VMEM((nf * 8, width // 4), F32),
            pltpu.VMEM((chips - 1, shard, widest), BF),
            pltpu.VMEM((nq * HD, q_wide), BF),
            pltpu.VMEM((nq * HD, q_wide), BF),
        ]
        + [pltpu.VMEM(w.shape, BF) for w in (w_q, w_k, w_v, w_o)]
        + [pltpu.VMEM((rows, width), BF)]
        + [pltpu.VMEM(w.shape, F32) for w in (w_q, w_k, w_v, w_o, w_g)]
        + [
            pltpu.VMEM((chips, shard, widest), BF),
        ]
        + [pltpu.VMEM((chips, shard, w), BF) for w in gwidths]
        + [pltpu.VMEM((chips, shard, w), BF) for w in gwidths]
        + [
            pltpu.SemaphoreType.DMA((7, chips)),
            pltpu.SemaphoreType.DMA((7, chips)),
            pltpu.SemaphoreType.DMA((7, chips)),
            pltpu.SemaphoreType.DMA((7, nf)),
            pltpu.SemaphoreType.DMA((7,)),
            pltpu.SemaphoreType.DMA((5, 2, 2, n)),
            pltpu.SemaphoreType.DMA((5, 2, n)),
            pltpu.SemaphoreType.DMA((4, 2, n)),
            pltpu.SemaphoreType.DMA((4, 2, n + 1)),
            pltpu.SemaphoreType.DMA((5,)),
            pltpu.SemaphoreType.DMA((5,)),
            pltpu.SemaphoreType.DMA((5, chips)),
            pltpu.SemaphoreType.DMA((5, chips)),
            pltpu.SemaphoreType.DMA((chips,)),
            pltpu.SemaphoreType.DMA((7,)),
            pltpu.SemaphoreType.DMA((7,)),
        ]
    )
    made = pl.pallas_call(
        partial(layer_kernel, dims),
        out_shape=out_shape,
        in_specs=[pl.BlockSpec(memory_space=pltpu.SMEM)] + [vmem] * 3 + [hbm] * 9,
        out_specs=[hbm] * 2 + [vmem] * 2 + [hbm] * 10,
        scratch_shapes=scratch,
        compiler_params=pltpu.CompilerParams(
            collective_id=0, has_side_effects=True, vmem_limit_bytes=67043328
        ),
        name="layer",
    )(lengths, freq, gain_a, gain_m, tokens, cot, w_q, w_k, w_v, w_o, w_d, w_g, w_u)
    count = len(results)
    return pl.pallas_call(
        pass_on,
        out_shape=results,
        in_specs=[hbm] * count,
        out_specs=[hbm] * count,
        scratch_shapes=[pltpu.VMEM(r.shape, r.dtype) for r in results]
        + [pltpu.SemaphoreType.DMA((count,)), pltpu.SemaphoreType.DMA((count,))],
        compiler_params=pltpu.CompilerParams(vmem_limit_bytes=67043328),
        name="results",
    )(*made[:count])


def body(
    n,
    chips,
    tokens,
    lengths,
    cotangent,
    attn_gain,
    w_query,
    w_key,
    w_value,
    w_out,
    mlp_gain,
    w_gate,
    w_up,
    w_down,
):
    frequency = ROPE_BASE ** (-jnp.arange(HALF, dtype=F32) / HALF)
    frequency = jnp.pad(frequency, (0, LANES // 2 - HALF))
    freq = jnp.concatenate([frequency, frequency])[None, :]
    results = run_layer(
        lengths,
        freq,
        tokens,
        cotangent,
        attn_gain,
        mlp_gain,
        w_query[0],
        w_key[0],
        w_value[0],
        w_out[0].T,
        w_down[0].T,
        w_gate[0],
        w_up[0],
        n,
        chips,
    )
    output, grad_tokens, g_again, g_mgain, g_q, g_k, g_v, g_o, g_gate, g_up, g_down = results
    return (
        output,
        grad_tokens,
        g_again,
        g_q[None],
        g_k[None],
        g_v[None],
        g_o.T[None],
        g_mgain,
        g_gate[None],
        g_up[None],
        g_down.T[None],
    )


def solution(mesh):
    placed = (
        P(("fsdp", "dp"), None),
        P("fsdp", None),
        P(("fsdp", "dp"), None),
        P(None, "fsdp"),
        P(None, "fsdp", "dp"),
        P(None, "fsdp", "dp"),
        P(None, "fsdp", "dp"),
        P(None, "dp", "fsdp"),
        P(None, "fsdp"),
        P(None, "fsdp", "dp"),
        P(None, "fsdp", "dp"),
        P(None, "dp", "fsdp"),
    )
    return jax.shard_map(
        partial(body, mesh.shape["dp"], mesh.shape["fsdp"] // 2),
        mesh=mesh,
        in_specs=placed,
        out_specs=(
            P(("fsdp", "dp"), None),
            P(("fsdp", "dp"), None),
            P(None, "fsdp"),
            P(None, "fsdp", "dp"),
            P(None, "fsdp", "dp"),
            P(None, "fsdp", "dp"),
            P(None, "dp", "fsdp"),
            P(None, "fsdp"),
            P(None, "fsdp", "dp"),
            P(None, "fsdp", "dp"),
            P(None, "dp", "fsdp"),
        ),
        check_vma=False,
    )
```

```python
from functools import partial

import jax
import jax.numpy as jnp
from jax import lax
from jax.experimental import pallas as pl
from jax.experimental.pallas import tpu as pltpu
from jax.sharding import PartitionSpec as P

HD = 96
HALF = 48
LANES = 128
EPSILON = 1e-05
ROPE_BASE = 100000.0
NEG_FILL = -1e30
MESH = pl.DeviceIdType.MESH
BF = jnp.bfloat16
F32 = jnp.float32
TILE = 256
CHUNK = 32


def mm(left, right):
    return jnp.dot(left, right, preferred_element_type=F32)


def mm_nt(left, right):
    return lax.dot_general(left, right, (((1,), (1,)), ((), ())), preferred_element_type=F32)


def mm_tn(left, right):
    return lax.dot_general(left, right, (((0,), (0,)), ((), ())), preferred_element_type=F32)


def loop(count, body):
    def step(index, carry):
        body(index)
        return carry

    lax.fori_loop(0, count, step, 0)


def whole_lanes(count):
    return -(-count // LANES) * LANES


def packed_widths(nq, nkv, ff):
    return (whole_lanes((nq + 2 * nkv) * HD), whole_lanes(nq * HD), ff, ff, ff)


def flip(chip, bits):
    other, bit = chip, 1
    while bit <= bits:
        if bits & bit:
            other = other + bit * (1 - 2 * ((chip // bit) % 2))
        bit *= 2
    return other


def layer_kernel(dims, *refs):
    n, chips, rows, width, nq, nkv, ff, nseq = dims
    nf = 2 * chips
    shard = width // nf
    total = n * rows
    half = rows // 2
    q_wide, kv_wide = nq * LANES, nkv * LANES
    widths = (q_wide + 2 * kv_wide, q_wide, ff, ff, ff)
    gwidths = packed_widths(nq, nkv, ff)
    widest = max(gwidths)
    near = [1] if chips > 1 else []
    far = [2 * k for k in range(1, chips // 2)]
    refs = list(refs)

    def take(count):
        taken = refs[:count]
        del refs[:count]
        return taken

    (lengths, freq, gain_a, gain_m) = take(4)
    (tokens, cot, w_q, w_k, w_v, w_o, w_d, w_g, w_u) = take(9)
    (out_ref, gtok_ref, out_ga, out_gm, out_q, out_k, out_v, out_o, out_g, out_u, out_d) = take(11)
    far_landing = take(3)
    near_landing = take(2)
    landing = near_landing + far_landing
    weights = take(5)
    (x_buf, ct_buf, mi_buf, gm_buf, r_two, cot_own) = take(6)
    (qkv, gqkv, probs, mixed, gmixed, hid, gg, gu, gqkv_pack, mixed_pack) = take(10)
    (t_one, t_two) = take(2)
    (s_buf, r_buf, own_sum, middle, gmid, wide_tile) = take(6)
    (sc_one, sc_two, cos_t, sin_t) = take(4)
    (gain_in, gain_row, gain_own, gain_z, gain_f, stage) = take(6)
    (pick_rope, pick_end) = take(2)
    (q_in, k_in, v_in, o_in) = take(4)
    (out_own, q_own, k_own, v_own, o_own, big_own) = take(6)
    send_b = take(1)[0]
    sums = take(5)
    from_partner = take(5)
    (w_ss, w_fs, w_qs, w_rs, w_ls) = take(5)
    (z_ss, z_rs) = take(2)
    (rs_ss, rs_rs) = take(2)
    (b_ss, b_rs, i_ss, i_rs, l_sem, in_sem, out_sem) = take(7)

    f = lax.axis_index("fsdp")
    d = lax.axis_index("dp")
    p = f // 2
    c = f % 2

    def at_f(index):
        return {"fsdp": index, "dp": d}

    def at_d(index):
        return {"fsdp": f, "dp": index}

    partner = p * 2 + 1 - c
    low = 1 - d // (n // 2)
    inner, outer = d - 1 + 2 * low, d + 1 - 2 * low
    end = (d == 0) | (d == n - 1)

    def remote(src, dst, ss, rs, where):
        return pltpu.make_async_remote_copy(
            src_ref=src, dst_ref=dst, send_sem=ss, recv_sem=rs, device_id=where, device_id_type=MESH
        )

    def span(index, size):
        return pl.ds(pl.multiple_of(index * size, size), size)

    def block(ref, index, size=rows):
        return ref.at[span(index, size)]

    def cols(index, size=TILE):
        return span(index, size)

    loads = [
        pltpu.make_async_copy(src, dst, in_sem.at[i])
        for i, (src, dst) in enumerate(
            (
                (w_q, q_in),
                (w_k, k_in),
                (w_v, v_in),
                (w_o, o_in),
                (tokens, block(x_buf, d)),
                (cot, block(ct_buf, d)),
                (cot, cot_own),
            )
        )
    ]
    for copy in loads:
        copy.start()

    barrier = pltpu.get_barrier_semaphore()
    for k in range(1, chips):
        pl.semaphore_signal(
            barrier, inc=1, device_id=at_f(flip(p, k) * 2 + c), device_id_type=MESH
        )
    pl.semaphore_signal(barrier, inc=1, device_id=at_f(partner), device_id_type=MESH)

    for k in range(1, n):
        pl.semaphore_signal(
            barrier, inc=1, device_id=at_d((d + k) % n), device_id_type=MESH
        )

    class Gather:
        def __init__(self, slot, dst, size, src=None, plain=False):
            self.slot, self.dst, self.size = slot, dst, size
            self.src = self.part(f) if src is None else src
            self.local = src is not None
            self.aimed = list(range(1, chips)) if plain else near + far
            self.plain = plain

        def part(self, index):
            return block(self.dst, index, self.size)

        def direct(self, k):
            where = partner if k == 0 else flip(p, k) * 2 + c
            return remote(
                self.src, self.part(f), w_ss.at[self.slot, k], w_rs.at[self.slot, f], at_f(where)
            )

        def onward(self, k):
            index = flip(p, k) * 2 + c
            return remote(
                self.part(index),
                self.part(index),
                w_fs.at[self.slot, k],
                w_rs.at[self.slot, index],
                at_f(partner),
            )

        def across(self, first, second):
            index = flip(p, first) * 2 + c
            return remote(
                self.part(index),
                self.part(index),
                w_qs.at[self.slot, first + second],
                w_rs.at[self.slot, index],
                at_f(flip(p, second) * 2 + c),
            )

        def own(self):
            return pltpu.make_async_copy(self.src, self.part(f), w_ls.at[self.slot])

        def start(self):
            for k in self.aimed + [0]:
                self.direct(k).start()
            if self.local:
                self.own().start()

        def relay(self):
            for core, first, second in ((0, near, far), (1, far, near)):

                @pl.when(c == core)
                def _():
                    for k in first:
                        copy = self.onward(k)
                        copy.wait_recv()
                        for other in second:
                            self.across(k, other).start()
                        copy.start()

        def forward(self):
            if self.plain:
                for k in range(1, chips):
                    copy = self.onward(k)
                    copy.wait_recv()
                    copy.start()
                return

            for core, second in ((0, far), (1, near)):

                @pl.when(c == core)
                def _():
                    for k in second:
                        copy = self.onward(k)
                        copy.wait_recv()
                        copy.start()

            for k in near:
                for other in far:
                    copy = self.onward(k + other)
                    copy.wait_recv()
                    copy.start()

        def finish(self):
            for k in range(chips):
                index = flip(p, k) * 2 + 1 - c
                remote(
                    self.part(index),
                    self.part(index),
                    w_fs.at[self.slot, k],
                    w_rs.at[self.slot, index],
                    at_f(partner),
                ).wait_recv()
            if self.local:
                self.own().wait()

        def drain(self):
            for k in self.aimed + [0]:
                self.direct(k).wait_send()
            for k in range(1, chips):
                self.onward(k).wait_send()
            if self.plain:
                return
            for k in near:
                for other in far:
                    remote(
                        self.part(f),
                        self.part(f),
                        w_qs.at[self.slot, k + other],
                        w_rs.at[self.slot, f],
                        at_f(partner),
                    ).wait_send()

    class Line:
        def __init__(self, slot, buf, size=rows, parts=1, src=None):
            self.slot, self.buf, self.size, self.parts, self.src = slot, buf, size, parts, src

        def copy(self, index, side, h, own=False):
            piece = self.size // self.parts
            part = block(self.buf, index * self.parts + h, piece)
            src = part
            if own and self.src is not None:
                src = self.src.at[pl.ds(h * piece, piece)]
            where = d + 1 if side == 0 else d - 1
            return remote(
                src,
                part,
                z_ss.at[self.slot, side, h, index],
                z_rs.at[self.slot, h, index],
                at_d(where),
            )

        def start(self, h=0):
            @pl.when(d < n - 1)
            def _():
                self.copy(d, 0, h, True).start()

            @pl.when(d > 0)
            def _():
                self.copy(d, 1, h, True).start()

        def pass_on(self, index, side, h):
            copy = self.copy(index, side, h)
            copy.wait_recv()
            copy.start()

        def inward(self, s, h=0):
            @pl.when((d > 0) & (d < n // 2) & (d + s < n))
            def _():
                self.pass_on(d + s, 1, h)

            @pl.when((d < n - 1) & (d >= n // 2) & (d - s >= 0))
            def _():
                self.pass_on(d - s, 0, h)

        def outward(self, s, h=0):
            @pl.when((d < n // 2) & (d - s >= 0))
            def _():
                self.pass_on(d - s, 0, h)

            @pl.when((d >= n // 2) & (d + s < n))
            def _():
                self.pass_on(d + s, 1, h)

        def step(self, s, h=0):
            self.inward(s, h)
            self.outward(s, h)

        def arrive(self, s, h=0):
            @pl.when((d - s >= 0) & (d == n - 1))
            def _():
                self.copy(d - s, 0, h).wait_recv()

            @pl.when((d + s < n) & (d == 0))
            def _():
                self.copy(d + s, 1, h).wait_recv()

        def drain(self):
            for h in range(self.parts):
                for j in range(n):

                    @pl.when((j <= d) & (d < n - 1))
                    def _():
                        self.copy(j, 0, h).wait_send()

                    @pl.when((j >= d) & (d > 0))
                    def _():
                        self.copy(j, 1, h).wait_send()

    class Reduce:
        def __init__(self, slot, tile_of, sends, gets, also=None):
            self.slot, self.tile_of, self.sends, self.gets = slot, tile_of, sends, gets
            self.also = also

        def copy(self, index, where, slot, h):
            return remote(
                block(self.sends, 2 * index + h, half),
                block(self.gets, 2 * slot + h, half),
                rs_ss.at[self.slot, h, index],
                rs_rs.at[self.slot, h, slot],
                at_d(where),
            )

        def got(self, slot, h):
            part = block(self.gets, 2 * slot + h, half)
            remote(
                part, part, rs_ss.at[self.slot, h, 0], rs_rs.at[self.slot, h, slot], at_d(d)
            ).wait_recv()

        def right(self, index, h):
            return self.copy(index, d + 1, index, h)

        def left(self, index, h, last):
            return self.copy(index, d - 1, n if last else index, h)

        def compute(self, keep=True):
            def tile(t):
                value = self.tile_of(t, pl.ds(0, total))
                if keep:
                    wide_tile[...] = value
                    own_sum[:, cols(t)] = wide_tile[span(d, rows), :]
                self.sends[pl.ds(0, total), cols(t)] = value.astype(BF)

            loop(width // TILE, tile)

        def pair(self):
            first = d - 1 + low

            def tile(t):
                value = self.tile_of(t, pl.ds(pl.multiple_of(first * rows, rows), 2 * rows))
                wide_tile[0 : 2 * rows, :] = value
                own_sum[:, cols(t)] = wide_tile[span(1 - low, rows), :]
                self.sends[span(inner, rows), cols(t)] = wide_tile[span(low, rows), :].astype(BF)
                if self.also is not None:
                    self.also(t, value, pl.ds(pl.multiple_of(first * rows, rows), 2 * rows))

            loop(width // TILE, tile)

        def single(self, j):
            def tile(t):
                value = self.tile_of(t, span(j, rows))
                self.sends[span(j, rows), cols(t)] = value.astype(BF)
                if self.also is not None:
                    self.also(t, value, span(j, rows))

            loop(width // TILE, tile)

        def send_at(self, s):
            @pl.when(d == 0)
            def _():
                for h in range(2):
                    self.right(d + s, h).start()

            @pl.when(d == n - 1)
            def _():
                for h in range(2):
                    self.left(d - s, h, s == 1).start()

        def add_right(self, index, h):
            self.add_into(index, h)
            self.right(index, h).start()

        def add_left(self, index, h, last):
            self.add_into(index, h)
            self.left(index, h, last).start()

        def out_adv(self, s, h):
            @pl.when((d > 0) & (d < n // 2) & (d + s < n))
            def _():
                self.add_right(d + s, h)

            @pl.when((d < n - 1) & (d >= n // 2) & (d - s >= 0))
            def _():
                self.add_left(d - s, h, s == 1)

        def in_adv(self, s, h):
            @pl.when((d < n // 2) & (d - s >= 0))
            def _():
                self.add_left(d - s, h, s == 1)

            @pl.when((d >= n // 2) & (d + s < n))
            def _():
                self.add_right(d + s, h)

        def launch(self, halves_first):
            order = [(s, h) for h in range(2) for s in range(n - 1, 0, -1)]
            if not halves_first:
                order = [(s, h) for s in range(n - 1, 0, -1) for h in range(2)]

            @pl.when(d == 0)
            def _():
                for s, h in order:
                    self.right(d + s, h).start()

            @pl.when(d == n - 1)
            def _():
                for s, h in order:
                    self.left(d - s, h, s == 1).start()

        def add_into(self, index, h):
            self.got(index, h)

            def some(i):
                r = pl.ds(pl.multiple_of(index * rows + h * half + i * CHUNK, CHUNK), CHUNK)
                self.sends[r, :] = (
                    self.sends[r, :].astype(F32) + self.gets[r, :].astype(F32)
                ).astype(BF)

            loop(half // CHUNK, some)

        def advance(self, s, h):
            right, left = d + s, d - s

            @pl.when((right < n) & (d > 0))
            def _():
                self.add_into(right, h)
                self.right(right, h).start()

            @pl.when((left >= 0) & (d < n - 1))
            def _():
                self.add_into(left, h)
                self.left(left, h, s == 1).start()

        def final(self, h):
            self.final_into(own_sum, h)

        def final_into(self, acc, h):
            def add(slot):
                self.got(slot, h)

                def some(i):
                    r = pl.ds(pl.multiple_of(h * half + i * CHUNK, CHUNK), CHUNK)
                    there = pl.ds(
                        pl.multiple_of(slot * rows + h * half + i * CHUNK, CHUNK), CHUNK
                    )
                    acc[r, :] = acc[r, :] + self.gets[there, :].astype(F32)

                loop(half // CHUNK, some)

            @pl.when(d > 0)
            def _():
                add(d)

            @pl.when(d < n - 1)
            def _():
                add(n)

        def drain(self):
            for h in range(2):
                for j in range(n):

                    @pl.when(d != j)
                    def _():
                        self.copy(j, d, j, h).wait_send()

    def tiles(wide, body):
        if wide % TILE == 0:
            loop(wide // TILE, lambda t: body(cols(t)))
        else:
            for start in range(0, wide, TILE):
                body(pl.ds(start, min(TILE, wide - start)))

    handing = []

    class Grad:
        def __init__(self, group, turned, terms, emit):
            self.group, self.turned, self.terms, self.emit = group, turned, terms, emit
            self.width = gwidths[group]

        def hand_over(self):
            src = send_b if self.width == widest else send_b.at[:, :, pl.ds(0, self.width)]
            return remote(
                src,
                from_partner[self.group],
                b_ss.at[self.group],
                b_rs.at[self.group],
                at_f(partner),
            )

        def ship(self, k):
            chip = flip(p, k)
            return remote(
                sums[self.group].at[chip],
                landing[self.group].at[k - 1],
                i_ss.at[self.group, k - 1],
                i_rs.at[self.group, k - 1],
                at_f(chip * 2 + c),
            )

        def blocks_of(self, core, lanes):
            left = jnp.concatenate(
                [self.turned[span(q * 2 + core, shard), :] for q in range(chips)], axis=0
            )
            value = mm(left, self.terms[:, lanes])
            return [value[q * shard : (q + 1) * shard] for q in range(chips)]

        def release(self):
            self.hand_over().wait_send()

        def send_all(self):
            if handing:
                handing.pop().release()

            def tile(lanes):
                for q, value in enumerate(self.blocks_of(1 - c, lanes)):
                    send_b[q, :, lanes] = value.astype(BF)

            tiles(self.width, tile)
            self.hand_over().start()
            handing.append(self)

        def own_sums(self):
            self.hand_over().wait_recv()

            def tile(lanes):
                for q, value in enumerate(self.blocks_of(c, lanes)):
                    other = from_partner[self.group][q, :, lanes].astype(F32)
                    sums[self.group][q, :, lanes] = (value + other).astype(BF)

            tiles(self.width, tile)

        def ship_all(self):
            for k in range(1, chips):
                self.ship(k).start()

        def own_all(self):
            self.own_sums()
            self.ship_all()

        def fetch(self, k):
            return pltpu.make_async_copy(
                landing[self.group].at[k - 1],
                stage.at[k - 1, :, pl.ds(0, self.width)],
                l_sem.at[k - 1],
            )

        def collect(self):
            for k in range(1, chips):
                self.ship(k).wait()
                if self.group >= 2:
                    self.fetch(k).start()

        def finish(self):
            if self.group >= 2:
                for k in range(1, chips):
                    self.fetch(k).wait()

            def parts(lanes):
                yield sums[self.group][p, :, lanes]
                for k in range(1, chips):
                    if self.group >= 2:
                        yield stage[k - 1, :, lanes]
                    else:
                        yield landing[self.group][k - 1, :, lanes]

            self.emit(parts)

    def total_of(values):
        result = None
        for value in values:
            result = value if result is None else result + value
        return result

    stores = []

    def store(src, dst):
        copy = pltpu.make_async_copy(src, dst, out_sem.at[len(stores)])
        copy.start()
        stores.append(copy)

    def emit_plain(out):
        def emit(parts):
            def tile(t):
                big_own[:, cols(t)] = total_of(v.astype(F32) for v in parts(cols(t)))

            if big_stores:
                big_stores.pop().wait()
            loop(ff // TILE, tile)
            copy = pltpu.make_async_copy(big_own, out, l_sem.at[chips - 1])
            copy.start()
            big_stores.append(copy)

        return emit

    big_stores = []

    def summed(parts, start, size):
        return total_of(v.astype(F32) for v in parts(pl.ds(start, size)))

    q_real, kv_real = nq * HD, nkv * HD

    def emit_out(parts):
        o_own[...] = summed(parts, 0, q_real)
        store(o_own, out_o)

    def emit_qkv(parts):
        q_own[...] = summed(parts, 0, q_real)
        store(q_own, out_q)
        k_own[...] = summed(parts, q_real, kv_real)
        store(k_own, out_k)
        v_own[...] = summed(parts, q_real + kv_real, kv_real)
        store(v_own, out_v)

    def fill(dst, r, value):
        spare = dst.shape[1] - value.shape[1]
        if spare:
            value = jnp.concatenate([value, jnp.zeros((value.shape[0], spare), F32)], axis=1)
        dst[r, :] = value.astype(BF)

    def pack_mixed():
        def one(b):
            r = span(b, rows)
            fill(mixed_pack, r, mm_nt(mixed[r, :], pick_end[...]))

        loop(n, one)

    def pack_gqkv():
        def one(b):
            r = span(b, rows)
            keys = slice(q_wide, q_wide + kv_wide)
            vals = slice(q_wide + kv_wide, q_wide + 2 * kv_wide)
            value = jnp.concatenate(
                [
                    mm_nt(gqkv[r, 0:q_wide], pick_rope[...]),
                    mm_nt(gqkv[r, keys], pick_rope[0:kv_real, 0:kv_wide]),
                    mm_nt(gqkv[r, vals], pick_end[0:kv_real, 0:kv_wide]),
                ],
                axis=1,
            )
            fill(gqkv_pack, r, value)

        loop(n, one)

    def turn(src, dst):
        def lane_block(t):
            dst[cols(t, LANES), :] = src[pl.ds(0, total), cols(t, LANES)].T

        loop(width // LANES, lane_block)

    def at(s, work):
        if s == 0:
            work(d)
            return

        def side(i):
            j = d - s + 2 * s * i

            @pl.when((j >= 0) & (j < n))
            def _():
                work(j)

        loop(2, side)

    def one_hot(split):
        shape = (nq * HD, q_wide)
        row = lax.broadcasted_iota(jnp.int32, shape, 0)
        lane = lax.broadcasted_iota(jnp.int32, shape, 1)
        inside = lane % LANES
        start = (lane // LANES) * HD
        if split:
            gap = LANES // 2 - HALF
            upper = inside >= LANES // 2
            source = start + jnp.where(upper, inside - gap, inside)
            real = (inside % (LANES // 2)) < HALF
        else:
            source = start + inside
            real = inside < HD
        return jnp.where(real & (row == source), 1.0, 0.0).astype(BF)

    pick_rope[...] = one_hot(True)
    pick_end[...] = one_hot(False)
    gain_mine = block(gain_in, f, 8)
    gain_mine[...] = jnp.zeros(gain_mine.shape, F32)
    gain_mine[0:1, 0:shard] = gain_a[...].astype(F32)
    gain_mine[1:2, 0:shard] = gain_m[...].astype(F32)

    gathers = [
        Gather(0, weights[0], shard, plain=True),
        Gather(1, weights[1], shard, plain=True),
        Gather(2, weights[2], shard, w_g),
        Gather(3, weights[3], shard, w_u),
        Gather(4, weights[4], shard, w_d),
    ]
    gain_gather = Gather(5, gain_in, 8, plain=True)
    tok_line = Line(0, x_buf, parts=2, src=tokens)
    cot_line = Line(1, ct_buf, src=cot)
    mi_line = Line(2, mi_buf, parts=2)
    gm_line = Line(3, gm_buf, parts=2)

    def gain_swap(k):
        mine = block(gain_z, d, 8)
        return remote(
            mine, mine, z_ss.at[4, 0, 0, k], z_rs.at[4, 0, d], at_d((d + k) % n)
        )

    def gain_got(k):
        other = (d + k) % n
        part = block(gain_z, other, 8)
        remote(part, part, z_ss.at[4, 0, 0, k], z_rs.at[4, 0, other], at_d(d)).wait_recv()

    def segments(b, shape, dim):
        index = lax.broadcasted_iota(jnp.int32, shape, dim)
        segment = jnp.zeros(shape, jnp.int32)
        offset = jnp.zeros(shape, jnp.int32)
        end = jnp.int32(0)
        for k in range(nseq):
            end = end + lengths[b, k]
            past = index >= end
            segment = segment + past.astype(jnp.int32)
            offset = jnp.where(past, end, offset)
        return index, segment, offset

    def tables(b):
        index, _, offset = segments(b, (rows, LANES), 0)
        angle = (index - offset).astype(F32) * freq[...]
        lane = lax.broadcasted_iota(jnp.int32, (rows, LANES), 1)
        sine = jnp.sin(angle)
        block(cos_t, b)[...] = jnp.cos(angle)
        block(sin_t, b)[...] = jnp.where(lane < LANES // 2, -sine, sine)

    pl.semaphore_wait(barrier, chips + n - 1)
    for h in range(2):
        tok_line.start(h)

    @pl.when(end)
    def _():
        cot_line.start()

    gain_gather.start()
    mine = span(f, shard)
    kv_rows = nkv * HD
    for copy in loads[:4]:
        copy.wait()
    weights[0][mine, 0:q_wide] = mm(q_in[...], pick_rope[...]).astype(BF)
    weights[0][mine, q_wide : q_wide + kv_wide] = mm(
        k_in[...], pick_rope[0:kv_rows, 0:kv_wide]
    ).astype(BF)
    weights[0][mine, q_wide + kv_wide : q_wide + 2 * kv_wide] = mm(
        v_in[...], pick_end[0:kv_rows, 0:kv_wide]
    ).astype(BF)
    gathers[0].start()
    weights[1][mine, :] = mm(o_in[...], pick_end[...]).astype(BF)
    for g in range(1, 5):
        gathers[g].start()
    loop(n, tables)
    loads[4].wait()
    gain_gather.forward()
    gain_gather.finish()
    for k in range(nf):
        gain_row[:, k * shard : (k + 1) * shard] = gain_in[8 * k : 8 * k + 8, 0:shard]

    def rms(value):
        mean = jnp.sum(value * value, axis=-1, keepdims=True) / width
        return lax.rsqrt(mean + EPSILON)

    def norm_one(j):
        def some(i):
            r = pl.ds(pl.multiple_of(j * rows + i * CHUNK, CHUNK), CHUNK)
            value = x_buf[r, :].astype(F32)
            scale = rms(value)
            sc_one[r, :] = scale
            mi_buf[r, :] = (value * scale * gain_row[0:1, :]).astype(BF)

        loop(rows // CHUNK, some)

    def rope(value, sign, cos_v, sin_v):
        return value * cos_v + sign * (pltpu.roll(value, LANES // 2, 1) * sin_v)

    heads = nq + 2 * nkv

    def head(ref, r, h):
        return ref[r, h * LANES : (h + 1) * LANES]

    def attend(b):
        r = span(b, rows)
        cos_v, sin_v = cos_t[r, :], sin_t[r, :]
        for t in range(heads // 2):
            both = mm(mi_buf[r, :], weights[0][:, 2 * t * LANES : 2 * (t + 1) * LANES])
            for h in (2 * t, 2 * t + 1):
                value = both[:, (h - 2 * t) * LANES : (h - 2 * t + 1) * LANES]
                if h < nq + nkv:
                    value = rope(value, 1.0, cos_v, sin_v)
                qkv[r, h * LANES : (h + 1) * LANES] = value.astype(BF)
        t_index, t_seg, _ = segments(b, (rows, rows), 0)
        s_index, s_seg, _ = segments(b, (rows, rows), 1)
        allowed = (t_seg == s_seg) & (s_index <= t_index)
        for h in range(nq):
            kv = h // (nq // nkv)
            score = mm_nt(head(qkv, r, h), head(qkv, r, nq + kv)) * HD ** (-0.5)
            score = jnp.where(allowed, score, NEG_FILL)
            top = jnp.max(score, axis=-1, keepdims=True)
            log_total = top + jnp.log(jnp.sum(jnp.exp(score - top), axis=-1, keepdims=True))
            prob = jnp.where(allowed, jnp.exp(score - log_total), 0.0)
            probs[b * nq + h] = prob
            mixed[r, h * LANES : (h + 1) * LANES] = mm(
                prob.astype(BF), head(qkv, r, nq + nkv + kv)
            ).astype(BF)

    def tokens_at(s):
        for h in range(2):
            tok_line.step(s, h)
            tok_line.arrive(s, h)

    norm_one(d)
    tokens_at(1)
    at(1, norm_one)
    early = min(2, n - 1)
    if early == 2:
        for h in range(2):
            tok_line.step(2, h)

    @pl.when((d > 0) & (d < n - 1))
    def _():
        cot_line.start()

    gathers[0].forward()
    if early == 2:
        for h in range(2):
            tok_line.arrive(2, h)
        at(2, norm_one)
    gathers[0].finish()
    for s in range(early + 1):
        at(s, attend)
    gathers[1].forward()
    cot_line.outward(1)
    for s in range(early + 1, n):
        tokens_at(s)
        at(s, norm_one)
        at(s, attend)
    gathers[1].finish()

    def by_turned(pairs):
        def tile_of(t, r):
            return total_of(mm_nt(left[r, :], weight[cols(t), :]) for left, weight in pairs)

        return tile_of

    def run(work):
        if work:
            todo = work.pop(0)
            if todo is not None:
                todo()

    def reduce_then_gather(red, finish_half, line, work):
        red.compute()
        red.launch(True)
        run(work)
        for s in range(n - 2, 0, -1):
            red.advance(s, 0)
            run(work)
        red.final(0)
        finish_half(0)
        line.start(0)
        run(work)
        for i in range(1, n - 1):
            red.advance(n - 1 - i, 1)
            if i == 1:
                line.inward(i, 0)
            run(work)
        red.final(1)
        finish_half(1)
        line.start(1)
        for i in range(1, n - 1):
            if i > 1:
                line.inward(i, 0)
            line.outward(i, 0)

    def arrived(line, s):
        line.step(s, 1)
        line.arrive(s, 0)
        line.arrive(s, 1)

    def norm_two(h):
        def some(i):
            r = pl.ds(pl.multiple_of(h * half + i * CHUNK, CHUNK), CHUNK)
            here = pl.ds(pl.multiple_of(d * rows + h * half + i * CHUNK, CHUNK), CHUNK)
            value = x_buf[here, :].astype(F32) + own_sum[r, :]
            scale = rms(value)
            middle[r, :] = value
            sc_two[r, :] = scale
            mi_buf[here, :] = (value * scale * gain_row[1:2, :]).astype(BF)

        loop(half // CHUNK, some)

    def both(*todo):
        def do():
            for one in todo:
                one()

        return do

    def cot_on(s):
        def do():
            cot_line.inward(s)
            if s > 1:
                cot_line.outward(s)

        return do

    after_attn = Reduce(0, by_turned([(mixed, weights[1])]), s_buf, r_buf)
    work = [cot_on(1)]
    work += [both(cot_on(2), gathers[2].relay)] if n > 2 else [gathers[2].relay]
    work += [gathers[3].relay, None, gathers[4].relay, gathers[2].forward]
    work += [cot_on(s) for s in range(3, n - 1)]
    reduce_then_gather(after_attn, norm_two, mi_line, work)
    while work:
        run(work)
    pack_mixed()
    gathers[3].forward()
    gathers[4].forward()
    for g in (2, 3, 4):
        gathers[g].finish()
    loads[5].wait()
    loads[6].wait()

    def feed(j):
        r = span(j, rows)

        def tile(t):
            left = mi_buf[r, :]
            gate = mm(left, weights[2][:, cols(t)])
            up = mm(left, weights[3][:, cols(t)])
            grad_hidden = mm(ct_buf[r, :], weights[4][:, cols(t)])
            sig = 1.0 / (1.0 + jnp.exp(-gate))
            hid[r, cols(t)] = (gate * sig * up).astype(BF)
            gu[r, cols(t)] = (grad_hidden * gate * sig).astype(BF)
            gg[r, cols(t)] = (grad_hidden * up * sig * (1.0 + gate * (1.0 - sig))).astype(BF)

        loop(ff // TILE, tile)

    def at_outer(work):
        @pl.when((outer >= 0) & (outer < n))
        def _():
            work(outer)

    after_mlp = Reduce(1, by_turned([(gg, weights[2]), (gu, weights[3])]), s_buf, r_buf)
    after_attn.drain()
    at(0, feed)
    mi_line.step(1, 1)
    for s in range(1, n):
        for h in range(2):
            mi_line.arrive(s, h)
        cot_line.arrive(s)
        at(s, feed)
        if s + 1 < n:
            mi_line.step(s + 1, 1)
        if s == 1:
            after_mlp.pair()
            after_mlp.send_at(1)
            at_outer(after_mlp.single)
        else:
            at(s, after_mlp.single)
            after_mlp.send_at(s)

    gain_own[...] = jnp.zeros((8, width), F32)

    def back_two(h):
        def some(i):
            r = pl.ds(pl.multiple_of(h * half + i * CHUNK, CHUNK), CHUNK)
            term = own_sum[r, :]
            scale = sc_two[r, :]
            normed = middle[r, :] * scale
            gain_sum = jnp.sum(term * normed, axis=0, keepdims=True)
            dn = term * gain_row[1:2, :]
            mean = jnp.sum(dn * normed, axis=-1, keepdims=True) / width
            here = pl.ds(pl.multiple_of(d * rows + h * half + i * CHUNK, CHUNK), CHUNK)
            value = cot_own[r, :].astype(F32) + scale * (dn - normed * mean)
            gmid[r, :] = value
            gm_buf[here, :] = value.astype(BF)
            gain_own[1:2, :] = gain_own[1:2, :] + gain_sum

        loop(half // CHUNK, some)

    down = Grad(4, t_one, hid, emit_plain(out_d))
    gate_g = Grad(2, t_two, gg, emit_plain(out_g))
    up_g = Grad(3, t_two, gu, emit_plain(out_u))

    def turn_mi():
        turn(mi_buf, t_two)

    def attn_in_again(j):
        def some(i):
            r = pl.ds(pl.multiple_of(j * rows + i * CHUNK, CHUNK), CHUNK)
            value = x_buf[r, :].astype(F32) * sc_one[r, :]
            s_buf[r, :] = (value * gain_row[0:1, :]).astype(BF)

        loop(rows // CHUNK, some)

    output = Reduce(2, by_turned([(hid, weights[4])]), ct_buf, r_two)

    def finish_mlp():
        for h in range(2):
            after_mlp.final(h)
            back_two(h)
            if h == 0:
                gm_line.start(h)

    turn(ct_buf, t_one)
    cot_line.drain()
    turn_mi()
    down.send_all()
    for h in range(2):
        after_mlp.out_adv(1, h)
    output.compute(keep=False)
    output.send_at(n - 1)
    down.own_all()
    for s in range(2, n - 1):
        for h in range(2):
            after_mlp.out_adv(s, h)

    @pl.when(jnp.logical_not(end))
    def _():
        finish_mlp()

    gate_g.send_all()
    work = [gate_g.own_all, up_g.send_all]
    for s in range(1, n - 1):
        for h in range(2):
            after_mlp.in_adv(s, h)
            run(work)
    while work:
        run(work)

    @pl.when(jnp.logical_not(end))
    def _():
        gm_line.start(1)

    gm_line.inward(1, 0)
    up_g.own_all()
    gm_line.inward(1, 1)
    gm_line.outward(1, 0)
    gm_line.outward(1, 1)

    @pl.when(end)
    def _():
        finish_mlp()
        gm_line.start(1)

    for s in range(n - 2, 1, -1):
        output.send_at(s)

    after_mlp.drain()
    mi_line.drain()

    def back(b):
        r = span(b, rows)

        def tile(t):
            gmixed[r, cols(t)] = mm(gm_buf[r, :], weights[1][:, cols(t)]).astype(BF)

        loop(q_wide // TILE, tile)
        cos_v, sin_v = cos_t[r, :], sin_t[r, :]
        group = nq // nkv
        for kv in range(nkv):
            key, val = head(qkv, r, nq + kv), head(qkv, r, nq + nkv + kv)
            grad_k = grad_v = None
            for h in range(kv * group, (kv + 1) * group):
                query, gm_h = head(qkv, r, h), head(gmixed, r, h)
                prob = probs[b * nq + h]
                delta = jnp.sum(
                    gm_h.astype(F32) * head(mixed, r, h).astype(F32), axis=-1, keepdims=True
                )
                grad_p = mm_nt(gm_h, val)
                grad_s = (prob * (grad_p - delta) * HD ** (-0.5)).astype(BF)
                grad_q = mm(grad_s, key)
                gqkv[r, h * LANES : (h + 1) * LANES] = rope(grad_q, -1.0, cos_v, sin_v).astype(BF)
                k_term, v_term = mm_tn(grad_s, query), mm_tn(prob.astype(BF), gm_h)
                grad_k = k_term if grad_k is None else grad_k + k_term
                grad_v = v_term if grad_v is None else grad_v + v_term
            k_at, v_at = (nq + kv) * LANES, (nq + nkv + kv) * LANES
            gqkv[r, k_at : k_at + LANES] = rope(grad_k, -1.0, cos_v, sin_v).astype(BF)
            gqkv[r, v_at : v_at + LANES] = grad_v.astype(BF)

    def add_gain(t, value, r):
        normed = x_buf[r, cols(t)].astype(F32) * sc_one[r, :]
        gain_own[0:1, cols(t)] = gain_own[0:1, cols(t)] + jnp.sum(
            value * normed, axis=0, keepdims=True
        )

    after_in = Reduce(3, by_turned([(gqkv, weights[0])]), s_buf, r_buf, add_gain)
    out_g_grad = Grad(1, t_one, mixed_pack, emit_out)
    qkv_g = Grad(0, t_two, gqkv_pack, emit_qkv)

    def pass_gm(h):
        for s in range(2, n - 1):
            gm_line.inward(s, h)
            gm_line.outward(s, h)

    at(0, back)
    pass_gm(0)
    for h in range(2):
        gm_line.arrive(1, h)
    back(inner)
    pass_gm(1)
    for s in range(n - 2, 1, -1):
        for h in range(2):
            output.out_adv(s, h)
    loop(n, attn_in_again)
    turn(s_buf, t_two)
    after_in.pair()
    after_in.send_at(1)
    if n > 2:
        for h in range(2):
            output.out_adv(1, h)

    def outer_back(j):
        back(j)
        after_in.single(j)

    at_outer(outer_back)
    for s in range(2, n):
        for h in range(2):
            gm_line.arrive(s, h)
        at(s, outer_back)
    quarter = width // 4
    gain_mine = block(gain_z, d, 8)
    for i in range(8):
        gain_mine[i : i + 1, :] = gain_own[i // 4 : i // 4 + 1, pl.ds(i % 4 * quarter, quarter)]
    for k in range(1, n):
        gain_swap(k).start()
    for s in range(n - 1, 1, -1):
        after_in.send_at(s)
    if n > 2:
        output.send_at(1)
    for s in range(1, n - 1):
        for h in range(2):
            output.in_adv(s, h)
    turn(gm_buf, t_one)
    out_g_grad.send_all()
    pack_gqkv()
    out_g_grad.own_all()
    qkv_g.send_all()
    for h in range(2):
        after_in.out_adv(n - 2, h)
    qkv_g.own_sums()
    for k in range(1, n):
        gain_got(k)
    block(gain_f, f, 8)[...] = total_of(gain_z[8 * k : 8 * k + 8, :] for k in range(n))
    gain_back = Gather(6, gain_f, 8, plain=True)
    gain_back.start()
    qkv_g.ship_all()
    for s in range(n - 2, 0, -1):
        for h in range(2):
            after_in.in_adv(s, h)
        if s < n - 2:
            for h in range(2):
                after_in.out_adv(s, h)

    def output_end():
        middle[...] = middle[...] + block(ct_buf, d)[...].astype(F32)
        for h in range(2):
            output.final_into(middle, h)
        out_own[...] = middle[...].astype(BF)
        store(out_own, out_ref)

    def gain_end():
        gain_back.forward()
        gain_back.finish()
        gain_all = total_of(gain_f[8 * k : 8 * k + 8, :] for k in range(nf))
        for i in range(8):
            gain_own[i // 4 : i // 4 + 1, pl.ds(i % 4 * quarter, quarter)] = gain_all[i : i + 1, :]
        gain_all = pltpu.roll(gain_own[...], (width - f * shard) % width, 1)
        out_ga[...] = gain_all[0:1, 0:shard]
        out_gm[...] = gain_all[1:2, 0:shard]

    work = [gain_end]
    for grad in (down, gate_g, up_g):
        work.append(both(grad.collect, grad.finish))
    while work:
        run(work)

    def back_one(h):
        def some(i):
            r = pl.ds(pl.multiple_of(h * half + i * CHUNK, CHUNK), CHUNK)
            there = pl.ds(pl.multiple_of(d * rows + h * half + i * CHUNK, CHUNK), CHUNK)
            scale = sc_one[there, :]
            normed = x_buf[there, :].astype(F32) * scale
            dm = own_sum[r, :] * gain_row[0:1, :]
            mean = jnp.sum(dm * normed, axis=-1, keepdims=True) / width
            gmid[r, :] = gmid[r, :] + scale * (dm - normed * mean)

        loop(half // CHUNK, some)

    for h in range(2):
        after_in.final(h)
        back_one(h)
        part = pl.ds(h * half, half)
        store(gmid.at[part], gtok_ref.at[part])
    output_end()
    for grad in (qkv_g, out_g_grad):
        grad.collect()
        grad.finish()

    handing.pop().release()
    output.drain()
    after_in.drain()
    tok_line.drain()
    gm_line.drain()
    for k in range(1, n):
        gain_swap(k).wait_send()
    for gather in gathers + [gain_gather, gain_back]:
        gather.drain()
    big_stores.pop().wait()
    for copy in stores:
        copy.wait()


def pass_on(*refs):
    count = (len(refs) - 2) // 3
    srcs, dsts, held = refs[:count], refs[count : 2 * count], refs[2 * count : 3 * count]
    in_sem, out_sem = refs[3 * count :]
    order = range(count)
    for i in order:
        pltpu.make_async_copy(srcs[i], held[i], in_sem.at[i]).start()
    for i in order:
        pltpu.make_async_copy(srcs[i], held[i], in_sem.at[i]).wait()
        pltpu.make_async_copy(held[i], dsts[i], out_sem.at[i]).start()
    for i in order:
        pltpu.make_async_copy(held[i], dsts[i], out_sem.at[i]).wait()


def run_layer(lengths, freq, tokens, cot, gain_a, gain_m, w_q, w_k, w_v, w_o, w_d, w_g, w_u, n, chips):
    rows, width = tokens.shape
    nq = w_q.shape[1] // HD
    nkv = w_k.shape[1] // HD
    total = n * rows
    nf = 2 * chips
    shard = w_q.shape[0]
    ff = w_g.shape[1]
    q_wide, kv_wide = nq * LANES, nkv * LANES
    widths = (q_wide + 2 * kv_wide, q_wide, ff, ff, ff)
    dims = (n, chips, rows, width, nq, nkv, ff, lengths.shape[1])
    vmem = pl.BlockSpec(memory_space=pltpu.VMEM)
    hbm = pl.BlockSpec(memory_space=pltpu.HBM)
    results = [
        jax.ShapeDtypeStruct((rows, width), BF),
        jax.ShapeDtypeStruct((rows, width), F32),
        jax.ShapeDtypeStruct((1, shard), F32),
        jax.ShapeDtypeStruct((1, shard), F32),
    ] + [jax.ShapeDtypeStruct(w.shape, F32) for w in (w_q, w_k, w_v, w_o, w_g, w_u, w_d)]
    out_shape = results + [jax.ShapeDtypeStruct((chips - 1, shard, w), BF) for w in widths[2:]]
    gwidths = packed_widths(nq, nkv, ff)
    widest = max(gwidths)
    scratch = (
        [pltpu.VMEM((chips - 1, shard, w), BF) for w in gwidths[:2]]
        + [pltpu.VMEM((width, w), BF) for w in widths]
        + [
            pltpu.VMEM((total, width), BF),
            pltpu.VMEM((total, width), BF),
            pltpu.VMEM((total, width), BF),
            pltpu.VMEM((total, width), BF),
            pltpu.VMEM((total + rows, width), BF),
            pltpu.VMEM((rows, width), BF),
            pltpu.VMEM((total, widths[0]), BF),
            pltpu.VMEM((total, widths[0]), BF),
            pltpu.VMEM((n * nq, rows, rows), F32),
            pltpu.VMEM((total, q_wide), BF),
            pltpu.VMEM((total, q_wide), BF),
            pltpu.VMEM((total, ff), BF),
            pltpu.VMEM((total, ff), BF),
            pltpu.VMEM((total, ff), BF),
            pltpu.VMEM((total, gwidths[0]), BF),
            pltpu.VMEM((total, gwidths[1]), BF),
            pltpu.VMEM((width, total), BF),
            pltpu.VMEM((width, total), BF),
            pltpu.VMEM((total, width), BF),
            pltpu.VMEM((total + rows, width), BF),
            pltpu.VMEM((rows, width), F32),
            pltpu.VMEM((rows, width), F32),
            pltpu.VMEM((rows, width), F32),
            pltpu.VMEM((total, TILE), F32),
            pltpu.VMEM((total, 1), F32),
            pltpu.VMEM((rows, 1), F32),
            pltpu.VMEM((total, LANES), F32),
            pltpu.VMEM((total, LANES), F32),
            pltpu.VMEM((nf * 8, -(-shard // LANES) * LANES), F32),
            pltpu.VMEM((8, width), F32),
            pltpu.VMEM((8, width), F32),
            pltpu.VMEM((n * 8, width // 4), F32),
            pltpu.VMEM((nf * 8, width // 4), F32),
            pltpu.VMEM((chips - 1, shard, widest), BF),
            pltpu.VMEM((nq * HD, q_wide), BF),
            pltpu.VMEM((nq * HD, q_wide), BF),
        ]
        + [pltpu.VMEM(w.shape, BF) for w in (w_q, w_k, w_v, w_o)]
        + [pltpu.VMEM((rows, width), BF)]
        + [pltpu.VMEM(w.shape, F32) for w in (w_q, w_k, w_v, w_o, w_g)]
        + [
            pltpu.VMEM((chips, shard, widest), BF),
        ]
        + [pltpu.VMEM((chips, shard, w), BF) for w in gwidths]
        + [pltpu.VMEM((chips, shard, w), BF) for w in gwidths]
        + [
            pltpu.SemaphoreType.DMA((7, chips)),
            pltpu.SemaphoreType.DMA((7, chips)),
            pltpu.SemaphoreType.DMA((7, chips)),
            pltpu.SemaphoreType.DMA((7, nf)),
            pltpu.SemaphoreType.DMA((7,)),
            pltpu.SemaphoreType.DMA((5, 2, 2, n)),
            pltpu.SemaphoreType.DMA((5, 2, n)),
            pltpu.SemaphoreType.DMA((4, 2, n)),
            pltpu.SemaphoreType.DMA((4, 2, n + 1)),
            pltpu.SemaphoreType.DMA((5,)),
            pltpu.SemaphoreType.DMA((5,)),
            pltpu.SemaphoreType.DMA((5, chips)),
            pltpu.SemaphoreType.DMA((5, chips)),
            pltpu.SemaphoreType.DMA((chips,)),
            pltpu.SemaphoreType.DMA((7,)),
            pltpu.SemaphoreType.DMA((7,)),
        ]
    )
    made = pl.pallas_call(
        partial(layer_kernel, dims),
        out_shape=out_shape,
        in_specs=[pl.BlockSpec(memory_space=pltpu.SMEM)] + [vmem] * 3 + [hbm] * 9,
        out_specs=[hbm] * 2 + [vmem] * 2 + [hbm] * 10,
        scratch_shapes=scratch,
        compiler_params=pltpu.CompilerParams(
            collective_id=0, has_side_effects=True, vmem_limit_bytes=67043328
        ),
        name="layer",
    )(lengths, freq, gain_a, gain_m, tokens, cot, w_q, w_k, w_v, w_o, w_d, w_g, w_u)
    count = len(results)
    return pl.pallas_call(
        pass_on,
        out_shape=results,
        in_specs=[hbm] * count,
        out_specs=[hbm] * count,
        scratch_shapes=[pltpu.VMEM(r.shape, r.dtype) for r in results]
        + [pltpu.SemaphoreType.DMA((count,)), pltpu.SemaphoreType.DMA((count,))],
        compiler_params=pltpu.CompilerParams(vmem_limit_bytes=67043328),
        name="results",
    )(*made[:count])


def body(
    n,
    chips,
    tokens,
    lengths,
    cotangent,
    attn_gain,
    w_query,
    w_key,
    w_value,
    w_out,
    mlp_gain,
    w_gate,
    w_up,
    w_down,
):
    frequency = ROPE_BASE ** (-jnp.arange(HALF, dtype=F32) / HALF)
    frequency = jnp.pad(frequency, (0, LANES // 2 - HALF))
    freq = jnp.concatenate([frequency, frequency])[None, :]
    results = run_layer(
        lengths,
        freq,
        tokens,
        cotangent,
        attn_gain,
        mlp_gain,
        w_query[0],
        w_key[0],
        w_value[0],
        w_out[0].T,
        w_down[0].T,
        w_gate[0],
        w_up[0],
        n,
        chips,
    )
    output, grad_tokens, g_again, g_mgain, g_q, g_k, g_v, g_o, g_gate, g_up, g_down = results
    return (
        output,
        grad_tokens,
        g_again,
        g_q[None],
        g_k[None],
        g_v[None],
        g_o.T[None],
        g_mgain,
        g_gate[None],
        g_up[None],
        g_down.T[None],
    )


def solution(mesh):
    placed = (
        P(("fsdp", "dp"), None),
        P("fsdp", None),
        P(("fsdp", "dp"), None),
        P(None, "fsdp"),
        P(None, "fsdp", "dp"),
        P(None, "fsdp", "dp"),
        P(None, "fsdp", "dp"),
        P(None, "dp", "fsdp"),
        P(None, "fsdp"),
        P(None, "fsdp", "dp"),
        P(None, "fsdp", "dp"),
        P(None, "dp", "fsdp"),
    )
    return jax.shard_map(
        partial(body, mesh.shape["dp"], mesh.shape["fsdp"] // 2),
        mesh=mesh,
        in_specs=placed,
        out_specs=(
            P(("fsdp", "dp"), None),
            P(("fsdp", "dp"), None),
            P(None, "fsdp"),
            P(None, "fsdp", "dp"),
            P(None, "fsdp", "dp"),
            P(None, "fsdp", "dp"),
            P(None, "dp", "fsdp"),
            P(None, "fsdp"),
            P(None, "fsdp", "dp"),
            P(None, "fsdp", "dp"),
            P(None, "dp", "fsdp"),
        ),
        check_vma=False,
    )
```

```python
from functools import partial

import jax
import jax.numpy as jnp
import numpy as np
from jax import lax
from jax.experimental import pallas as pl
from jax.experimental.pallas import tpu as pltpu
from jax.sharding import PartitionSpec as P

HD = 96
HALF = 48
LANES = 128
EPSILON = 1e-05
ROPE_BASE = 100000.0
NEG_FILL = -1e30
MESH = pl.DeviceIdType.MESH
BF = jnp.bfloat16
F32 = jnp.float32
TILE = 256
CHUNK = 32


def mm(left, right):
    return jnp.dot(left, right, preferred_element_type=F32)


def mm_nt(left, right):
    return lax.dot_general(left, right, (((1,), (1,)), ((), ())), preferred_element_type=F32)


def mm_tn(left, right):
    return lax.dot_general(left, right, (((0,), (0,)), ((), ())), preferred_element_type=F32)


def loop(count, body):
    def step(index, carry):
        body(index)
        return carry

    lax.fori_loop(0, count, step, 0)


def whole_lanes(count):
    return -(-count // LANES) * LANES


def packed_widths(nq, nkv, ff):
    return (whole_lanes((nq + 2 * nkv) * HD), whole_lanes(nq * HD), ff, ff, ff)


def flip(chip, bits):
    other, bit = chip, 1
    while bit <= bits:
        if bits & bit:
            other = other + bit * (1 - 2 * ((chip // bit) % 2))
        bit *= 2
    return other


def layer_kernel(dims, *refs):
    n, chips, rows, width, nq, nkv, ff, nseq = dims
    nf = 2 * chips
    shard = width // nf
    total = n * rows
    half = rows // 2
    q_wide, kv_wide = nq * LANES, nkv * LANES
    widths = (q_wide + 2 * kv_wide, q_wide, ff, ff, ff)
    gwidths = packed_widths(nq, nkv, ff)
    widest = max(gwidths)
    near = [1] if chips > 1 else []
    far = [2 * k for k in range(1, chips // 2)]
    both_axes = [k + other for k in near for other in far]
    refs = list(refs)

    def take(count):
        taken = refs[:count]
        del refs[:count]
        return taken

    (lengths_in, freq_in, gain_a_in, gain_m_in) = take(4)
    (tokens, cot, w_q, w_k, w_v, w_o, w_d, w_g, w_u) = take(9)
    (out_ref, gtok_ref, out_ga, out_gm, out_q, out_k, out_v, out_o, out_g, out_u, out_d) = take(11)
    far_landing = take(3)
    near_landing = take(2)
    landing = near_landing + far_landing
    weights = take(5)
    (x_buf, ct_buf, mi_buf, gm_buf, r_two, cot_own) = take(6)
    (qkv, gqkv, probs, mixed, gmixed, hid, gg, gu, gqkv_pack, mixed_pack) = take(10)
    (t_one, t_two) = take(2)
    (s_buf, r_buf, own_sum, middle, gmid, wide_tile) = take(6)
    (sc_one, sc_two, cos_t, sin_t) = take(4)
    (gain_in, gain_row, gain_own, gain_z, gain_f, stage) = take(6)
    (pick_rope, pick_end) = take(2)
    (q_in, k_in, v_in, o_in) = take(4)
    (lengths, freq, gain_a, gain_m) = take(4)
    (out_own, q_own, k_own, v_own, o_own, big_own) = take(6)
    send_b = take(1)[0]
    sums = take(5)
    from_partner = take(5)
    (w_ss, w_fs, w_qs, w_rs, w_ls) = take(5)
    (z_ss, z_rs) = take(2)
    (rs_ss, rs_rs) = take(2)
    (b_ss, b_rs, i_ss, i_rs, l_sem, in_sem, out_sem, v_ss, v_rs) = take(9)
    between = take(3)

    f = lax.axis_index("fsdp")
    d = lax.axis_index("dp")
    p = f // 2
    c = f % 2

    def at_f(index):
        return {"fsdp": index, "dp": d}

    def at_d(index):
        return {"fsdp": f, "dp": index}

    partner = p * 2 + 1 - c
    low = 1 - d // (n // 2)
    inner, outer = d - 1 + 2 * low, d + 1 - 2 * low
    end = (d == 0) | (d == n - 1)

    def remote(src, dst, ss, rs, where):
        return pltpu.make_async_remote_copy(
            src_ref=src, dst_ref=dst, send_sem=ss, recv_sem=rs, device_id=where, device_id_type=MESH
        )

    def span(index, size):
        return pl.ds(pl.multiple_of(index * size, size), size)

    def block(ref, index, size=rows):
        return ref.at[span(index, size)]

    def cols(index, size=TILE):
        if isinstance(index, int):
            return pl.ds(index * size, size)
        return span(index, size)

    loads = [
        pltpu.make_async_copy(src, dst, in_sem.at[i])
        for i, (src, dst) in enumerate(
            (
                (w_q, q_in),
                (w_k, k_in),
                (w_v, v_in),
                (w_o, o_in),
                (tokens, block(x_buf, d)),
                (cot, block(ct_buf, d)),
                (cot, cot_own),
                (lengths_in, lengths),
                (freq_in, freq),
                (gain_a_in, gain_a),
                (gain_m_in, gain_m),
            )
        )
    ]
    for copy in loads:
        copy.start()

    barrier = pltpu.get_barrier_semaphore()
    for k in range(1, chips):
        pl.semaphore_signal(
            barrier, inc=1, device_id=at_f(flip(p, k) * 2 + c), device_id_type=MESH
        )
    pl.semaphore_signal(barrier, inc=1, device_id=at_f(partner), device_id_type=MESH)

    for k in range(1, n):
        pl.semaphore_signal(
            barrier, inc=1, device_id=at_d((d + k) % n), device_id_type=MESH
        )

    class Gather:
        def __init__(self, slot, dst, size, src=None, plain=False):
            self.slot, self.dst, self.size = slot, dst, size
            self.src = self.part(f) if src is None else src
            self.local = src is not None
            self.aimed = list(range(1, chips)) if plain else near + far
            self.plain = plain

        def part(self, index):
            return block(self.dst, index, self.size)

        def direct(self, k):
            where = partner if k == 0 else flip(p, k) * 2 + c
            return remote(
                self.src, self.part(f), w_ss.at[self.slot, k], w_rs.at[self.slot, f], at_f(where)
            )

        def onward(self, k):
            index = flip(p, k) * 2 + c
            return remote(
                self.part(index),
                self.part(index),
                w_fs.at[self.slot, k],
                w_rs.at[self.slot, index],
                at_f(partner),
            )

        def across(self, first, second):
            index = flip(p, first) * 2 + c
            return remote(
                self.part(index),
                self.part(index),
                w_qs.at[self.slot, first + second],
                w_rs.at[self.slot, index],
                at_f(flip(p, second) * 2 + c),
            )

        def own(self):
            return pltpu.make_async_copy(self.src, self.part(f), w_ls.at[self.slot])

        def start(self):
            for k in self.aimed + [0]:
                self.direct(k).start()
            if self.local:
                self.own().start()

        def relay(self):
            for core, first, second in ((0, near, far), (1, far, near)):

                @pl.when(c == core)
                def _():
                    for k in first:
                        copy = self.onward(k)
                        copy.wait_recv()
                        for other in second:
                            self.across(k, other).start()
                        copy.start()

        def forward(self):
            if self.plain:
                for k in range(1, chips):
                    copy = self.onward(k)
                    copy.wait_recv()
                    copy.start()
                return

            for core, second in ((0, far), (1, near)):

                @pl.when(c == core)
                def _():
                    for k in second:
                        copy = self.onward(k)
                        copy.wait_recv()
                        copy.start()

            for k in near:
                for other in far:
                    copy = self.onward(k + other)
                    copy.wait_recv()
                    copy.start()

        def finish(self):
            for k in range(chips):
                index = flip(p, k) * 2 + 1 - c
                remote(
                    self.part(index),
                    self.part(index),
                    w_fs.at[self.slot, k],
                    w_rs.at[self.slot, index],
                    at_f(partner),
                ).wait_recv()
            if self.local:
                self.own().wait()

        def drain(self):
            for k in self.aimed + [0]:
                self.direct(k).wait_send()
            for k in range(1, chips):
                self.onward(k).wait_send()
            if self.plain:
                return
            for k in near:
                for other in far:
                    remote(
                        self.part(f),
                        self.part(f),
                        w_qs.at[self.slot, k + other],
                        w_rs.at[self.slot, f],
                        at_f(partner),
                    ).wait_send()

    class Line:
        def __init__(self, slot, buf, size=rows, parts=1, src=None):
            self.slot, self.buf, self.size, self.parts, self.src = slot, buf, size, parts, src

        def copy(self, index, side, h, own=False):
            piece = self.size // self.parts
            part = block(self.buf, index * self.parts + h, piece)
            src = part
            if own and self.src is not None:
                src = self.src.at[pl.ds(h * piece, piece)]
            where = d + 1 if side == 0 else d - 1
            return remote(
                src,
                part,
                z_ss.at[self.slot, side, h, index],
                z_rs.at[self.slot, h, index],
                at_d(where),
            )

        def start(self, h=0):
            @pl.when(d < n - 1)
            def _():
                self.copy(d, 0, h, True).start()

            @pl.when(d > 0)
            def _():
                self.copy(d, 1, h, True).start()

        def pass_on(self, index, side, h):
            copy = self.copy(index, side, h)
            copy.wait_recv()
            copy.start()

        def inward(self, s, h=0):
            @pl.when((d > 0) & (d < n // 2) & (d + s < n))
            def _():
                self.pass_on(d + s, 1, h)

            @pl.when((d < n - 1) & (d >= n // 2) & (d - s >= 0))
            def _():
                self.pass_on(d - s, 0, h)

        def outward(self, s, h=0):
            @pl.when((d < n // 2) & (d - s >= 0))
            def _():
                self.pass_on(d - s, 0, h)

            @pl.when((d >= n // 2) & (d + s < n))
            def _():
                self.pass_on(d + s, 1, h)

        def step(self, s, h=0):
            self.inward(s, h)
            self.outward(s, h)

        def arrive(self, s, h=0):
            @pl.when((d - s >= 0) & (d == n - 1))
            def _():
                self.copy(d - s, 0, h).wait_recv()

            @pl.when((d + s < n) & (d == 0))
            def _():
                self.copy(d + s, 1, h).wait_recv()

        def drain(self):
            for h in range(self.parts):
                for j in range(n):

                    @pl.when((j <= d) & (d < n - 1))
                    def _():
                        self.copy(j, 0, h).wait_send()

                    @pl.when((j >= d) & (d > 0))
                    def _():
                        self.copy(j, 1, h).wait_send()

    class Reduce:
        def __init__(self, slot, tile_of, sends, gets, also=None, plain=False):
            self.slot, self.tile_of, self.sends, self.gets = slot, tile_of, sends, gets
            self.also, self.plain = also, plain

        def over_tiles(self, tile):
            if self.plain:
                for t in range(width // TILE):
                    tile(t)
            else:
                loop(width // TILE, tile)

        def copy(self, index, where, slot, h):
            return remote(
                block(self.sends, 2 * index + h, half),
                block(self.gets, 2 * slot + h, half),
                rs_ss.at[self.slot, h, index],
                rs_rs.at[self.slot, h, slot],
                at_d(where),
            )

        def got(self, slot, h):
            part = block(self.gets, 2 * slot + h, half)
            remote(
                part, part, rs_ss.at[self.slot, h, 0], rs_rs.at[self.slot, h, slot], at_d(d)
            ).wait_recv()

        def right(self, index, h):
            return self.copy(index, d + 1, index, h)

        def left(self, index, h, last):
            return self.copy(index, d - 1, n if last else index, h)

        def compute(self, keep=True):
            def tile(t):
                value = self.tile_of(t, pl.ds(0, total))
                if keep:
                    wide_tile[...] = value
                    own_sum[:, cols(t)] = wide_tile[span(d, rows), :]
                self.sends[pl.ds(0, total), cols(t)] = value.astype(BF)

            loop(width // TILE, tile)

        def pair(self):
            first = d - 1 + low

            def tile(t):
                value = self.tile_of(t, pl.ds(pl.multiple_of(first * rows, rows), 2 * rows))
                wide_tile[0 : 2 * rows, :] = value
                own_sum[:, cols(t)] = wide_tile[span(1 - low, rows), :]
                self.sends[span(inner, rows), cols(t)] = wide_tile[span(low, rows), :].astype(BF)
                if self.also is not None:
                    self.also(t, value, pl.ds(pl.multiple_of(first * rows, rows), 2 * rows))

            self.over_tiles(tile)

        def single(self, j):
            def tile(t):
                value = self.tile_of(t, span(j, rows))
                self.sends[span(j, rows), cols(t)] = value.astype(BF)
                if self.also is not None:
                    self.also(t, value, span(j, rows))

            self.over_tiles(tile)

        def send_at(self, s):
            @pl.when(d == 0)
            def _():
                for h in range(2):
                    self.right(d + s, h).start()

            @pl.when(d == n - 1)
            def _():
                for h in range(2):
                    self.left(d - s, h, s == 1).start()

        def add_right(self, index, h):
            self.add_into(index, h)
            self.right(index, h).start()

        def add_left(self, index, h, last):
            self.add_into(index, h)
            self.left(index, h, last).start()

        def out_adv(self, s, h):
            @pl.when((d > 0) & (d < n // 2) & (d + s < n))
            def _():
                self.add_right(d + s, h)

            @pl.when((d < n - 1) & (d >= n // 2) & (d - s >= 0))
            def _():
                self.add_left(d - s, h, s == 1)

        def in_adv(self, s, h):
            @pl.when((d < n // 2) & (d - s >= 0))
            def _():
                self.add_left(d - s, h, s == 1)

            @pl.when((d >= n // 2) & (d + s < n))
            def _():
                self.add_right(d + s, h)

        def launch(self, halves_first):
            order = [(s, h) for h in range(2) for s in range(n - 1, 0, -1)]
            if not halves_first:
                order = [(s, h) for s in range(n - 1, 0, -1) for h in range(2)]

            @pl.when(d == 0)
            def _():
                for s, h in order:
                    self.right(d + s, h).start()

            @pl.when(d == n - 1)
            def _():
                for s, h in order:
                    self.left(d - s, h, s == 1).start()

        def add_into(self, index, h):
            self.got(index, h)

            def some(i):
                r = pl.ds(pl.multiple_of(index * rows + h * half + i * CHUNK, CHUNK), CHUNK)
                self.sends[r, :] = (
                    self.sends[r, :].astype(F32) + self.gets[r, :].astype(F32)
                ).astype(BF)

            loop(half // CHUNK, some)

        def advance(self, s, h):
            right, left = d + s, d - s

            @pl.when((right < n) & (d > 0))
            def _():
                self.add_into(right, h)
                self.right(right, h).start()

            @pl.when((left >= 0) & (d < n - 1))
            def _():
                self.add_into(left, h)
                self.left(left, h, s == 1).start()

        def final(self, h):
            self.final_into(own_sum, h)

        def final_into(self, acc, h):
            def add(slot):
                self.got(slot, h)

                def some(i):
                    r = pl.ds(pl.multiple_of(h * half + i * CHUNK, CHUNK), CHUNK)
                    there = pl.ds(
                        pl.multiple_of(slot * rows + h * half + i * CHUNK, CHUNK), CHUNK
                    )
                    acc[r, :] = acc[r, :] + self.gets[there, :].astype(F32)

                loop(half // CHUNK, some)

            @pl.when(d > 0)
            def _():
                add(d)

            @pl.when(d < n - 1)
            def _():
                add(n)

        def drain(self):
            for h in range(2):
                for j in range(n):

                    @pl.when(d != j)
                    def _():
                        self.copy(j, d, j, h).wait_send()

    def tiles(wide, body):
        if wide % TILE == 0:
            loop(wide // TILE, lambda t: body(cols(t)))
        else:
            for start in range(0, wide, TILE):
                body(pl.ds(start, min(TILE, wide - start)))

    handing = []

    class Grad:
        def __init__(self, group, turned, terms, emit):
            self.group, self.turned, self.terms, self.emit = group, turned, terms, emit
            self.width = gwidths[group]

        def hand_over(self):
            src = send_b if self.width == widest else send_b.at[:, :, pl.ds(0, self.width)]
            return remote(
                src,
                from_partner[self.group],
                b_ss.at[self.group],
                b_rs.at[self.group],
                at_f(partner),
            )

        def ship(self, k):
            chip = flip(p, k)
            return remote(
                sums[self.group].at[chip],
                landing[self.group].at[k - 1],
                i_ss.at[self.group, k - 1],
                i_rs.at[self.group, k - 1],
                at_f(chip * 2 + c),
            )

        def blocks_of(self, core, lanes):
            left = jnp.concatenate(
                [self.turned[span(q * 2 + core, shard), :] for q in range(chips)], axis=0
            )
            value = mm(left, self.terms[:, lanes])
            return [value[q * shard : (q + 1) * shard] for q in range(chips)]

        def release(self):
            self.hand_over().wait_send()

        def send_all(self):
            if handing:
                handing.pop().release()

            def tile(lanes):
                for q, value in enumerate(self.blocks_of(1 - c, lanes)):
                    send_b[q, :, lanes] = value.astype(BF)

            tiles(self.width, tile)
            self.hand_over().start()
            handing.append(self)

        def own_sums(self):
            self.hand_over().wait_recv()

            def tile(lanes):
                for q, value in enumerate(self.blocks_of(c, lanes)):
                    other = from_partner[self.group][q, :, lanes].astype(F32)
                    sums[self.group][q, :, lanes] = (value + other).astype(BF)

            tiles(self.width, tile)

        def ship_all(self):
            if self.group < 2:
                for k in range(1, chips):
                    self.ship(k).start()
                return

            for core, first, second in ((0, near, far), (1, far, near)):

                @pl.when(c == core)
                def _():
                    for k in second:
                        for other in first:
                            self.via(other, k).start()
                        self.ship(k).start()

        def via(self, first, second):
            return remote(
                sums[self.group].at[flip(p, first + second)],
                between[self.group - 2].at[both_axes.index(first + second)],
                v_ss.at[self.group, first + second],
                v_rs.at[self.group, first + second],
                at_f(flip(p, second) * 2 + c),
            )

        def relay(self):
            for core, first, second in ((0, near, far), (1, far, near)):

                @pl.when(c == core)
                def _():
                    for k in first:
                        chip = flip(p, k)
                        for other in second:
                            self.via(k, other).wait_recv()
                            held = between[self.group - 2].at[both_axes.index(k + other)]

                            def tile(lanes):
                                total_here = sums[self.group][chip, :, lanes].astype(F32)
                                total_here = total_here + held[:, lanes].astype(F32)
                                sums[self.group][chip, :, lanes] = total_here.astype(BF)

                            tiles(self.width, tile)
                        self.ship(k).start()

        def partners(self):
            return near + far if self.group >= 2 else list(range(1, chips))

        def own_all(self):
            self.own_sums()
            self.ship_all()

        def fetch(self, k):
            return pltpu.make_async_copy(
                landing[self.group].at[k - 1],
                stage.at[k - 1, :, pl.ds(0, self.width)],
                l_sem.at[k - 1],
            )

        def collect(self):
            for k in self.partners():
                self.ship(k).wait()
                if self.group >= 2:
                    self.fetch(k).start()
            if self.group >= 2:
                for k in near:
                    for other in far:
                        self.via(k, other).wait_send()

        def finish(self):
            if self.group >= 2:
                for k in self.partners():
                    self.fetch(k).wait()

            def parts(lanes):
                yield sums[self.group][p, :, lanes]
                for k in self.partners():
                    if self.group >= 2:
                        yield stage[k - 1, :, lanes]
                    else:
                        yield landing[self.group][k - 1, :, lanes]

            self.emit(parts)

    def total_of(values):
        result = None
        for value in values:
            result = value if result is None else result + value
        return result

    stores = []

    def store(src, dst):
        copy = pltpu.make_async_copy(src, dst, out_sem.at[len(stores)])
        copy.start()
        stores.append(copy)

    def emit_plain(out):
        def emit(parts):
            def tile(t):
                big_own[:, cols(t)] = total_of(v.astype(F32) for v in parts(cols(t)))

            if big_stores:
                big_stores.pop().wait()
            loop(ff // TILE, tile)
            copy = pltpu.make_async_copy(big_own, out, l_sem.at[chips - 1])
            copy.start()
            big_stores.append(copy)

        return emit

    big_stores = []

    def summed(parts, start, size):
        return total_of(v.astype(F32) for v in parts(pl.ds(start, size)))

    q_real, kv_real = nq * HD, nkv * HD

    def emit_out(parts):
        o_own[...] = summed(parts, 0, q_real)
        store(o_own, out_o)

    def emit_qkv(parts):
        q_own[...] = summed(parts, 0, q_real)
        store(q_own, out_q)
        k_own[...] = summed(parts, q_real, kv_real)
        store(k_own, out_k)
        v_own[...] = summed(parts, q_real + kv_real, kv_real)
        store(v_own, out_v)

    def fill(dst, r, value):
        spare = dst.shape[1] - value.shape[1]
        if spare:
            value = jnp.concatenate([value, jnp.zeros((value.shape[0], spare), F32)], axis=1)
        dst[r, :] = value.astype(BF)

    def pack_mixed():
        def one(b):
            r = span(b, rows)
            fill(mixed_pack, r, mm_nt(mixed[r, :], pick_end[...]))

        loop(n, one)

    def pack_gqkv():
        def one(b):
            r = span(b, rows)
            keys = slice(q_wide, q_wide + kv_wide)
            vals = slice(q_wide + kv_wide, q_wide + 2 * kv_wide)
            value = jnp.concatenate(
                [
                    mm_nt(gqkv[r, 0:q_wide], pick_rope[...]),
                    mm_nt(gqkv[r, keys], pick_rope[0:kv_real, 0:kv_wide]),
                    mm_nt(gqkv[r, vals], pick_end[0:kv_real, 0:kv_wide]),
                ],
                axis=1,
            )
            fill(gqkv_pack, r, value)

        loop(n, one)

    def turn(src, dst):
        def lane_block(t):
            dst[cols(t, LANES), :] = src[pl.ds(0, total), cols(t, LANES)].T

        loop(width // LANES, lane_block)

    def at(s, work):
        if s == 0:
            work(d)
            return

        def side(i):
            j = d - s + 2 * s * i

            @pl.when((j >= 0) & (j < n))
            def _():
                work(j)

        loop(2, side)

    def one_hot(split):
        shape = (nq * HD, q_wide)
        row = lax.broadcasted_iota(jnp.int32, shape, 0)
        lane = lax.broadcasted_iota(jnp.int32, shape, 1)
        inside = lane % LANES
        start = (lane // LANES) * HD
        if split:
            gap = LANES // 2 - HALF
            upper = inside >= LANES // 2
            source = start + jnp.where(upper, inside - gap, inside)
            real = (inside % (LANES // 2)) < HALF
        else:
            source = start + inside
            real = inside < HD
        return jnp.where(real & (row == source), 1.0, 0.0).astype(BF)

    pick_rope[...] = one_hot(True)
    pick_end[...] = one_hot(False)
    for copy in loads[7:]:
        copy.wait()
    gain_mine = block(gain_in, f, 8)
    gain_mine[...] = jnp.zeros(gain_mine.shape, F32)
    gain_mine[0:1, 0:shard] = gain_a[...].astype(F32)
    gain_mine[1:2, 0:shard] = gain_m[...].astype(F32)

    gathers = [
        Gather(0, weights[0], shard, plain=True),
        Gather(1, weights[1], shard, plain=True),
        Gather(2, weights[2], shard, w_g),
        Gather(3, weights[3], shard, w_u),
        Gather(4, weights[4], shard, w_d),
    ]
    gain_gather = Gather(5, gain_in, 8, plain=True)
    tok_line = Line(0, x_buf, parts=2, src=tokens)
    cot_line = Line(1, ct_buf, src=cot)
    mi_line = Line(2, mi_buf, parts=2)
    gm_line = Line(3, gm_buf, parts=2)

    def gain_swap(k):
        mine = block(gain_z, d, 8)
        return remote(
            mine, mine, z_ss.at[4, 0, 0, k], z_rs.at[4, 0, d], at_d((d + k) % n)
        )

    def gain_got(k):
        other = (d + k) % n
        part = block(gain_z, other, 8)
        remote(part, part, z_ss.at[4, 0, 0, k], z_rs.at[4, 0, other], at_d(d)).wait_recv()

    def segments(b, shape, dim):
        index = lax.broadcasted_iota(jnp.int32, shape, dim)
        segment = jnp.zeros(shape, jnp.int32)
        offset = jnp.zeros(shape, jnp.int32)
        end = jnp.int32(0)
        for k in range(nseq):
            end = end + lengths[b, k]
            past = index >= end
            segment = segment + past.astype(jnp.int32)
            offset = jnp.where(past, end, offset)
        return index, segment, offset

    def tables(b):
        index, _, offset = segments(b, (rows, LANES), 0)
        angle = (index - offset).astype(F32) * freq[...]
        lane = lax.broadcasted_iota(jnp.int32, (rows, LANES), 1)
        sine = jnp.sin(angle)
        block(cos_t, b)[...] = jnp.cos(angle)
        block(sin_t, b)[...] = jnp.where(lane < LANES // 2, -sine, sine)

    pl.semaphore_wait(barrier, chips + n - 1)
    for h in range(2):
        tok_line.start(h)

    @pl.when(end)
    def _():
        cot_line.start()

    gain_gather.start()
    mine = span(f, shard)
    kv_rows = nkv * HD
    for copy in loads[:4]:
        copy.wait()
    weights[0][mine, 0:q_wide] = mm(q_in[...], pick_rope[...]).astype(BF)
    weights[0][mine, q_wide : q_wide + kv_wide] = mm(
        k_in[...], pick_rope[0:kv_rows, 0:kv_wide]
    ).astype(BF)
    weights[0][mine, q_wide + kv_wide : q_wide + 2 * kv_wide] = mm(
        v_in[...], pick_end[0:kv_rows, 0:kv_wide]
    ).astype(BF)
    gathers[0].start()
    weights[1][mine, :] = mm(o_in[...], pick_end[...]).astype(BF)
    for g in range(1, 5):
        gathers[g].start()
    loop(n, tables)
    loads[4].wait()
    gain_gather.forward()
    gain_gather.finish()
    for k in range(nf):
        gain_row[:, k * shard : (k + 1) * shard] = gain_in[8 * k : 8 * k + 8, 0:shard]

    def rms(value):
        mean = jnp.sum(value * value, axis=-1, keepdims=True) / width
        return lax.rsqrt(mean + EPSILON)

    def norm_one(j):
        def some(i):
            r = pl.ds(pl.multiple_of(j * rows + i * CHUNK, CHUNK), CHUNK)
            value = x_buf[r, :].astype(F32)
            scale = rms(value)
            sc_one[r, :] = scale
            mi_buf[r, :] = (value * scale * gain_row[0:1, :]).astype(BF)

        loop(rows // CHUNK, some)

    def rope(value, sign, cos_v, sin_v):
        return value * cos_v + sign * (pltpu.roll(value, LANES // 2, 1) * sin_v)

    heads = nq + 2 * nkv

    def head(ref, r, h):
        return ref[r, h * LANES : (h + 1) * LANES]

    def attend(b):
        r = span(b, rows)
        cos_v, sin_v = cos_t[r, :], sin_t[r, :]
        for t in range(heads // 2):
            both = mm(mi_buf[r, :], weights[0][:, 2 * t * LANES : 2 * (t + 1) * LANES])
            for h in (2 * t, 2 * t + 1):
                value = both[:, (h - 2 * t) * LANES : (h - 2 * t + 1) * LANES]
                if h < nq + nkv:
                    value = rope(value, 1.0, cos_v, sin_v)
                qkv[r, h * LANES : (h + 1) * LANES] = value.astype(BF)
        t_index, t_seg, _ = segments(b, (rows, rows), 0)
        s_index, s_seg, _ = segments(b, (rows, rows), 1)
        allowed = (t_seg == s_seg) & (s_index <= t_index)
        for h in range(nq):
            kv = h // (nq // nkv)
            score = mm_nt(head(qkv, r, h), head(qkv, r, nq + kv)) * HD ** (-0.5)
            score = jnp.where(allowed, score, NEG_FILL)
            top = jnp.max(score, axis=-1, keepdims=True)
            log_total = top + jnp.log(jnp.sum(jnp.exp(score - top), axis=-1, keepdims=True))
            prob = jnp.where(allowed, jnp.exp(score - log_total), 0.0)
            probs[b * nq + h] = prob
            mixed[r, h * LANES : (h + 1) * LANES] = mm(
                prob.astype(BF), head(qkv, r, nq + nkv + kv)
            ).astype(BF)

    def tokens_at(s):
        for h in range(2):
            tok_line.step(s, h)
            tok_line.arrive(s, h)

    norm_one(d)
    tokens_at(1)
    at(1, norm_one)
    early = min(2, n - 1)
    if early == 2:
        for h in range(2):
            tok_line.step(2, h)

    @pl.when((d > 0) & (d < n - 1))
    def _():
        cot_line.start()

    gathers[0].forward()
    if early == 2:
        for h in range(2):
            tok_line.arrive(2, h)
        at(2, norm_one)
    gathers[0].finish()
    for s in range(early + 1):
        at(s, attend)
    gathers[1].forward()
    cot_line.outward(1)
    for s in range(early + 1, n):
        tokens_at(s)
        at(s, norm_one)
        at(s, attend)
    gathers[1].finish()

    def by_turned(pairs):
        def tile_of(t, r):
            return total_of(mm_nt(left[r, :], weight[cols(t), :]) for left, weight in pairs)

        return tile_of

    def run(work):
        if work:
            todo = work.pop(0)
            if todo is not None:
                todo()

    def reduce_then_gather(red, finish_half, line, work):
        red.compute()
        red.launch(True)
        run(work)
        for s in range(n - 2, 0, -1):
            red.advance(s, 0)
            run(work)
        red.final(0)
        finish_half(0)
        line.start(0)
        run(work)
        for i in range(1, n - 1):
            red.advance(n - 1 - i, 1)
            if i == 1:
                line.inward(i, 0)
            run(work)
        red.final(1)
        finish_half(1)
        line.start(1)
        for i in range(1, n - 1):
            if i > 1:
                line.inward(i, 0)
            line.outward(i, 0)

    def arrived(line, s):
        line.step(s, 1)
        line.arrive(s, 0)
        line.arrive(s, 1)

    def norm_two(h):
        def some(i):
            r = pl.ds(pl.multiple_of(h * half + i * CHUNK, CHUNK), CHUNK)
            here = pl.ds(pl.multiple_of(d * rows + h * half + i * CHUNK, CHUNK), CHUNK)
            value = x_buf[here, :].astype(F32) + own_sum[r, :]
            scale = rms(value)
            middle[r, :] = value
            sc_two[r, :] = scale
            mi_buf[here, :] = (value * scale * gain_row[1:2, :]).astype(BF)

        loop(half // CHUNK, some)

    def both(*todo):
        def do():
            for one in todo:
                one()

        return do

    def cot_on(s):
        def do():
            cot_line.inward(s)
            if s > 1:
                cot_line.outward(s)

        return do

    after_attn = Reduce(0, by_turned([(mixed, weights[1])]), s_buf, r_buf)
    work = [cot_on(1)]
    work += [both(cot_on(2), gathers[2].relay)] if n > 2 else [gathers[2].relay]
    work += [gathers[3].relay, None, gathers[4].relay, gathers[2].forward]
    work += [cot_on(s) for s in range(3, n - 1)]
    reduce_then_gather(after_attn, norm_two, mi_line, work)
    while work:
        run(work)
    pack_mixed()
    gathers[3].forward()
    gathers[4].forward()
    for g in (2, 3, 4):
        gathers[g].finish()
    loads[5].wait()
    loads[6].wait()

    def feed(j):
        r = span(j, rows)

        def tile(t):
            left = mi_buf[r, :]
            gate = mm(left, weights[2][:, cols(t)])
            up = mm(left, weights[3][:, cols(t)])
            grad_hidden = mm(ct_buf[r, :], weights[4][:, cols(t)])
            sig = 1.0 / (1.0 + jnp.exp(-gate))
            hid[r, cols(t)] = (gate * sig * up).astype(BF)
            gu[r, cols(t)] = (grad_hidden * gate * sig).astype(BF)
            gg[r, cols(t)] = (grad_hidden * up * sig * (1.0 + gate * (1.0 - sig))).astype(BF)

        loop(ff // TILE, tile)

    def at_outer(work):
        @pl.when((outer >= 0) & (outer < n))
        def _():
            work(outer)

    after_mlp = Reduce(1, by_turned([(gg, weights[2]), (gu, weights[3])]), s_buf, r_buf)
    after_attn.drain()
    at(0, feed)
    mi_line.step(1, 1)
    for s in range(1, n):
        for h in range(2):
            mi_line.arrive(s, h)
        cot_line.arrive(s)
        at(s, feed)
        if s + 1 < n:
            mi_line.step(s + 1, 1)
        if s == 1:
            after_mlp.pair()
            after_mlp.send_at(1)
            at_outer(after_mlp.single)
        else:
            at(s, after_mlp.single)
            after_mlp.send_at(s)

    gain_own[...] = jnp.zeros((8, width), F32)

    def back_two(h):
        def some(i):
            r = pl.ds(pl.multiple_of(h * half + i * CHUNK, CHUNK), CHUNK)
            term = own_sum[r, :]
            scale = sc_two[r, :]
            normed = middle[r, :] * scale
            gain_sum = jnp.sum(term * normed, axis=0, keepdims=True)
            dn = term * gain_row[1:2, :]
            mean = jnp.sum(dn * normed, axis=-1, keepdims=True) / width
            here = pl.ds(pl.multiple_of(d * rows + h * half + i * CHUNK, CHUNK), CHUNK)
            value = cot_own[r, :].astype(F32) + scale * (dn - normed * mean)
            gmid[r, :] = value
            gm_buf[here, :] = value.astype(BF)
            gain_own[1:2, :] = gain_own[1:2, :] + gain_sum

        loop(half // CHUNK, some)

    down = Grad(4, t_one, hid, emit_plain(out_d))
    gate_g = Grad(2, t_two, gg, emit_plain(out_g))
    up_g = Grad(3, t_two, gu, emit_plain(out_u))

    def turn_mi():
        turn(mi_buf, t_two)

    def attn_in_again(j):
        def some(i):
            r = pl.ds(pl.multiple_of(j * rows + i * CHUNK, CHUNK), CHUNK)
            value = x_buf[r, :].astype(F32) * sc_one[r, :]
            s_buf[r, :] = (value * gain_row[0:1, :]).astype(BF)

        loop(rows // CHUNK, some)

    output = Reduce(2, by_turned([(hid, weights[4])]), ct_buf, r_two)

    fits = widths[0] <= width and 3 * ff >= width and ff % TILE == 0

    def turn_qkv():
        for t in range(width // LANES if fits else 0):
            at_lane = t * LANES
            dst = weights[2 + at_lane // ff]
            dst[0 : widths[0], at_lane % ff : at_lane % ff + LANES] = weights[0][
                at_lane : at_lane + LANES, :
            ].T

    def finish_mlp():
        for h in range(2):
            after_mlp.final(h)
            back_two(h)
            if h == 0:
                gm_line.start(h)

    turn(ct_buf, t_one)
    cot_line.drain()
    turn_mi()
    down.send_all()
    for h in range(2):
        after_mlp.out_adv(1, h)
    output.compute(keep=False)
    output.send_at(n - 1)
    down.own_all()
    for s in range(2, n - 1):
        for h in range(2):
            after_mlp.out_adv(s, h)

    @pl.when(jnp.logical_not(end))
    def _():
        finish_mlp()

    gate_g.send_all()
    for g in (2, 3, 4):
        gathers[g].drain()
    turn_qkv()
    work = [both(gate_g.own_all, down.relay), up_g.send_all]
    for s in range(1, n - 1):
        for h in range(2):
            after_mlp.in_adv(s, h)
            run(work)
    while work:
        run(work)

    @pl.when(jnp.logical_not(end))
    def _():
        gm_line.start(1)

    gm_line.inward(1, 0)
    up_g.own_all()
    gm_line.inward(1, 1)
    gm_line.outward(1, 0)
    gm_line.outward(1, 1)

    @pl.when(end)
    def _():
        finish_mlp()
        gm_line.start(1)

    for s in range(n - 2, 1, -1):
        output.send_at(s)

    gate_g.relay()
    after_mlp.drain()
    mi_line.drain()

    def back(b):
        r = span(b, rows)

        def tile(t):
            gmixed[r, cols(t)] = mm(gm_buf[r, :], weights[1][:, cols(t)]).astype(BF)

        loop(q_wide // TILE, tile)
        cos_v, sin_v = cos_t[r, :], sin_t[r, :]
        group = nq // nkv
        for kv in range(nkv):
            key, val = head(qkv, r, nq + kv), head(qkv, r, nq + nkv + kv)
            grad_k = grad_v = None
            for h in range(kv * group, (kv + 1) * group):
                query, gm_h = head(qkv, r, h), head(gmixed, r, h)
                prob = probs[b * nq + h]
                delta = jnp.sum(
                    gm_h.astype(F32) * head(mixed, r, h).astype(F32), axis=-1, keepdims=True
                )
                grad_p = mm_nt(gm_h, val)
                grad_s = (prob * (grad_p - delta) * HD ** (-0.5)).astype(BF)
                grad_q = mm(grad_s, key)
                gqkv[r, h * LANES : (h + 1) * LANES] = rope(grad_q, -1.0, cos_v, sin_v).astype(BF)
                k_term, v_term = mm_tn(grad_s, query), mm_tn(prob.astype(BF), gm_h)
                grad_k = k_term if grad_k is None else grad_k + k_term
                grad_v = v_term if grad_v is None else grad_v + v_term
            k_at, v_at = (nq + kv) * LANES, (nq + nkv + kv) * LANES
            gqkv[r, k_at : k_at + LANES] = rope(grad_k, -1.0, cos_v, sin_v).astype(BF)
            gqkv[r, v_at : v_at + LANES] = grad_v.astype(BF)

    def add_gain(t, value, r):
        normed = x_buf[r, cols(t)].astype(F32) * sc_one[r, :]
        gain_own[0:1, cols(t)] = gain_own[0:1, cols(t)] + jnp.sum(
            value * normed, axis=0, keepdims=True
        )

    def by_qkv():
        if not fits:
            return by_turned([(gqkv, weights[0])])

        def tile_of(t, r):
            at_lane = t * TILE
            held = weights[2 + at_lane // ff]
            return mm(gqkv[r, :], held[0 : widths[0], at_lane % ff : at_lane % ff + TILE])

        return tile_of

    after_in = Reduce(3, by_qkv(), s_buf, r_buf, add_gain, plain=fits)
    out_g_grad = Grad(1, t_one, mixed_pack, emit_out)
    qkv_g = Grad(0, t_two, gqkv_pack, emit_qkv)

    def pass_gm(h):
        for s in range(2, n - 1):
            gm_line.inward(s, h)
            gm_line.outward(s, h)

    at(0, back)
    pass_gm(0)
    for h in range(2):
        gm_line.arrive(1, h)
    back(inner)
    pass_gm(1)
    for s in range(n - 2, 1, -1):
        for h in range(2):
            output.out_adv(s, h)
    loop(n, attn_in_again)
    turn(s_buf, t_two)
    after_in.pair()
    after_in.send_at(1)
    if n > 2:
        for h in range(2):
            output.out_adv(1, h)

    def outer_back(j):
        back(j)
        after_in.single(j)

    at_outer(outer_back)
    for s in range(2, n):
        for h in range(2):
            gm_line.arrive(s, h)
        at(s, outer_back)
        if s == 2:
            up_g.relay()
    if n == 2:
        up_g.relay()
    quarter = width // 4
    gain_mine = block(gain_z, d, 8)
    for i in range(8):
        gain_mine[i : i + 1, :] = gain_own[i // 4 : i // 4 + 1, pl.ds(i % 4 * quarter, quarter)]
    for k in range(1, n):
        gain_swap(k).start()
    for s in range(n - 1, 1, -1):
        after_in.send_at(s)
    if n > 2:
        output.send_at(1)
    for s in range(1, n - 1):
        for h in range(2):
            output.in_adv(s, h)
    turn(gm_buf, t_one)
    out_g_grad.send_all()
    pack_gqkv()
    out_g_grad.own_all()
    qkv_g.send_all()
    for h in range(2):
        after_in.out_adv(n - 2, h)
    qkv_g.own_sums()
    for k in range(1, n):
        gain_got(k)
    block(gain_f, f, 8)[...] = total_of(gain_z[8 * k : 8 * k + 8, :] for k in range(n))
    gain_back = Gather(6, gain_f, 8, plain=True)
    gain_back.start()
    qkv_g.ship_all()
    for s in range(n - 2, 0, -1):
        for h in range(2):
            after_in.in_adv(s, h)
        if s < n - 2:
            for h in range(2):
                after_in.out_adv(s, h)

    def output_end():
        middle[...] = middle[...] + block(ct_buf, d)[...].astype(F32)
        for h in range(2):
            output.final_into(middle, h)
        out_own[...] = middle[...].astype(BF)
        store(out_own, out_ref)

    def gain_end():
        gain_back.forward()
        gain_back.finish()
        gain_all = total_of(gain_f[8 * k : 8 * k + 8, :] for k in range(nf))
        for i in range(8):
            gain_own[i // 4 : i // 4 + 1, pl.ds(i % 4 * quarter, quarter)] = gain_all[i : i + 1, :]
        gain_all = pltpu.roll(gain_own[...], (width - f * shard) % width, 1)
        out_ga[...] = gain_all[0:1, 0:shard]
        out_gm[...] = gain_all[1:2, 0:shard]

    work = [gain_end]
    for grad in (down, gate_g, up_g):
        work.append(both(grad.collect, grad.finish))
    while work:
        run(work)

    def back_one(h):
        def some(i):
            r = pl.ds(pl.multiple_of(h * half + i * CHUNK, CHUNK), CHUNK)
            there = pl.ds(pl.multiple_of(d * rows + h * half + i * CHUNK, CHUNK), CHUNK)
            scale = sc_one[there, :]
            normed = x_buf[there, :].astype(F32) * scale
            dm = own_sum[r, :] * gain_row[0:1, :]
            mean = jnp.sum(dm * normed, axis=-1, keepdims=True) / width
            gmid[r, :] = gmid[r, :] + scale * (dm - normed * mean)

        loop(half // CHUNK, some)

    for h in range(2):
        after_in.final(h)
        back_one(h)
        part = pl.ds(h * half, half)
        store(gmid.at[part], gtok_ref.at[part])
    output_end()
    for grad in (qkv_g, out_g_grad):
        grad.collect()
        grad.finish()

    handing.pop().release()
    output.drain()
    after_in.drain()
    tok_line.drain()
    gm_line.drain()
    for k in range(1, n):
        gain_swap(k).wait_send()
    for gather in gathers[:2] + [gain_gather, gain_back]:
        gather.drain()
    big_stores.pop().wait()
    for copy in stores:
        copy.wait()


def pass_on(*refs):
    count = (len(refs) - 2) // 3
    srcs, dsts, held = refs[:count], refs[count : 2 * count], refs[2 * count : 3 * count]
    in_sem, out_sem = refs[3 * count :]
    order = range(count)
    for i in order:
        pltpu.make_async_copy(srcs[i], held[i], in_sem.at[i]).start()
    for i in order:
        pltpu.make_async_copy(srcs[i], held[i], in_sem.at[i]).wait()
        pltpu.make_async_copy(held[i], dsts[i], out_sem.at[i]).start()
    for i in order:
        pltpu.make_async_copy(held[i], dsts[i], out_sem.at[i]).wait()


def run_layer(lengths, freq, tokens, cot, gain_a, gain_m, w_q, w_k, w_v, w_o, w_d, w_g, w_u, n, chips):
    rows, width = tokens.shape
    nq = w_q.shape[1] // HD
    nkv = w_k.shape[1] // HD
    total = n * rows
    nf = 2 * chips
    shard = w_q.shape[0]
    ff = w_g.shape[1]
    q_wide, kv_wide = nq * LANES, nkv * LANES
    widths = (q_wide + 2 * kv_wide, q_wide, ff, ff, ff)
    dims = (n, chips, rows, width, nq, nkv, ff, lengths.shape[1])
    vmem = pl.BlockSpec(memory_space=pltpu.VMEM)
    hbm = pl.BlockSpec(memory_space=pltpu.HBM)
    results = [
        jax.ShapeDtypeStruct((rows, width), BF),
        jax.ShapeDtypeStruct((rows, width), F32),
        jax.ShapeDtypeStruct((1, shard), F32),
        jax.ShapeDtypeStruct((1, shard), F32),
    ] + [jax.ShapeDtypeStruct(w.shape, F32) for w in (w_q, w_k, w_v, w_o, w_g, w_u, w_d)]
    out_shape = results + [jax.ShapeDtypeStruct((chips - 1, shard, w), BF) for w in widths[2:]]
    gwidths = packed_widths(nq, nkv, ff)
    widest = max(gwidths)
    scratch = (
        [pltpu.VMEM((chips - 1, shard, w), BF) for w in gwidths[:2]]
        + [pltpu.VMEM((width, w), BF) for w in widths]
        + [
            pltpu.VMEM((total, width), BF),
            pltpu.VMEM((total, width), BF),
            pltpu.VMEM((total, width), BF),
            pltpu.VMEM((total, width), BF),
            pltpu.VMEM((total + rows, width), BF),
            pltpu.VMEM((rows, width), BF),
            pltpu.VMEM((total, widths[0]), BF),
            pltpu.VMEM((total, widths[0]), BF),
            pltpu.VMEM((n * nq, rows, rows), F32),
            pltpu.VMEM((total, q_wide), BF),
            pltpu.VMEM((total, q_wide), BF),
            pltpu.VMEM((total, ff), BF),
            pltpu.VMEM((total, ff), BF),
            pltpu.VMEM((total, ff), BF),
            pltpu.VMEM((total, gwidths[0]), BF),
            pltpu.VMEM((total, gwidths[1]), BF),
            pltpu.VMEM((width, total), BF),
            pltpu.VMEM((width, total), BF),
            pltpu.VMEM((total, width), BF),
            pltpu.VMEM((total + rows, width), BF),
            pltpu.VMEM((rows, width), F32),
            pltpu.VMEM((rows, width), F32),
            pltpu.VMEM((rows, width), F32),
            pltpu.VMEM((total, TILE), F32),
            pltpu.VMEM((total, 1), F32),
            pltpu.VMEM((rows, 1), F32),
            pltpu.VMEM((total, LANES), F32),
            pltpu.VMEM((total, LANES), F32),
            pltpu.VMEM((nf * 8, -(-shard // LANES) * LANES), F32),
            pltpu.VMEM((8, width), F32),
            pltpu.VMEM((8, width), F32),
            pltpu.VMEM((n * 8, width // 4), F32),
            pltpu.VMEM((nf * 8, width // 4), F32),
            pltpu.VMEM((chips - 1, shard, widest), BF),
            pltpu.VMEM((nq * HD, q_wide), BF),
            pltpu.VMEM((nq * HD, q_wide), BF),
        ]
        + [pltpu.VMEM(w.shape, BF) for w in (w_q, w_k, w_v, w_o)]
        + [
            pltpu.SMEM(lengths.shape, jnp.int32),
            pltpu.VMEM(freq.shape, F32),
            pltpu.VMEM(gain_a.shape, BF),
            pltpu.VMEM(gain_m.shape, BF),
        ]
        + [pltpu.VMEM((rows, width), BF)]
        + [pltpu.VMEM(w.shape, F32) for w in (w_q, w_k, w_v, w_o, w_g)]
        + [
            pltpu.VMEM((chips, shard, widest), BF),
        ]
        + [pltpu.VMEM((chips, shard, w), BF) for w in gwidths]
        + [pltpu.VMEM((chips, shard, w), BF) for w in gwidths]
        + [
            pltpu.SemaphoreType.DMA((7, chips)),
            pltpu.SemaphoreType.DMA((7, chips)),
            pltpu.SemaphoreType.DMA((7, chips)),
            pltpu.SemaphoreType.DMA((7, nf)),
            pltpu.SemaphoreType.DMA((7,)),
            pltpu.SemaphoreType.DMA((5, 2, 2, n)),
            pltpu.SemaphoreType.DMA((5, 2, n)),
            pltpu.SemaphoreType.DMA((4, 2, n)),
            pltpu.SemaphoreType.DMA((4, 2, n + 1)),
            pltpu.SemaphoreType.DMA((5,)),
            pltpu.SemaphoreType.DMA((5,)),
            pltpu.SemaphoreType.DMA((5, chips)),
            pltpu.SemaphoreType.DMA((5, chips)),
            pltpu.SemaphoreType.DMA((chips,)),
            pltpu.SemaphoreType.DMA((11,)),
            pltpu.SemaphoreType.DMA((7,)),
            pltpu.SemaphoreType.DMA((5, chips)),
            pltpu.SemaphoreType.DMA((5, chips)),
        ]
        + [pltpu.VMEM((max(1, chips // 2 - 1), shard, ff), BF)] * 3
    )
    made = pl.pallas_call(
        partial(layer_kernel, dims),
        out_shape=out_shape,
        in_specs=[hbm] * 13,
        out_specs=[hbm] * 2 + [vmem] * 2 + [hbm] * 10,
        scratch_shapes=scratch,
        compiler_params=pltpu.CompilerParams(
            collective_id=0, has_side_effects=True, vmem_limit_bytes=67043328
        ),
        name="layer",
    )(lengths, freq, gain_a, gain_m, tokens, cot, w_q, w_k, w_v, w_o, w_d, w_g, w_u)
    count = len(results)
    return pl.pallas_call(
        pass_on,
        out_shape=results,
        in_specs=[hbm] * count,
        out_specs=[hbm] * count,
        scratch_shapes=[pltpu.VMEM(r.shape, r.dtype) for r in results]
        + [pltpu.SemaphoreType.DMA((count,)), pltpu.SemaphoreType.DMA((count,))],
        compiler_params=pltpu.CompilerParams(vmem_limit_bytes=67043328),
        name="results",
    )(*made[:count])


def body(
    n,
    chips,
    tokens,
    lengths,
    cotangent,
    attn_gain,
    w_query,
    w_key,
    w_value,
    w_out,
    mlp_gain,
    w_gate,
    w_up,
    w_down,
):
    frequency = np.float64(ROPE_BASE) ** (-np.arange(HALF) / HALF)
    frequency = np.pad(frequency, (0, LANES // 2 - HALF))
    freq = jnp.asarray(np.concatenate([frequency, frequency])[None, :], F32)
    results = run_layer(
        lengths,
        freq,
        tokens,
        cotangent,
        attn_gain,
        mlp_gain,
        w_query[0],
        w_key[0],
        w_value[0],
        w_out[0].T,
        w_down[0].T,
        w_gate[0],
        w_up[0],
        n,
        chips,
    )
    output, grad_tokens, g_again, g_mgain, g_q, g_k, g_v, g_o, g_gate, g_up, g_down = results
    return (
        output,
        grad_tokens,
        g_again,
        g_q[None],
        g_k[None],
        g_v[None],
        g_o.T[None],
        g_mgain,
        g_gate[None],
        g_up[None],
        g_down.T[None],
    )


def solution(mesh):
    placed = (
        P(("fsdp", "dp"), None),
        P("fsdp", None),
        P(("fsdp", "dp"), None),
        P(None, "fsdp"),
        P(None, "fsdp", "dp"),
        P(None, "fsdp", "dp"),
        P(None, "fsdp", "dp"),
        P(None, "dp", "fsdp"),
        P(None, "fsdp"),
        P(None, "fsdp", "dp"),
        P(None, "fsdp", "dp"),
        P(None, "dp", "fsdp"),
    )
    return jax.shard_map(
        partial(body, mesh.shape["dp"], mesh.shape["fsdp"] // 2),
        mesh=mesh,
        in_specs=placed,
        out_specs=(
            P(("fsdp", "dp"), None),
            P(("fsdp", "dp"), None),
            P(None, "fsdp"),
            P(None, "fsdp", "dp"),
            P(None, "fsdp", "dp"),
            P(None, "fsdp", "dp"),
            P(None, "dp", "fsdp"),
            P(None, "fsdp"),
            P(None, "fsdp", "dp"),
            P(None, "fsdp", "dp"),
            P(None, "dp", "fsdp"),
        ),
        check_vma=False,
    )
```

```python
from functools import partial

import jax
import jax.numpy as jnp
import numpy as np
from jax import lax
from jax.experimental import pallas as pl
from jax.experimental.pallas import tpu as pltpu
from jax.sharding import PartitionSpec as P

HD = 96
HALF = 48
LANES = 128
EPSILON = 1e-05
ROPE_BASE = 100000.0
NEG_FILL = -1e30
MESH = pl.DeviceIdType.MESH
BF = jnp.bfloat16
F32 = jnp.float32
TILE = 256
CHUNK = 32


def mm(left, right):
    return jnp.dot(left, right, preferred_element_type=F32)


def mm_nt(left, right):
    return lax.dot_general(left, right, (((1,), (1,)), ((), ())), preferred_element_type=F32)


def mm_tn(left, right):
    return lax.dot_general(left, right, (((0,), (0,)), ((), ())), preferred_element_type=F32)


def loop(count, body):
    def step(index, carry):
        body(index)
        return carry

    lax.fori_loop(0, count, step, 0)


def whole_lanes(count):
    return -(-count // LANES) * LANES


def packed_widths(nq, nkv, ff):
    return (whole_lanes((nq + 2 * nkv) * HD), whole_lanes(nq * HD), ff, ff, ff)


def flip(chip, bits):
    other, bit = chip, 1
    while bit <= bits:
        if bits & bit:
            other = other + bit * (1 - 2 * ((chip // bit) % 2))
        bit *= 2
    return other


def layer_kernel(dims, *refs):
    n, chips, rows, width, nq, nkv, ff, nseq = dims
    nf = 2 * chips
    shard = width // nf
    total = n * rows
    half = rows // 2
    q_wide, kv_wide = nq * LANES, nkv * LANES
    widths = (q_wide + 2 * kv_wide, q_wide, ff, ff, ff)
    gwidths = packed_widths(nq, nkv, ff)
    widest = max(gwidths)
    near = [1] if chips > 1 else []
    far = [2 * k for k in range(1, chips // 2)]
    both_axes = [k + other for k in near for other in far]
    refs = list(refs)

    def take(count):
        taken = refs[:count]
        del refs[:count]
        return taken

    (lengths_in, freq_in, gain_a_in, gain_m_in) = take(4)
    (tokens, cot, w_q, w_k, w_v, w_o, w_d, w_g, w_u) = take(9)
    (out_ref, gtok_ref, out_ga, out_gm, out_q, out_k, out_v, out_o, out_g, out_u, out_d) = take(11)
    far_landing = take(3)
    near_landing = take(2)
    landing = near_landing + far_landing
    weights = take(5)
    (x_buf, ct_buf, mi_buf, gm_buf, r_two, cot_own) = take(6)
    (qkv, gqkv, probs, mixed, gmixed, hid, gg, gu, gqkv_pack, mixed_pack) = take(10)
    (t_one, t_two) = take(2)
    (s_buf, r_buf, own_sum, middle, gmid, wide_tile) = take(6)
    (sc_one, sc_two, cos_t, sin_t) = take(4)
    (gain_in, gain_row, gain_own, gain_z, gain_f, stage) = take(6)
    (pick_rope, pick_end) = take(2)
    (q_in, k_in, v_in, o_in) = take(4)
    (lengths, freq, gain_a, gain_m) = take(4)
    (out_own, q_own, k_own, v_own, o_own, big_own) = take(6)
    send_b, send_c = take(2)
    sums = take(5)
    from_partner = take(5)
    (w_ss, w_fs, w_qs, w_rs, w_ls) = take(5)
    (z_ss, z_rs) = take(2)
    (rs_ss, rs_rs) = take(2)
    (b_ss, b_rs, i_ss, i_rs, l_sem, in_sem, out_sem, v_ss, v_rs) = take(9)
    between = take(3)

    f = lax.axis_index("fsdp")
    d = lax.axis_index("dp")
    p = f // 2
    c = f % 2

    def at_f(index):
        return {"fsdp": index, "dp": d}

    def at_d(index):
        return {"fsdp": f, "dp": index}

    partner = p * 2 + 1 - c
    low = 1 - d // (n // 2)
    inner, outer = d - 1 + 2 * low, d + 1 - 2 * low
    end = (d == 0) | (d == n - 1)

    def remote(src, dst, ss, rs, where):
        return pltpu.make_async_remote_copy(
            src_ref=src, dst_ref=dst, send_sem=ss, recv_sem=rs, device_id=where, device_id_type=MESH
        )

    def span(index, size):
        return pl.ds(pl.multiple_of(index * size, size), size)

    def block(ref, index, size=rows):
        return ref.at[span(index, size)]

    def cols(index, size=TILE):
        if isinstance(index, int):
            return pl.ds(index * size, size)
        return span(index, size)

    loads = [
        pltpu.make_async_copy(src, dst, in_sem.at[i])
        for i, (src, dst) in enumerate(
            (
                (w_q, q_in),
                (w_k, k_in),
                (w_v, v_in),
                (w_o, o_in),
                (tokens, block(x_buf, d)),
                (cot, block(ct_buf, d)),
                (cot, cot_own),
                (lengths_in, lengths),
                (freq_in, freq),
                (gain_a_in, gain_a),
                (gain_m_in, gain_m),
            )
        )
    ]
    for copy in loads:
        copy.start()

    barrier = pltpu.get_barrier_semaphore()
    for k in range(1, chips):
        pl.semaphore_signal(
            barrier, inc=1, device_id=at_f(flip(p, k) * 2 + c), device_id_type=MESH
        )
    pl.semaphore_signal(barrier, inc=1, device_id=at_f(partner), device_id_type=MESH)

    for k in range(1, n):
        pl.semaphore_signal(
            barrier, inc=1, device_id=at_d((d + k) % n), device_id_type=MESH
        )

    class Gather:
        def __init__(self, slot, dst, size, src=None, plain=False):
            self.slot, self.dst, self.size = slot, dst, size
            self.src = self.part(f) if src is None else src
            self.local = src is not None
            self.aimed = list(range(1, chips)) if plain else near + far
            self.plain = plain

        def part(self, index):
            return block(self.dst, index, self.size)

        def direct(self, k):
            where = partner if k == 0 else flip(p, k) * 2 + c
            return remote(
                self.src, self.part(f), w_ss.at[self.slot, k], w_rs.at[self.slot, f], at_f(where)
            )

        def onward(self, k):
            index = flip(p, k) * 2 + c
            return remote(
                self.part(index),
                self.part(index),
                w_fs.at[self.slot, k],
                w_rs.at[self.slot, index],
                at_f(partner),
            )

        def across(self, first, second):
            index = flip(p, first) * 2 + c
            return remote(
                self.part(index),
                self.part(index),
                w_qs.at[self.slot, first + second],
                w_rs.at[self.slot, index],
                at_f(flip(p, second) * 2 + c),
            )

        def own(self):
            return pltpu.make_async_copy(self.src, self.part(f), w_ls.at[self.slot])

        def start(self):
            for k in self.aimed + [0]:
                self.direct(k).start()
            if self.local:
                self.own().start()

        def relay(self):
            for core, first, second in ((0, near, far), (1, far, near)):

                @pl.when(c == core)
                def _():
                    for k in first:
                        copy = self.onward(k)
                        copy.wait_recv()
                        for other in second:
                            self.across(k, other).start()
                        copy.start()

        def forward(self):
            if self.plain:
                for k in range(1, chips):
                    copy = self.onward(k)
                    copy.wait_recv()
                    copy.start()
                return

            for core, second in ((0, far), (1, near)):

                @pl.when(c == core)
                def _():
                    for k in second:
                        copy = self.onward(k)
                        copy.wait_recv()
                        copy.start()

            for k in near:
                for other in far:
                    copy = self.onward(k + other)
                    copy.wait_recv()
                    copy.start()

        def finish(self):
            for k in range(chips):
                index = flip(p, k) * 2 + 1 - c
                remote(
                    self.part(index),
                    self.part(index),
                    w_fs.at[self.slot, k],
                    w_rs.at[self.slot, index],
                    at_f(partner),
                ).wait_recv()
            if self.local:
                self.own().wait()

        def drain(self):
            for k in self.aimed + [0]:
                self.direct(k).wait_send()
            for k in range(1, chips):
                self.onward(k).wait_send()
            if self.plain:
                return
            for k in near:
                for other in far:
                    remote(
                        self.part(f),
                        self.part(f),
                        w_qs.at[self.slot, k + other],
                        w_rs.at[self.slot, f],
                        at_f(partner),
                    ).wait_send()

    class Line:
        def __init__(self, slot, buf, size=rows, parts=1, src=None):
            self.slot, self.buf, self.size, self.parts, self.src = slot, buf, size, parts, src

        def copy(self, index, side, h, own=False):
            piece = self.size // self.parts
            part = block(self.buf, index * self.parts + h, piece)
            src = part
            if own and self.src is not None:
                src = self.src.at[pl.ds(h * piece, piece)]
            where = d + 1 if side == 0 else d - 1
            return remote(
                src,
                part,
                z_ss.at[self.slot, side, h, index],
                z_rs.at[self.slot, h, index],
                at_d(where),
            )

        def start(self, h=0):
            @pl.when(d < n - 1)
            def _():
                self.copy(d, 0, h, True).start()

            @pl.when(d > 0)
            def _():
                self.copy(d, 1, h, True).start()

        def pass_on(self, index, side, h):
            copy = self.copy(index, side, h)
            copy.wait_recv()
            copy.start()

        def inward(self, s, h=0):
            @pl.when((d > 0) & (d < n // 2) & (d + s < n))
            def _():
                self.pass_on(d + s, 1, h)

            @pl.when((d < n - 1) & (d >= n // 2) & (d - s >= 0))
            def _():
                self.pass_on(d - s, 0, h)

        def outward(self, s, h=0):
            @pl.when((d < n // 2) & (d - s >= 0))
            def _():
                self.pass_on(d - s, 0, h)

            @pl.when((d >= n // 2) & (d + s < n))
            def _():
                self.pass_on(d + s, 1, h)

        def step(self, s, h=0):
            self.inward(s, h)
            self.outward(s, h)

        def arrive(self, s, h=0):
            @pl.when((d - s >= 0) & (d == n - 1))
            def _():
                self.copy(d - s, 0, h).wait_recv()

            @pl.when((d + s < n) & (d == 0))
            def _():
                self.copy(d + s, 1, h).wait_recv()

        def drain(self):
            for h in range(self.parts):
                for j in range(n):

                    @pl.when((j <= d) & (d < n - 1))
                    def _():
                        self.copy(j, 0, h).wait_send()

                    @pl.when((j >= d) & (d > 0))
                    def _():
                        self.copy(j, 1, h).wait_send()

    class Reduce:
        def __init__(self, slot, tile_of, sends, gets, also=None, plain=False):
            self.slot, self.tile_of, self.sends, self.gets = slot, tile_of, sends, gets
            self.also, self.plain = also, plain

        def over_tiles(self, tile):
            if self.plain:
                for t in range(width // TILE):
                    tile(t)
            else:
                loop(width // TILE, tile)

        def copy(self, index, where, slot, h):
            return remote(
                block(self.sends, 2 * index + h, half),
                block(self.gets, 2 * slot + h, half),
                rs_ss.at[self.slot, h, index],
                rs_rs.at[self.slot, h, slot],
                at_d(where),
            )

        def got(self, slot, h):
            part = block(self.gets, 2 * slot + h, half)
            remote(
                part, part, rs_ss.at[self.slot, h, 0], rs_rs.at[self.slot, h, slot], at_d(d)
            ).wait_recv()

        def right(self, index, h):
            return self.copy(index, d + 1, index, h)

        def left(self, index, h, last):
            return self.copy(index, d - 1, n if last else index, h)

        def compute(self, keep=True):
            def tile(t):
                value = self.tile_of(t, pl.ds(0, total))
                if keep:
                    wide_tile[...] = value
                    own_sum[:, cols(t)] = wide_tile[span(d, rows), :]
                self.sends[pl.ds(0, total), cols(t)] = value.astype(BF)

            loop(width // TILE, tile)

        def pair(self):
            first = d - 1 + low

            def tile(t):
                value = self.tile_of(t, pl.ds(pl.multiple_of(first * rows, rows), 2 * rows))
                wide_tile[0 : 2 * rows, :] = value
                own_sum[:, cols(t)] = wide_tile[span(1 - low, rows), :]
                self.sends[span(inner, rows), cols(t)] = wide_tile[span(low, rows), :].astype(BF)
                if self.also is not None:
                    self.also(t, value, pl.ds(pl.multiple_of(first * rows, rows), 2 * rows))

            self.over_tiles(tile)

        def single(self, j):
            def tile(t):
                value = self.tile_of(t, span(j, rows))
                self.sends[span(j, rows), cols(t)] = value.astype(BF)
                if self.also is not None:
                    self.also(t, value, span(j, rows))

            self.over_tiles(tile)

        def send_at(self, s, halves=(0, 1)):
            @pl.when(d == 0)
            def _():
                for h in halves:
                    self.right(d + s, h).start()

            @pl.when(d == n - 1)
            def _():
                for h in halves:
                    self.left(d - s, h, s == 1).start()

        def send_on(self, s):
            if s < n - 1:
                self.send_at(s, (0,))
            else:
                self.send_at(s)
                for nearer in range(2, n - 1):
                    self.send_at(nearer, (1,))

        def add_right(self, index, h):
            self.add_into(index, h)
            self.right(index, h).start()

        def add_left(self, index, h, last):
            self.add_into(index, h)
            self.left(index, h, last).start()

        def out_adv(self, s, h):
            @pl.when((d > 0) & (d < n // 2) & (d + s < n))
            def _():
                self.add_right(d + s, h)

            @pl.when((d < n - 1) & (d >= n // 2) & (d - s >= 0))
            def _():
                self.add_left(d - s, h, s == 1)

        def in_adv(self, s, h):
            @pl.when((d < n // 2) & (d - s >= 0))
            def _():
                self.add_left(d - s, h, s == 1)

            @pl.when((d >= n // 2) & (d + s < n))
            def _():
                self.add_right(d + s, h)

        def launch(self, halves_first):
            order = [(s, h) for h in range(2) for s in range(n - 1, 0, -1)]
            if not halves_first:
                order = [(s, h) for s in range(n - 1, 0, -1) for h in range(2)]

            @pl.when(d == 0)
            def _():
                for s, h in order:
                    self.right(d + s, h).start()

            @pl.when(d == n - 1)
            def _():
                for s, h in order:
                    self.left(d - s, h, s == 1).start()

        def add_into(self, index, h):
            self.got(index, h)

            def some(i):
                r = pl.ds(pl.multiple_of(index * rows + h * half + i * CHUNK, CHUNK), CHUNK)
                self.sends[r, :] = (
                    self.sends[r, :].astype(F32) + self.gets[r, :].astype(F32)
                ).astype(BF)

            loop(half // CHUNK, some)

        def advance(self, s, h):
            right, left = d + s, d - s

            @pl.when((right < n) & (d > 0))
            def _():
                self.add_into(right, h)
                self.right(right, h).start()

            @pl.when((left >= 0) & (d < n - 1))
            def _():
                self.add_into(left, h)
                self.left(left, h, s == 1).start()

        def final(self, h):
            self.final_into(own_sum, h)

        def final_into(self, acc, h):
            def add(slot):
                self.got(slot, h)

                def some(i):
                    r = pl.ds(pl.multiple_of(h * half + i * CHUNK, CHUNK), CHUNK)
                    there = pl.ds(
                        pl.multiple_of(slot * rows + h * half + i * CHUNK, CHUNK), CHUNK
                    )
                    acc[r, :] = acc[r, :] + self.gets[there, :].astype(F32)

                loop(half // CHUNK, some)

            @pl.when(d > 0)
            def _():
                add(d)

            @pl.when(d < n - 1)
            def _():
                add(n)

        def drain(self):
            for h in range(2):
                for j in range(n):

                    @pl.when(d != j)
                    def _():
                        self.copy(j, d, j, h).wait_send()

    def tiles(wide, body):
        if wide % TILE == 0:
            loop(wide // TILE, lambda t: body(cols(t)))
        else:
            for start in range(0, wide, TILE):
                body(pl.ds(start, min(TILE, wide - start)))

    handing = []

    class Grad:
        def __init__(self, group, turned, terms, emit):
            self.group, self.turned, self.terms, self.emit = group, turned, terms, emit
            self.width = gwidths[group]
            self.buffer = send_c if group == 1 else send_b

        def hand_over(self):
            src = self.buffer
            if self.group != 1 and self.width != widest:
                src = send_b.at[:, :, pl.ds(0, self.width)]
            return remote(
                src,
                from_partner[self.group],
                b_ss.at[self.group],
                b_rs.at[self.group],
                at_f(partner),
            )

        def ship(self, k):
            chip = flip(p, k)
            return remote(
                sums[self.group].at[chip],
                landing[self.group].at[k - 1],
                i_ss.at[self.group, k - 1],
                i_rs.at[self.group, k - 1],
                at_f(chip * 2 + c),
            )

        def blocks_of(self, core, lanes):
            left = jnp.concatenate(
                [self.turned[span(q * 2 + core, shard), :] for q in range(chips)], axis=0
            )
            value = mm(left, self.terms[:, lanes])
            return [value[q * shard : (q + 1) * shard] for q in range(chips)]

        def release(self):
            self.hand_over().wait_send()

        def send_all(self):
            if self.group != 1 and handing:
                handing.pop().release()

            def tile(lanes):
                for q, value in enumerate(self.blocks_of(1 - c, lanes)):
                    self.buffer[q, :, lanes] = value.astype(BF)

            tiles(self.width, tile)
            self.hand_over().start()
            if self.group != 1:
                handing.append(self)

        def own_sums(self):
            self.hand_over().wait_recv()

            def tile(lanes):
                for q, value in enumerate(self.blocks_of(c, lanes)):
                    other = from_partner[self.group][q, :, lanes].astype(F32)
                    sums[self.group][q, :, lanes] = (value + other).astype(BF)

            tiles(self.width, tile)

        def ship_all(self):
            if self.group < 2:
                for k in range(1, chips):
                    self.ship(k).start()
                return

            for core, first, second in ((0, near, far), (1, far, near)):

                @pl.when(c == core)
                def _():
                    for k in second:
                        for other in first:
                            self.via(other, k).start()
                        self.ship(k).start()

        def via(self, first, second):
            return remote(
                sums[self.group].at[flip(p, first + second)],
                between[self.group - 2].at[both_axes.index(first + second)],
                v_ss.at[self.group, first + second],
                v_rs.at[self.group, first + second],
                at_f(flip(p, second) * 2 + c),
            )

        def relay(self):
            for core, first, second in ((0, near, far), (1, far, near)):

                @pl.when(c == core)
                def _():
                    for k in first:
                        chip = flip(p, k)
                        for other in second:
                            self.via(k, other).wait_recv()
                            held = between[self.group - 2].at[both_axes.index(k + other)]

                            def tile(lanes):
                                total_here = sums[self.group][chip, :, lanes].astype(F32)
                                total_here = total_here + held[:, lanes].astype(F32)
                                sums[self.group][chip, :, lanes] = total_here.astype(BF)

                            tiles(self.width, tile)
                        self.ship(k).start()

        def partners(self):
            return near + far if self.group >= 2 else list(range(1, chips))

        def own_all(self):
            self.own_sums()
            self.ship_all()

        def fetch(self, k):
            return pltpu.make_async_copy(
                landing[self.group].at[k - 1],
                stage.at[k - 1, :, pl.ds(0, self.width)],
                l_sem.at[k - 1],
            )

        def collect(self):
            for k in self.partners():
                self.ship(k).wait()
                if self.group >= 2:
                    self.fetch(k).start()
            if self.group >= 2:
                for k in near:
                    for other in far:
                        self.via(k, other).wait_send()

        def finish(self):
            if self.group >= 2:
                for k in self.partners():
                    self.fetch(k).wait()

            def parts(lanes):
                yield sums[self.group][p, :, lanes]
                for k in self.partners():
                    if self.group >= 2:
                        yield stage[k - 1, :, lanes]
                    else:
                        yield landing[self.group][k - 1, :, lanes]

            self.emit(parts)

    def total_of(values):
        result = None
        for value in values:
            result = value if result is None else result + value
        return result

    stores = []

    def store(src, dst):
        copy = pltpu.make_async_copy(src, dst, out_sem.at[len(stores)])
        copy.start()
        stores.append(copy)

    def emit_plain(out):
        def emit(parts):
            def tile(t):
                big_own[:, cols(t)] = total_of(v.astype(F32) for v in parts(cols(t)))

            if big_stores:
                big_stores.pop().wait()
            loop(ff // TILE, tile)
            copy = pltpu.make_async_copy(big_own, out, l_sem.at[chips - 1])
            copy.start()
            big_stores.append(copy)

        return emit

    big_stores = []

    def summed(parts, start, size):
        return total_of(v.astype(F32) for v in parts(pl.ds(start, size)))

    q_real, kv_real = nq * HD, nkv * HD

    def emit_out(parts):
        o_own[...] = summed(parts, 0, q_real)
        store(o_own, out_o)

    def emit_qkv(parts):
        q_own[...] = summed(parts, 0, q_real)
        store(q_own, out_q)
        k_own[...] = summed(parts, q_real, kv_real)
        store(k_own, out_k)
        v_own[...] = summed(parts, q_real + kv_real, kv_real)
        store(v_own, out_v)

    def fill(dst, r, value):
        spare = dst.shape[1] - value.shape[1]
        if spare:
            value = jnp.concatenate([value, jnp.zeros((value.shape[0], spare), F32)], axis=1)
        dst[r, :] = value.astype(BF)

    def pack_mixed():
        def one(b):
            r = span(b, rows)
            fill(mixed_pack, r, mm_nt(mixed[r, :], pick_end[...]))

        loop(n, one)

    def pack_gqkv(b):
        r = span(b, rows)
        keys = slice(q_wide, q_wide + kv_wide)
        vals = slice(q_wide + kv_wide, q_wide + 2 * kv_wide)
        value = jnp.concatenate(
            [
                mm_nt(gqkv[r, 0:q_wide], pick_rope[...]),
                mm_nt(gqkv[r, keys], pick_rope[0:kv_real, 0:kv_wide]),
                mm_nt(gqkv[r, vals], pick_end[0:kv_real, 0:kv_wide]),
            ],
            axis=1,
        )
        fill(gqkv_pack, r, value)


    def turn(src, dst):
        def lane_block(t):
            dst[cols(t, LANES), :] = src[pl.ds(0, total), cols(t, LANES)].T

        loop(width // LANES, lane_block)

    def at(s, work):
        if s == 0:
            work(d)
            return

        def side(i):
            j = d - s + 2 * s * i

            @pl.when((j >= 0) & (j < n))
            def _():
                work(j)

        loop(2, side)

    def one_hot(split):
        shape = (nq * HD, q_wide)
        row = lax.broadcasted_iota(jnp.int32, shape, 0)
        lane = lax.broadcasted_iota(jnp.int32, shape, 1)
        inside = lane % LANES
        start = (lane // LANES) * HD
        if split:
            gap = LANES // 2 - HALF
            upper = inside >= LANES // 2
            source = start + jnp.where(upper, inside - gap, inside)
            real = (inside % (LANES // 2)) < HALF
        else:
            source = start + inside
            real = inside < HD
        return jnp.where(real & (row == source), 1.0, 0.0).astype(BF)

    pick_rope[...] = one_hot(True)
    pick_end[...] = one_hot(False)
    for copy in loads[7:]:
        copy.wait()
    gain_mine = block(gain_in, f, 8)
    gain_mine[...] = jnp.zeros(gain_mine.shape, F32)
    gain_mine[0:1, 0:shard] = gain_a[...].astype(F32)
    gain_mine[1:2, 0:shard] = gain_m[...].astype(F32)

    gathers = [
        Gather(0, weights[0], shard, plain=True),
        Gather(1, weights[1], shard, plain=True),
        Gather(2, weights[2], shard, w_g),
        Gather(3, weights[3], shard, w_u),
        Gather(4, weights[4], shard, w_d),
    ]
    gain_gather = Gather(5, gain_in, 8, plain=True)
    tok_line = Line(0, x_buf, parts=2, src=tokens)
    cot_line = Line(1, ct_buf, src=cot)
    mi_line = Line(2, mi_buf, parts=2)
    gm_line = Line(3, gm_buf, parts=2)

    def gain_swap(k):
        mine = block(gain_z, d, 8)
        return remote(
            mine, mine, z_ss.at[4, 0, 0, k], z_rs.at[4, 0, d], at_d((d + k) % n)
        )

    def gain_got(k):
        other = (d + k) % n
        part = block(gain_z, other, 8)
        remote(part, part, z_ss.at[4, 0, 0, k], z_rs.at[4, 0, other], at_d(d)).wait_recv()

    def segments(b, shape, dim):
        index = lax.broadcasted_iota(jnp.int32, shape, dim)
        segment = jnp.zeros(shape, jnp.int32)
        offset = jnp.zeros(shape, jnp.int32)
        end = jnp.int32(0)
        for k in range(nseq):
            end = end + lengths[b, k]
            past = index >= end
            segment = segment + past.astype(jnp.int32)
            offset = jnp.where(past, end, offset)
        return index, segment, offset

    def tables(b):
        index, _, offset = segments(b, (rows, LANES), 0)
        angle = (index - offset).astype(F32) * freq[...]
        lane = lax.broadcasted_iota(jnp.int32, (rows, LANES), 1)
        sine = jnp.sin(angle)
        block(cos_t, b)[...] = jnp.cos(angle)
        block(sin_t, b)[...] = jnp.where(lane < LANES // 2, -sine, sine)

    pl.semaphore_wait(barrier, chips + n - 1)
    for h in range(2):
        tok_line.start(h)

    @pl.when(end)
    def _():
        cot_line.start()

    gain_gather.start()
    mine = span(f, shard)
    kv_rows = nkv * HD
    for copy in loads[:4]:
        copy.wait()
    weights[0][mine, 0:q_wide] = mm(q_in[...], pick_rope[...]).astype(BF)
    weights[0][mine, q_wide : q_wide + kv_wide] = mm(
        k_in[...], pick_rope[0:kv_rows, 0:kv_wide]
    ).astype(BF)
    weights[0][mine, q_wide + kv_wide : q_wide + 2 * kv_wide] = mm(
        v_in[...], pick_end[0:kv_rows, 0:kv_wide]
    ).astype(BF)
    gathers[0].start()
    weights[1][mine, :] = mm(o_in[...], pick_end[...]).astype(BF)
    for g in range(1, 5):
        gathers[g].start()
    loop(n, tables)
    loads[4].wait()
    gain_gather.forward()
    gain_gather.finish()
    for k in range(nf):
        gain_row[:, k * shard : (k + 1) * shard] = gain_in[8 * k : 8 * k + 8, 0:shard]

    def rms(value):
        mean = jnp.sum(value * value, axis=-1, keepdims=True) / width
        return lax.rsqrt(mean + EPSILON)

    def norm_one(j):
        def some(i):
            r = pl.ds(pl.multiple_of(j * rows + i * CHUNK, CHUNK), CHUNK)
            value = x_buf[r, :].astype(F32)
            scale = rms(value)
            sc_one[r, :] = scale
            mi_buf[r, :] = (value * scale * gain_row[0:1, :]).astype(BF)

        loop(rows // CHUNK, some)

    def rope(value, sign, cos_v, sin_v):
        return value * cos_v + sign * (pltpu.roll(value, LANES // 2, 1) * sin_v)

    heads = nq + 2 * nkv

    def head(ref, r, h):
        return ref[r, h * LANES : (h + 1) * LANES]

    def attend(b):
        r = span(b, rows)
        cos_v, sin_v = cos_t[r, :], sin_t[r, :]
        for t in range(heads // 2):
            both = mm(mi_buf[r, :], weights[0][:, 2 * t * LANES : 2 * (t + 1) * LANES])
            for h in (2 * t, 2 * t + 1):
                value = both[:, (h - 2 * t) * LANES : (h - 2 * t + 1) * LANES]
                if h < nq + nkv:
                    value = rope(value, 1.0, cos_v, sin_v)
                qkv[r, h * LANES : (h + 1) * LANES] = value.astype(BF)
        t_index, t_seg, _ = segments(b, (rows, rows), 0)
        s_index, s_seg, _ = segments(b, (rows, rows), 1)
        allowed = (t_seg == s_seg) & (s_index <= t_index)
        for h in range(nq):
            kv = h // (nq // nkv)
            score = mm_nt(head(qkv, r, h), head(qkv, r, nq + kv)) * HD ** (-0.5)
            score = jnp.where(allowed, score, NEG_FILL)
            top = jnp.max(score, axis=-1, keepdims=True)
            log_total = top + jnp.log(jnp.sum(jnp.exp(score - top), axis=-1, keepdims=True))
            prob = jnp.where(allowed, jnp.exp(score - log_total), 0.0)
            probs[b * nq + h] = prob
            mixed[r, h * LANES : (h + 1) * LANES] = mm(
                prob.astype(BF), head(qkv, r, nq + nkv + kv)
            ).astype(BF)

    def tokens_at(s):
        for h in range(2):
            tok_line.step(s, h)
            tok_line.arrive(s, h)

    norm_one(d)
    tokens_at(1)
    at(1, norm_one)
    early = min(2, n - 1)
    if early == 2:
        for h in range(2):
            tok_line.step(2, h)

    @pl.when((d > 0) & (d < n - 1))
    def _():
        cot_line.start()

    gathers[0].forward()
    if early == 2:
        for h in range(2):
            tok_line.arrive(2, h)
        at(2, norm_one)
    gathers[0].finish()
    for s in range(early + 1):
        at(s, attend)
    gathers[1].forward()
    cot_line.outward(1)
    for s in range(early + 1, n):
        tokens_at(s)
        at(s, norm_one)
        at(s, attend)
    gathers[1].finish()

    def by_turned(pairs):
        def tile_of(t, r):
            return total_of(mm_nt(left[r, :], weight[cols(t), :]) for left, weight in pairs)

        return tile_of

    def run(work):
        if work:
            todo = work.pop(0)
            if todo is not None:
                todo()

    def reduce_then_gather(red, finish_half, line, work):
        red.compute()
        red.launch(True)
        run(work)
        for s in range(n - 2, 0, -1):
            red.advance(s, 0)
            run(work)
        red.final(0)
        finish_half(0)
        line.start(0)
        run(work)
        for i in range(1, n - 1):
            red.advance(n - 1 - i, 1)
            if i == 1:
                line.inward(i, 0)
            run(work)
        red.final(1)
        finish_half(1)
        line.start(1)
        for i in range(1, n - 1):
            if i > 1:
                line.inward(i, 0)
            line.outward(i, 0)

    def arrived(line, s):
        line.step(s, 1)
        line.arrive(s, 0)
        line.arrive(s, 1)

    def norm_two(h):
        def some(i):
            r = pl.ds(pl.multiple_of(h * half + i * CHUNK, CHUNK), CHUNK)
            here = pl.ds(pl.multiple_of(d * rows + h * half + i * CHUNK, CHUNK), CHUNK)
            value = x_buf[here, :].astype(F32) + own_sum[r, :]
            scale = rms(value)
            middle[r, :] = value
            sc_two[r, :] = scale
            mi_buf[here, :] = (value * scale * gain_row[1:2, :]).astype(BF)

        loop(half // CHUNK, some)

    def both(*todo):
        def do():
            for one in todo:
                one()

        return do

    def cot_on(s):
        def do():
            cot_line.inward(s)
            if s > 1:
                cot_line.outward(s)

        return do

    after_attn = Reduce(0, by_turned([(mixed, weights[1])]), s_buf, r_buf)
    work = [cot_on(1)]
    work += [both(cot_on(2), gathers[2].relay)] if n > 2 else [gathers[2].relay]
    work += [gathers[3].relay, None, gathers[4].relay, gathers[2].forward]
    work += [cot_on(s) for s in range(3, n - 1)]
    reduce_then_gather(after_attn, norm_two, mi_line, work)
    while work:
        run(work)
    pack_mixed()
    gathers[3].forward()
    gathers[4].forward()
    for g in (2, 3, 4):
        gathers[g].finish()
    loads[5].wait()
    loads[6].wait()

    def feed(j):
        r = span(j, rows)

        def tile(t):
            left = mi_buf[r, :]
            gate = mm(left, weights[2][:, cols(t)])
            up = mm(left, weights[3][:, cols(t)])
            grad_hidden = mm(ct_buf[r, :], weights[4][:, cols(t)])
            sig = 1.0 / (1.0 + jnp.exp(-gate))
            hid[r, cols(t)] = (gate * sig * up).astype(BF)
            gu[r, cols(t)] = (grad_hidden * gate * sig).astype(BF)
            gg[r, cols(t)] = (grad_hidden * up * sig * (1.0 + gate * (1.0 - sig))).astype(BF)

        loop(ff // TILE, tile)

    def at_outer(work):
        @pl.when((outer >= 0) & (outer < n))
        def _():
            work(outer)

    after_mlp = Reduce(1, by_turned([(gg, weights[2]), (gu, weights[3])]), s_buf, r_buf)
    after_attn.drain()
    at(0, feed)
    mi_line.step(1, 1)
    for s in range(1, n):
        for h in range(2):
            mi_line.arrive(s, h)
        cot_line.arrive(s)
        at(s, feed)
        if s + 1 < n:
            mi_line.step(s + 1, 1)
        if s == 1:
            after_mlp.pair()
            after_mlp.send_at(1)
            at_outer(after_mlp.single)
        else:
            at(s, after_mlp.single)
            after_mlp.send_at(s)

    gain_own[...] = jnp.zeros((8, width), F32)

    def back_two(h):
        def some(i):
            r = pl.ds(pl.multiple_of(h * half + i * CHUNK, CHUNK), CHUNK)
            term = own_sum[r, :]
            scale = sc_two[r, :]
            normed = middle[r, :] * scale
            gain_sum = jnp.sum(term * normed, axis=0, keepdims=True)
            dn = term * gain_row[1:2, :]
            mean = jnp.sum(dn * normed, axis=-1, keepdims=True) / width
            here = pl.ds(pl.multiple_of(d * rows + h * half + i * CHUNK, CHUNK), CHUNK)
            value = cot_own[r, :].astype(F32) + scale * (dn - normed * mean)
            gmid[r, :] = value
            gm_buf[here, :] = value.astype(BF)
            gain_own[1:2, :] = gain_own[1:2, :] + gain_sum

        loop(half // CHUNK, some)

    down = Grad(4, t_one, hid, emit_plain(out_d))
    gate_g = Grad(2, t_two, gg, emit_plain(out_g))
    up_g = Grad(3, t_two, gu, emit_plain(out_u))

    def turn_mi():
        turn(mi_buf, t_two)

    def attn_in_again(j):
        def some(i):
            r = pl.ds(pl.multiple_of(j * rows + i * CHUNK, CHUNK), CHUNK)
            value = x_buf[r, :].astype(F32) * sc_one[r, :]
            s_buf[r, :] = (value * gain_row[0:1, :]).astype(BF)

        loop(rows // CHUNK, some)

    output = Reduce(2, by_turned([(hid, weights[4])]), ct_buf, r_two)

    fits = widths[0] <= width and 3 * ff >= width and ff % TILE == 0

    def turn_qkv():
        for t in range(width // LANES if fits else 0):
            at_lane = t * LANES
            dst = weights[2 + at_lane // ff]
            dst[0 : widths[0], at_lane % ff : at_lane % ff + LANES] = weights[0][
                at_lane : at_lane + LANES, :
            ].T

    def finish_mlp():
        for h in range(2):
            after_mlp.final(h)
            back_two(h)
            if h == 0:
                gm_line.start(h)

    turn(ct_buf, t_one)
    cot_line.drain()
    turn_mi()
    down.send_all()
    for h in range(2):
        after_mlp.out_adv(1, h)
    output.compute(keep=False)
    output.send_at(n - 1)
    for s in range(2, n - 1):
        output.send_at(s, (0,))
    down.own_all()
    for s in range(2, n - 1):
        for h in range(2):
            after_mlp.out_adv(s, h)

    @pl.when(jnp.logical_not(end))
    def _():
        finish_mlp()

    gate_g.send_all()
    for g in (2, 3, 4):
        gathers[g].drain()
    turn_qkv()
    work = [both(gate_g.own_all, down.relay), up_g.send_all]
    for s in range(1, n - 1):
        for h in range(2):
            after_mlp.in_adv(s, h)
            run(work)
    while work:
        run(work)

    @pl.when(jnp.logical_not(end))
    def _():
        gm_line.start(1)

    gm_line.inward(1, 0)
    up_g.own_all()
    gm_line.inward(1, 1)
    gm_line.outward(1, 0)
    gm_line.outward(1, 1)

    @pl.when(end)
    def _():
        finish_mlp()
        gm_line.start(1)

    for s in range(2, n - 1):
        output.send_at(s, (1,))

    gate_g.relay()
    after_mlp.drain()
    mi_line.drain()

    def back(b):
        r = span(b, rows)

        def tile(t):
            gmixed[r, cols(t)] = mm(gm_buf[r, :], weights[1][:, cols(t)]).astype(BF)

        loop(q_wide // TILE, tile)
        cos_v, sin_v = cos_t[r, :], sin_t[r, :]
        group = nq // nkv
        for kv in range(nkv):
            key, val = head(qkv, r, nq + kv), head(qkv, r, nq + nkv + kv)
            grad_k = grad_v = None
            for h in range(kv * group, (kv + 1) * group):
                query, gm_h = head(qkv, r, h), head(gmixed, r, h)
                prob = probs[b * nq + h]
                delta = jnp.sum(
                    gm_h.astype(F32) * head(mixed, r, h).astype(F32), axis=-1, keepdims=True
                )
                grad_p = mm_nt(gm_h, val)
                grad_s = (prob * (grad_p - delta) * HD ** (-0.5)).astype(BF)
                grad_q = mm(grad_s, key)
                gqkv[r, h * LANES : (h + 1) * LANES] = rope(grad_q, -1.0, cos_v, sin_v).astype(BF)
                k_term, v_term = mm_tn(grad_s, query), mm_tn(prob.astype(BF), gm_h)
                grad_k = k_term if grad_k is None else grad_k + k_term
                grad_v = v_term if grad_v is None else grad_v + v_term
            k_at, v_at = (nq + kv) * LANES, (nq + nkv + kv) * LANES
            gqkv[r, k_at : k_at + LANES] = rope(grad_k, -1.0, cos_v, sin_v).astype(BF)
            gqkv[r, v_at : v_at + LANES] = grad_v.astype(BF)

    def add_gain(t, value, r):
        normed = x_buf[r, cols(t)].astype(F32) * sc_one[r, :]
        gain_own[0:1, cols(t)] = gain_own[0:1, cols(t)] + jnp.sum(
            value * normed, axis=0, keepdims=True
        )

    def by_qkv():
        if not fits:
            return by_turned([(gqkv, weights[0])])

        def tile_of(t, r):
            at_lane = t * TILE
            held = weights[2 + at_lane // ff]
            return mm(gqkv[r, :], held[0 : widths[0], at_lane % ff : at_lane % ff + TILE])

        return tile_of

    after_in = Reduce(3, by_qkv(), s_buf, r_buf, add_gain, plain=fits)
    out_g_grad = Grad(1, t_one, mixed_pack, emit_out)
    qkv_g = Grad(0, t_two, gqkv_pack, emit_qkv)

    def pass_gm(h):
        for s in range(2, n - 1):
            gm_line.inward(s, h)
            gm_line.outward(s, h)

    at(0, back)
    pass_gm(0)
    for h in range(2):
        gm_line.arrive(1, h)
    back(inner)
    pass_gm(1)
    for s in range(n - 2, 1, -1):
        for h in range(2):
            output.out_adv(s, h)
    loop(n, attn_in_again)
    turn(s_buf, t_two)
    after_in.pair()
    after_in.send_at(1)
    if n > 2:
        for h in range(2):
            output.out_adv(1, h)

    def outer_back(j):
        back(j)
        after_in.single(j)

    def ready(j):
        pack_gqkv(j)

        def lane_block(t):
            t_one[cols(t, LANES), span(j, rows)] = gm_buf[span(j, rows), cols(t, LANES)].T

        loop(width // LANES, lane_block)


    ready(d)
    ready(inner)
    at_outer(outer_back)
    at_outer(ready)
    for s in range(2, n):
        for h in range(2):
            gm_line.arrive(s, h)
        at(s, outer_back)
        if s < n - 1:
            after_in.send_on(s)
        if s == 2:
            up_g.relay()
        if s < n - 1:
            at(s, ready)
    if n == 2:
        up_g.relay()
    quarter = width // 4
    gain_mine = block(gain_z, d, 8)
    for i in range(8):
        gain_mine[i : i + 1, :] = gain_own[i // 4 : i // 4 + 1, pl.ds(i % 4 * quarter, quarter)]
    for k in range(1, n):
        gain_swap(k).start()
    if n > 2:
        after_in.send_on(n - 1)
        output.send_at(1)
    for s in range(1, n - 1):
        for h in range(2):
            output.in_adv(s, h)
    if n > 2:
        at(n - 1, ready)
    out_g_grad.send_all()
    qkv_g.send_all()
    out_g_grad.own_all()
    for h in range(2):
        after_in.out_adv(n - 2, h)
    qkv_g.own_sums()
    for k in range(1, n):
        gain_got(k)
    block(gain_f, f, 8)[...] = total_of(gain_z[8 * k : 8 * k + 8, :] for k in range(n))
    gain_back = Gather(6, gain_f, 8, plain=True)
    gain_back.start()
    qkv_g.ship_all()
    for s in range(n - 2, 0, -1):
        if s < n - 2:
            after_in.out_adv(s, 0)
        for h in range(2):
            after_in.in_adv(s, h)
        if s < n - 2:
            after_in.out_adv(s, 1)

    def output_end():
        middle[...] = middle[...] + block(ct_buf, d)[...].astype(F32)
        for h in range(2):
            output.final_into(middle, h)
        out_own[...] = middle[...].astype(BF)
        store(out_own, out_ref)

    def gain_end():
        gain_back.forward()
        gain_back.finish()
        gain_all = total_of(gain_f[8 * k : 8 * k + 8, :] for k in range(nf))
        for i in range(8):
            gain_own[i // 4 : i // 4 + 1, pl.ds(i % 4 * quarter, quarter)] = gain_all[i : i + 1, :]
        gain_all = pltpu.roll(gain_own[...], (width - f * shard) % width, 1)
        out_ga[...] = gain_all[0:1, 0:shard]
        out_gm[...] = gain_all[1:2, 0:shard]

    work = [gain_end]
    for grad in (down, gate_g, up_g):
        work.append(both(grad.collect, grad.finish))
    while work:
        run(work)

    def back_one(h):
        def some(i):
            r = pl.ds(pl.multiple_of(h * half + i * CHUNK, CHUNK), CHUNK)
            there = pl.ds(pl.multiple_of(d * rows + h * half + i * CHUNK, CHUNK), CHUNK)
            scale = sc_one[there, :]
            normed = x_buf[there, :].astype(F32) * scale
            dm = own_sum[r, :] * gain_row[0:1, :]
            mean = jnp.sum(dm * normed, axis=-1, keepdims=True) / width
            gmid[r, :] = gmid[r, :] + scale * (dm - normed * mean)

        loop(half // CHUNK, some)

    for h in range(2):
        after_in.final(h)
        back_one(h)
        part = pl.ds(h * half, half)
        store(gmid.at[part], gtok_ref.at[part])
    output_end()
    for grad in (qkv_g, out_g_grad):
        grad.collect()
        grad.finish()

    handing.pop().release()
    out_g_grad.release()
    output.drain()
    after_in.drain()
    tok_line.drain()
    gm_line.drain()
    for k in range(1, n):
        gain_swap(k).wait_send()
    for gather in gathers[:2] + [gain_gather, gain_back]:
        gather.drain()
    big_stores.pop().wait()
    for copy in stores:
        copy.wait()


def pass_on(*refs):
    count = (len(refs) - 2) // 3
    srcs, dsts, held = refs[:count], refs[count : 2 * count], refs[2 * count : 3 * count]
    in_sem, out_sem = refs[3 * count :]
    order = range(count)
    for i in order:
        pltpu.make_async_copy(srcs[i], held[i], in_sem.at[i]).start()
    for i in order:
        pltpu.make_async_copy(srcs[i], held[i], in_sem.at[i]).wait()
        pltpu.make_async_copy(held[i], dsts[i], out_sem.at[i]).start()
    for i in order:
        pltpu.make_async_copy(held[i], dsts[i], out_sem.at[i]).wait()


def run_layer(lengths, freq, tokens, cot, gain_a, gain_m, w_q, w_k, w_v, w_o, w_d, w_g, w_u, n, chips):
    rows, width = tokens.shape
    nq = w_q.shape[1] // HD
    nkv = w_k.shape[1] // HD
    total = n * rows
    nf = 2 * chips
    shard = w_q.shape[0]
    ff = w_g.shape[1]
    q_wide, kv_wide = nq * LANES, nkv * LANES
    widths = (q_wide + 2 * kv_wide, q_wide, ff, ff, ff)
    dims = (n, chips, rows, width, nq, nkv, ff, lengths.shape[1])
    vmem = pl.BlockSpec(memory_space=pltpu.VMEM)
    hbm = pl.BlockSpec(memory_space=pltpu.HBM)
    results = [
        jax.ShapeDtypeStruct((rows, width), BF),
        jax.ShapeDtypeStruct((rows, width), F32),
        jax.ShapeDtypeStruct((1, shard), F32),
        jax.ShapeDtypeStruct((1, shard), F32),
    ] + [jax.ShapeDtypeStruct(w.shape, F32) for w in (w_q, w_k, w_v, w_o, w_g, w_u, w_d)]
    out_shape = results + [jax.ShapeDtypeStruct((chips - 1, shard, w), BF) for w in widths[2:]]
    gwidths = packed_widths(nq, nkv, ff)
    widest = max(gwidths)
    scratch = (
        [pltpu.VMEM((chips - 1, shard, w), BF) for w in gwidths[:2]]
        + [pltpu.VMEM((width, w), BF) for w in widths]
        + [
            pltpu.VMEM((total, width), BF),
            pltpu.VMEM((total, width), BF),
            pltpu.VMEM((total, width), BF),
            pltpu.VMEM((total, width), BF),
            pltpu.VMEM((total + rows, width), BF),
            pltpu.VMEM((rows, width), BF),
            pltpu.VMEM((total, widths[0]), BF),
            pltpu.VMEM((total, widths[0]), BF),
            pltpu.VMEM((n * nq, rows, rows), F32),
            pltpu.VMEM((total, q_wide), BF),
            pltpu.VMEM((total, q_wide), BF),
            pltpu.VMEM((total, ff), BF),
            pltpu.VMEM((total, ff), BF),
            pltpu.VMEM((total, ff), BF),
            pltpu.VMEM((total, gwidths[0]), BF),
            pltpu.VMEM((total, gwidths[1]), BF),
            pltpu.VMEM((width, total), BF),
            pltpu.VMEM((width, total), BF),
            pltpu.VMEM((total, width), BF),
            pltpu.VMEM((total + rows, width), BF),
            pltpu.VMEM((rows, width), F32),
            pltpu.VMEM((rows, width), F32),
            pltpu.VMEM((rows, width), F32),
            pltpu.VMEM((total, TILE), F32),
            pltpu.VMEM((total, 1), F32),
            pltpu.VMEM((rows, 1), F32),
            pltpu.VMEM((total, LANES), F32),
            pltpu.VMEM((total, LANES), F32),
            pltpu.VMEM((nf * 8, -(-shard // LANES) * LANES), F32),
            pltpu.VMEM((8, width), F32),
            pltpu.VMEM((8, width), F32),
            pltpu.VMEM((n * 8, width // 4), F32),
            pltpu.VMEM((nf * 8, width // 4), F32),
            pltpu.VMEM((chips - 1, shard, widest), BF),
            pltpu.VMEM((nq * HD, q_wide), BF),
            pltpu.VMEM((nq * HD, q_wide), BF),
        ]
        + [pltpu.VMEM(w.shape, BF) for w in (w_q, w_k, w_v, w_o)]
        + [
            pltpu.SMEM(lengths.shape, jnp.int32),
            pltpu.VMEM(freq.shape, F32),
            pltpu.VMEM(gain_a.shape, BF),
            pltpu.VMEM(gain_m.shape, BF),
        ]
        + [pltpu.VMEM((rows, width), BF)]
        + [pltpu.VMEM(w.shape, F32) for w in (w_q, w_k, w_v, w_o, w_g)]
        + [
            pltpu.VMEM((chips, shard, widest), BF),
            pltpu.VMEM((chips, shard, gwidths[1]), BF),
        ]
        + [pltpu.VMEM((chips, shard, w), BF) for w in gwidths]
        + [pltpu.VMEM((chips, shard, w), BF) for w in gwidths]
        + [
            pltpu.SemaphoreType.DMA((7, chips)),
            pltpu.SemaphoreType.DMA((7, chips)),
            pltpu.SemaphoreType.DMA((7, chips)),
            pltpu.SemaphoreType.DMA((7, nf)),
            pltpu.SemaphoreType.DMA((7,)),
            pltpu.SemaphoreType.DMA((5, 2, 2, n)),
            pltpu.SemaphoreType.DMA((5, 2, n)),
            pltpu.SemaphoreType.DMA((4, 2, n)),
            pltpu.SemaphoreType.DMA((4, 2, n + 1)),
            pltpu.SemaphoreType.DMA((5,)),
            pltpu.SemaphoreType.DMA((5,)),
            pltpu.SemaphoreType.DMA((5, chips)),
            pltpu.SemaphoreType.DMA((5, chips)),
            pltpu.SemaphoreType.DMA((chips,)),
            pltpu.SemaphoreType.DMA((11,)),
            pltpu.SemaphoreType.DMA((7,)),
            pltpu.SemaphoreType.DMA((5, chips)),
            pltpu.SemaphoreType.DMA((5, chips)),
        ]
        + [pltpu.VMEM((max(1, chips // 2 - 1), shard, ff), BF)] * 3
    )
    made = pl.pallas_call(
        partial(layer_kernel, dims),
        out_shape=out_shape,
        in_specs=[hbm] * 13,
        out_specs=[hbm] * 2 + [vmem] * 2 + [hbm] * 10,
        scratch_shapes=scratch,
        compiler_params=pltpu.CompilerParams(
            collective_id=0, has_side_effects=True, vmem_limit_bytes=67043328
        ),
        name="layer",
    )(lengths, freq, gain_a, gain_m, tokens, cot, w_q, w_k, w_v, w_o, w_d, w_g, w_u)
    count = len(results)
    return pl.pallas_call(
        pass_on,
        out_shape=results,
        in_specs=[hbm] * count,
        out_specs=[hbm] * count,
        scratch_shapes=[pltpu.VMEM(r.shape, r.dtype) for r in results]
        + [pltpu.SemaphoreType.DMA((count,)), pltpu.SemaphoreType.DMA((count,))],
        compiler_params=pltpu.CompilerParams(vmem_limit_bytes=67043328),
        name="results",
    )(*made[:count])


def body(
    n,
    chips,
    tokens,
    lengths,
    cotangent,
    attn_gain,
    w_query,
    w_key,
    w_value,
    w_out,
    mlp_gain,
    w_gate,
    w_up,
    w_down,
):
    frequency = np.float64(ROPE_BASE) ** (-np.arange(HALF) / HALF)
    frequency = np.pad(frequency, (0, LANES // 2 - HALF))
    freq = jnp.asarray(np.concatenate([frequency, frequency])[None, :], F32)
    results = run_layer(
        lengths,
        freq,
        tokens,
        cotangent,
        attn_gain,
        mlp_gain,
        w_query[0],
        w_key[0],
        w_value[0],
        w_out[0].T,
        w_down[0].T,
        w_gate[0],
        w_up[0],
        n,
        chips,
    )
    output, grad_tokens, g_again, g_mgain, g_q, g_k, g_v, g_o, g_gate, g_up, g_down = results
    return (
        output,
        grad_tokens,
        g_again,
        g_q[None],
        g_k[None],
        g_v[None],
        g_o.T[None],
        g_mgain,
        g_gate[None],
        g_up[None],
        g_down.T[None],
    )


def solution(mesh):
    placed = (
        P(("fsdp", "dp"), None),
        P("fsdp", None),
        P(("fsdp", "dp"), None),
        P(None, "fsdp"),
        P(None, "fsdp", "dp"),
        P(None, "fsdp", "dp"),
        P(None, "fsdp", "dp"),
        P(None, "dp", "fsdp"),
        P(None, "fsdp"),
        P(None, "fsdp", "dp"),
        P(None, "fsdp", "dp"),
        P(None, "dp", "fsdp"),
    )
    return jax.shard_map(
        partial(body, mesh.shape["dp"], mesh.shape["fsdp"] // 2),
        mesh=mesh,
        in_specs=placed,
        out_specs=(
            P(("fsdp", "dp"), None),
            P(("fsdp", "dp"), None),
            P(None, "fsdp"),
            P(None, "fsdp", "dp"),
            P(None, "fsdp", "dp"),
            P(None, "fsdp", "dp"),
            P(None, "dp", "fsdp"),
            P(None, "fsdp"),
            P(None, "fsdp", "dp"),
            P(None, "fsdp", "dp"),
            P(None, "dp", "fsdp"),
        ),
        check_vma=False,
    )
```
